256 devices in a mesh: groups: 2 (over z), gx: 128 (over x, y, core).
Axes of the slice: x: 8, y: 8, z: 2, core: 2. Of those that a mesh axis runs over, the one named last changes fastest.
The devices are a block of a 8x8x16 slice.
Arguments:
- fields: float32 [3, 1024, 32768], P(None, 'groups', 'gx'), parts along dimension 1, may hold values from -0.7 to 1.4, as said below
- friction: float32 [1024, 32768], P('groups', 'gx'), parts along dimension 0, may hold values from 0.2 to 1.6
- wet_mask: int32 [1024, 32768], P('groups', 'gx'), parts along dimension 0, may hold values from 0 to 1, as said below
- owner_table: int32 [4, 128], P('groups'), parts along dimension 0, may hold values from 0 to 127, as said below
Outputs:
- final_fields: float32 [3, 1024, 32768], P(None, 'groups', 'gx'), parts along dimension 1
- owned_depth: float32 [1024, 32768], P('groups', 'gx'), parts along dimension 0
The draws below stay inside these ranges and needn't reach their ends.
There are 2 independent parts, one for each index of `groups`. The reference program is written for one: setup_inputs(seed, part) draws one part's arguments, and reference() takes and returns one part's arrays. A program takes and returns all parts, laid end to end along the dimension named above; each array names one. Nothing has to cross between parts.
Inputs may be any that keep to these rules, and one draw needn't show every extreme that they name: fields[0] is the depth, 0.6 to 1.4; fields[1] and fields[2] are the momenta, -0.7 to 0.7. `wet_mask`: land covers whole tiles: in each home column the tiles that hold water are the first ones (tile rows 0 up to some row, at least row 0), and some tiles hold no water. In each tile row and each aligned block of 8 home columns, owner_table[r, c] = c XOR k for one k from 0 to 7, so every device owns exactly one tile of each tile row.
All inputs are finite; a program needn't handle non-finite values.
Results may differ from the reference program's by a relative error of at most 0.0003.
Values sent between devices are 32-bit elements; how exact they have to be, the bound alone decides.
A program may use at most 64 MiB of HBM per device.

```python
import math
import jax
import jax.numpy as jnp
from jax import lax

TILE = 256
TILE_ROWS = 2
STEPS = 2
BLOCK = 8
NR = 512
NC = 32768
N_GX = 128


def coast_layout(key):
    layout_key = jax.random.fold_in(key, 101)
    first_key, second_key, order_key = jax.random.split(layout_key, 3)
    coast_depth = jnp.maximum(jax.random.randint(first_key, (N_GX,), 1, TILE_ROWS + 1) * jax.random.randint(second_key, (N_GX,), 0, 2), 1)
    row_numbers = jnp.arange(TILE_ROWS, dtype=jnp.int32)
    tile_wet = (row_numbers[:, None] < coast_depth[None, :]).astype(jnp.int32)
    block_count = N_GX // BLOCK
    combos = BLOCK ** TILE_ROWS
    combo_index = jnp.arange(combos, dtype=jnp.int32)
    powers = jnp.array([BLOCK ** power_index for power_index in range(TILE_ROWS)], jnp.int32)
    digits = combo_index[:, None] // powers[None, :] % BLOCK
    slot_numbers = jnp.arange(BLOCK, dtype=jnp.int32)
    source = jnp.bitwise_xor(slot_numbers[None, None, :], digits[:, :, None])
    wet_blocks = tile_wet.reshape(TILE_ROWS, block_count, BLOCK).transpose(1, 0, 2)
    spread_wet = jnp.broadcast_to(wet_blocks[:, None], (block_count, combos, TILE_ROWS, BLOCK))
    spread_source = jnp.broadcast_to(source[None], (block_count, combos, TILE_ROWS, BLOCK))
    gathered = jnp.take_along_axis(spread_wet, spread_source, axis=3)
    loads = jnp.max(jnp.sum(gathered, axis=2), axis=2)

    def shuffle(sub_key):
        return jax.random.permutation(sub_key, combos)
    ranks = jax.vmap(shuffle)(jax.random.split(order_key, block_count)).astype(jnp.int32)
    score = loads * combos + ranks
    best = jnp.argmin(score, axis=1)
    chosen_digits = digits[best]
    column_numbers = jnp.arange(N_GX, dtype=jnp.int32)
    owner_rows = jnp.bitwise_xor(column_numbers[None, :], chosen_digits[column_numbers // BLOCK].T)
    return (tile_wet, owner_rows.astype(jnp.int32))


def draw_wet_mask(key, part):
    tile_wet, owner_rows = coast_layout(key)
    cells = jax.random.randint(jax.random.fold_in(key, 202), (TILE_ROWS * TILE, N_GX * TILE), 0, 8)
    spread = jnp.repeat(jnp.repeat(tile_wet, TILE, axis=0), TILE, axis=1)
    return (spread * (cells > 0)).astype(jnp.int32)


def draw_owner_table(key, part):
    tile_wet, owner_rows = coast_layout(key)
    return owner_rows


def draw_fields(key, part):
    row_total = TILE_ROWS * TILE
    column_total = N_GX * TILE
    depth_key, flow_key = jax.random.split(jax.random.fold_in(key, 303))
    rough_depth = jax.random.uniform(depth_key, (row_total, column_total), jnp.float32, -1.0, 1.0)
    rough_flow = jax.random.uniform(flow_key, (2, row_total, column_total), jnp.float32, -1.0, 1.0)
    water = 1.0 + 0.4 * rough_depth
    flows = 0.7 * rough_flow
    return jnp.concatenate([water[None], flows], 0).astype(jnp.float32)


def steps_of(key, shape, cuts, smallest, top_value):
    def one(position, blocks):
        draws = jax.random.uniform(jax.random.fold_in(jax.random.fold_in(key, 6), position), (blocks,), jnp.float32, smallest / len(cuts), top_value / len(cuts))
        return jnp.repeat(jnp.exp(draws), shape[position] // blocks).reshape((-1,) + (1,) * (len(shape) - position - 1))

    level = one(*cuts[0])
    for cut in cuts[1:]:
        level = level * one(*cut)
    return level


def setup_inputs(seed: int = 0, part: int = 0) -> dict:
    streams_of = jax.random.split(jax.random.key(seed), 5)
    part_splits = jax.random.split(jax.random.fold_in(streams_of[4], part), 5)
    return {
        "fields": draw_fields(jax.random.fold_in(jax.random.fold_in(streams_of[4], part), 71), part),
        "friction": jnp.clip(jnp.exp(math.log(1.6) - 2.0794415 * jax.random.uniform(part_splits[1], (NR, NC), jnp.float32) ** steps_of(part_splits[1], (NR, NC), ((1, 128),), -0.2, 0.2)), 0.2, 1.6),
        "wet_mask": draw_wet_mask(jax.random.fold_in(jax.random.fold_in(streams_of[4], part), 71), part),
        "owner_table": draw_owner_table(jax.random.fold_in(jax.random.fold_in(streams_of[4], part), 71), part),
    }


gravity_half = 0.5
depth_floor = 0.25
flux_factor = 0.1
time_step = 0.25


def advance(padded, openness):
    water_depth = padded[0]
    east_flow = padded[1]
    south_flow = padded[2]
    safe_depth = jnp.maximum(water_depth, depth_floor)
    speed_east = east_flow / safe_depth
    speed_south = south_flow / safe_depth
    pressure = gravity_half * water_depth * water_depth
    flux_east = jnp.stack([east_flow, east_flow * speed_east + pressure, south_flow * speed_east])
    flux_south = jnp.stack([south_flow, east_flow * speed_south, south_flow * speed_south + pressure])
    average = 0.25 * (padded[:, 1:-1, 2:] + padded[:, 1:-1, :-2] + padded[:, 2:, 1:-1] + padded[:, :-2, 1:-1])
    update = average - flux_factor * (flux_east[:, 1:-1, 2:] - flux_east[:, 1:-1, :-2]) - flux_factor * (flux_south[:, 2:, 1:-1] - flux_south[:, :-2, 1:-1])
    wet_cells = (openness > 0.0).astype(jnp.float32)
    damping = wet_cells / (1.0 + time_step * openness)
    return jnp.stack([wet_cells * update[0], damping * update[1], damping * update[2]])


def reference(fields, friction, wet_mask, owner_table):
    openness = wet_mask.astype(jnp.float32) * friction
    wet_cells = (openness > 0.0).astype(jnp.float32)
    current = fields * wet_cells[None]
    for step_index in range(STEPS):
        padded = jnp.pad(current, ((0, 0), (1, 1), (1, 1)))

        def column_step(column_index):
            first_cell = (column_index * TILE).astype(jnp.int32)
            block_fields = lax.dynamic_slice_in_dim(padded, first_cell, TILE + 2, 2)
            local_open = lax.dynamic_slice_in_dim(openness, first_cell, TILE, 1)
            return advance(block_fields, local_open)

        pieces = lax.map(column_step, jnp.arange(N_GX, dtype=jnp.int32))
        current = jnp.transpose(pieces, (1, 2, 0, 3)).reshape(3, NR, NC)
    depth_tiles = current[0].reshape(TILE_ROWS, TILE, N_GX, TILE)
    columns = jnp.arange(N_GX, dtype=jnp.int32)
    row_numbers = jnp.arange(TILE_ROWS, dtype=jnp.int32)
    inverse = jnp.zeros((TILE_ROWS, N_GX), jnp.int32).at[row_numbers[:, None], owner_table].set(jnp.broadcast_to(columns[None, :], (TILE_ROWS, N_GX)))
    index_table = jnp.broadcast_to(inverse[:, None, :, None], (TILE_ROWS, TILE, N_GX, TILE))
    owned_depth = jnp.take_along_axis(depth_tiles, index_table, axis=2).reshape(NR, NC)
    return current, owned_depth
```

```python
import functools

import jax
import jax.numpy as jnp
from jax import lax
from jax.experimental import pallas as pl
from jax.experimental.pallas import tpu as pltpu
from jax.sharding import PartitionSpec as P

STEPS = 2
PAD = 8
CHUNKS = 4
LANES = 128

gravity_half = 0.5
depth_floor = 0.25
flux_factor = 0.1
time_step = 0.25


def advance(state, wet, damping, east, west, south, north):
    h, p, q = state
    inverse = 1.0 / jnp.maximum(h, depth_floor)
    u = p * inverse
    v = q * inverse
    pressure = gravity_half * h * h
    cross = q * u
    flux_p = p * u + pressure
    flux_q = q * v + pressure

    def gather(cell, flux_east, flux_south):
        quarter = 0.25 * cell
        along = flux_factor * flux_east
        down = flux_factor * flux_south
        return (east(quarter - along) + west(quarter + along)) + (
            south(quarter - down) + north(quarter + down)
        )

    return (
        wet * gather(h, p, q),
        damping * gather(p, flux_p, cross),
        damping * gather(q, cross, flux_q),
    )


def masks(openness):
    wet = jnp.where(openness > 0.0, 1.0, 0.0)
    return wet, wet / (1.0 + time_step * openness)


def flip(me, bit):
    stride = 2 ** bit
    return me + stride - 2 * stride * ((me // stride) % 2)


def kernel(
    axis,
    count,
    fields_ref,
    friction_ref,
    wet_ref,
    owner_ref,
    out_fields,
    out_depth,
    state,
    fric,
    mask,
    first,
    got_one,
    mid,
    got_mid,
    second,
    got_two,
    packed,
    halo_left,
    halo_right,
    edge,
    edge_turn,
    edge_first,
    edge_mid,
    edge_second,
    edge_got,
    edge_final,
    edge_wide,
    load_sem,
    send_sem,
    recv_sem,
    halo_send,
    halo_recv,
    edge_send,
    edge_recv,
):
    rows, cols = friction_ref.shape
    tile = cols
    tile_rows = rows // tile
    chunk = tile // CHUNKS
    me = lax.axis_index(axis)
    left = lax.rem(me + count - 1, count)
    right = lax.rem(me + 1, count)
    partner = [flip(me, bit) for bit in range(3)]

    loads = [
        pltpu.make_async_copy(
            fields_ref.at[plane], state.at[plane, pl.ds(PAD, rows), :], load_sem.at[plane]
        )
        for plane in range(3)
    ]
    loads.append(pltpu.make_async_copy(friction_ref, fric.at[pl.ds(PAD, rows), :], load_sem.at[3]))
    loads.append(pltpu.make_async_copy(wet_ref, mask.at[pl.ds(PAD, rows), :], load_sem.at[4]))
    for load in loads:
        load.start()

    barrier = pltpu.get_barrier_semaphore()
    peers = [left, right] + partner
    for peer in peers:
        pl.semaphore_signal(
            barrier, inc=1, device_id={axis: peer}, device_id_type=pl.DeviceIdType.MESH
        )

    zero_rows = jnp.zeros((PAD, cols), jnp.float32)
    for start in (0, PAD + rows):
        for plane in range(3):
            state[plane, start : start + PAD, :] = zero_rows
        fric[start : start + PAD, :] = zero_rows
        mask[start : start + PAD, :] = jnp.zeros((PAD, cols), jnp.int32)
    edge[...] = jnp.zeros_like(edge)
    edge_wide[...] = jnp.zeros_like(edge_wide)

    def bit_of(tile_row, bit):
        own = owner_ref[tile_row, me]
        return ((own // 2 ** bit) + (me // 2 ** bit)) % 2

    early = [2 if tile_row % 2 == 0 else 1 for tile_row in range(tile_rows)]
    late = [3 - bit for bit in early]

    def remote(src, dst, sems, bit):
        return pltpu.make_async_remote_copy(
            src_ref=src,
            dst_ref=dst,
            send_sem=sems[0],
            recv_sem=sems[1],
            device_id={axis: partner[bit]},
            device_id_type=pl.DeviceIdType.MESH,
        )

    def exchange(stage, tile_row, i):
        src, dst = ((first, got_one), (mid, got_mid), (second, got_two))[stage]
        bit = (early[tile_row], 0, late[tile_row])[stage]
        where = pl.ds(pl.multiple_of(i * chunk, chunk), chunk)
        return remote(
            src.at[tile_row, where, :],
            dst.at[tile_row, where, :],
            (send_sem.at[stage, tile_row, i], recv_sem.at[stage, tile_row, i]),
            bit,
        )

    def shift(axis_number, amount, size):
        return lambda a: pltpu.roll(a, amount % size, axis_number)

    def compute(tile_row, i):
        span = chunk + 2 * PAD
        at = pl.multiple_of(tile_row * tile + i * chunk, PAD)
        where = pl.ds(at, span)
        openness = mask[where, :].astype(jnp.float32) * fric[where, :]
        wet, damping = masks(openness)
        values = tuple(state[plane, where, :] * wet for plane in range(3))
        for _ in range(STEPS):
            values = advance(
                values,
                wet,
                damping,
                shift(1, -1, cols),
                shift(1, 1, cols),
                shift(0, -1, span),
                shift(0, 1, span),
            )
        here = pl.ds(at, chunk)
        for plane in range(3):
            out_fields[plane, here, :] = values[plane][PAD : PAD + chunk]
        first[tile_row, pl.ds(pl.multiple_of(i * chunk, chunk), chunk), :] = values[0][
            PAD : PAD + chunk
        ]

    for load in loads:
        load.wait()

    for tile_row in range(tile_rows):
        compute(tile_row, 0)
    pl.semaphore_wait(barrier, len(peers))
    for tile_row in range(tile_rows):
        exchange(0, tile_row, 0).start()

    lane = lax.broadcasted_iota(jnp.int32, (LANES, LANES), 1)

    @pl.loop(0, rows // LANES)
    def _(block):
        where = pl.ds(pl.multiple_of(PAD + block * LANES, PAD), LANES)
        open_sides = []
        for low in (0, cols - LANES):
            cut = pl.ds(low, LANES)
            open_sides.append(mask[where, cut].astype(jnp.float32) * fric[where, cut])
        result = jnp.zeros((LANES, LANES), jnp.float32)
        for side, low in enumerate((0, cols - LANES)):
            wet, _ = masks(open_sides[side])
            cut = pl.ds(low, LANES)
            planes = [state[plane, where, cut] * wet for plane in range(3)] + [open_sides[side]]
            for number, values in enumerate(planes):
                for inner in range(2):
                    if side == 0:
                        source = 2 * inner
                    else:
                        source = LANES - 2 - 2 * inner
                    target = 16 * inner + 8 * side + 2 * number
                    moved = pltpu.roll(values, (target - source) % LANES, 1)
                    result = jnp.where((lane >= target) & (lane < target + 2), moved, result)
        packed[:, pl.ds(pl.multiple_of(block * LANES, LANES), LANES)] = result.T[0:32]

    halo_copies = [
        pltpu.make_async_remote_copy(
            src_ref=packed.at[pl.ds(8 * side, 8), :],
            dst_ref=(halo_right, halo_left)[side],
            send_sem=halo_send.at[side],
            recv_sem=halo_recv.at[side],
            device_id={axis: (left, right)[side]},
            device_id_type=pl.DeviceIdType.MESH,
        )
        for side in range(2)
    ]
    for copy in halo_copies:
        copy.start()

    @pl.loop(1, CHUNKS)
    def _(i):
        for tile_row in range(tile_rows):
            compute(tile_row, i)
            exchange(0, tile_row, i).start()

    for copy in halo_copies:
        copy.wait_recv()

    keep_left = jnp.where(me > 0, 1.0, 0.0)
    keep_right = jnp.where(me < count - 1, 1.0, 0.0)
    for number in range(4):
        pair = pl.ds(2 * number, 2)
        edge[number, 0:2, :] = halo_left[pair, :] * keep_left
        edge[number, 2:4, :] = packed[pl.ds(2 * number, 2), :]
        edge[number, 4:6, :] = packed[pl.ds(16 + 2 * number, 2), :]
        edge[number, 8:10, :] = packed[pl.ds(24 + 2 * number, 2), :]
        edge[number, 10:12, :] = packed[pl.ds(8 + 2 * number, 2), :]
        edge[number, 12:14, :] = halo_right[pair, :] * keep_right

    place = lax.broadcasted_iota(jnp.int32, (16, rows), 1)
    wet, damping = masks(edge[3])
    values = tuple(edge[plane] for plane in range(3))
    for _ in range(STEPS):
        values = advance(
            values,
            wet,
            damping,
            shift(0, -1, 16),
            shift(0, 1, 16),
            lambda a: jnp.where(place == rows - 1, 0.0, pltpu.roll(a, rows - 1, 1)),
            lambda a: jnp.where(place == 0, 0.0, pltpu.roll(a, 1, 1)),
        )
    edge_turn[...] = jnp.zeros_like(edge_turn)
    for plane in range(3):
        edge_turn[16 * plane : 16 * plane + 16, :] = values[plane]
    for tile_row in range(tile_rows):
        cut = pl.ds(tile_row * tile, tile)
        edge_first[4 * tile_row : 4 * tile_row + 2, :] = edge_turn[2:4, cut]
        edge_first[4 * tile_row + 2 : 4 * tile_row + 4, :] = edge_turn[10:12, cut]

    edge_bits = (2, 0, 1)
    edge_sends = (edge_first, edge_mid, edge_second)

    def edge_exchange(stage):
        return remote(
            edge_sends[stage],
            edge_got.at[stage],
            (edge_send.at[stage], edge_recv.at[stage]),
            edge_bits[stage],
        )

    edge_line = lax.broadcasted_iota(jnp.int32, (8, tile), 0)

    def edge_select(stage):
        bit = edge_bits[stage]
        taken = jnp.where(edge_line < 4, bit_of(0, bit), bit_of(1, bit))
        return jnp.where(taken == 1, edge_got[stage], edge_sends[stage][...])

    edge_exchange(0).start()

    narrow = lax.broadcasted_iota(jnp.int32, (LANES, LANES), 1)

    @pl.loop(0, rows // LANES)
    def _(block):
        where = pl.ds(pl.multiple_of(block * LANES, LANES), LANES)
        turned = edge_turn[:, where].T
        for plane in range(3):
            on_left = pltpu.roll(turned, (-16 * plane - 2) % LANES, 1)
            cut = pl.ds(0, LANES)
            out_fields[plane, where, cut] = jnp.where(
                narrow < 2, on_left, out_fields[plane, where, cut]
            )
            on_right = pltpu.roll(turned, (LANES - 2 - 16 * plane - 10) % LANES, 1)
            cut = pl.ds(cols - LANES, LANES)
            out_fields[plane, where, cut] = jnp.where(
                narrow >= LANES - 2, on_right, out_fields[plane, where, cut]
            )

    def pick(stage, tile_row, i):
        src, dst = ((first, got_one), (mid, got_mid), (second, got_two))[stage]
        bit = (early[tile_row], 0, late[tile_row])[stage]
        where = pl.ds(i * chunk, chunk)
        taken = jnp.full((chunk, tile), bit_of(tile_row, bit), jnp.int32)
        return jnp.where(taken == 1, dst[tile_row, where, :], src[tile_row, where, :])

    for i in range(CHUNKS + 1):
        if i < CHUNKS:
            for tile_row in range(tile_rows):
                exchange(0, tile_row, i).wait_recv()
                mid[tile_row, i * chunk : (i + 1) * chunk, :] = pick(0, tile_row, i)
                exchange(1, tile_row, i).start()
        if i == CHUNKS - 1:
            edge_exchange(0).wait_recv()
            edge_mid[...] = edge_select(0)
            edge_exchange(1).start()
        if i == CHUNKS:
            edge_exchange(1).wait_recv()
            edge_second[...] = edge_select(1)
            edge_exchange(2).start()
        if i >= 1:
            for tile_row in range(tile_rows):
                exchange(1, tile_row, i - 1).wait_recv()
                second[tile_row, (i - 1) * chunk : i * chunk, :] = pick(1, tile_row, i - 1)
                exchange(2, tile_row, i - 1).start()

    edge_exchange(2).wait_recv()
    edge_final[...] = jnp.zeros_like(edge_final)
    edge_final[0:8, :] = edge_select(2)
    for tile_row in range(tile_rows):
        for block in range(tile // LANES):
            turned = edge_final[:, block * LANES : (block + 1) * LANES].T
            where = pl.ds(block * LANES, LANES)
            edge_wide[tile_row, where, 0:LANES] = pltpu.roll(turned, (-4 * tile_row) % LANES, 1)
            edge_wide[tile_row, where, cols - LANES : cols] = pltpu.roll(
                turned, (LANES - 2 - 4 * tile_row - 2) % LANES, 1
            )

    column = lax.broadcasted_iota(jnp.int32, (chunk, cols), 1)
    inside = (column >= 2) & (column < cols - 2)
    for i in range(CHUNKS):
        for tile_row in range(tile_rows):
            exchange(2, tile_row, i).wait_recv()
            out_depth[tile_row * tile + i * chunk : tile_row * tile + (i + 1) * chunk, :] = jnp.where(
                inside, pick(2, tile_row, i), edge_wide[tile_row, i * chunk : (i + 1) * chunk, :]
            )

    for copy in halo_copies:
        copy.wait_send()
    for stage in range(3):
        edge_exchange(stage).wait_send()
        for tile_row in range(tile_rows):
            for i in range(CHUNKS):
                exchange(stage, tile_row, i).wait_send()


def solution(mesh):
    axis = "gx"
    count = mesh.shape[axis]

    def body(fields, friction, wet_mask, owner_table):
        rows, cols = friction.shape
        tile_rows = rows // cols
        tiles = (tile_rows, cols, cols)
        padded = rows + 2 * PAD
        f32 = jnp.float32
        scratch = [
            pltpu.VMEM((3, padded, cols), f32),
            pltpu.VMEM((padded, cols), f32),
            pltpu.VMEM((padded, cols), jnp.int32),
            pltpu.VMEM(tiles, f32),
            pltpu.VMEM(tiles, f32),
            pltpu.VMEM(tiles, f32),
            pltpu.VMEM(tiles, f32),
            pltpu.VMEM(tiles, f32),
            pltpu.VMEM(tiles, f32),
            pltpu.VMEM((32, rows), f32),
            pltpu.VMEM((8, rows), f32),
            pltpu.VMEM((8, rows), f32),
            pltpu.VMEM((4, 16, rows), f32),
            pltpu.VMEM((LANES, rows), f32),
            pltpu.VMEM((8, cols), f32),
            pltpu.VMEM((8, cols), f32),
            pltpu.VMEM((8, cols), f32),
            pltpu.VMEM((3, 8, cols), f32),
            pltpu.VMEM((LANES, cols), f32),
            pltpu.VMEM(tiles, f32),
            pltpu.SemaphoreType.DMA((5,)),
            pltpu.SemaphoreType.DMA((3, tile_rows, CHUNKS)),
            pltpu.SemaphoreType.DMA((3, tile_rows, CHUNKS)),
            pltpu.SemaphoreType.DMA((2,)),
            pltpu.SemaphoreType.DMA((2,)),
            pltpu.SemaphoreType.DMA((3,)),
            pltpu.SemaphoreType.DMA((3,)),
        ]
        return pl.pallas_call(
            functools.partial(kernel, axis, count),
            out_shape=(
                jax.ShapeDtypeStruct(fields.shape, f32),
                jax.ShapeDtypeStruct(friction.shape, f32),
            ),
            in_specs=[
                pl.BlockSpec(memory_space=pl.ANY),
                pl.BlockSpec(memory_space=pl.ANY),
                pl.BlockSpec(memory_space=pl.ANY),
                pl.BlockSpec(memory_space=pltpu.SMEM),
            ],
            out_specs=(
                pl.BlockSpec(memory_space=pltpu.VMEM),
                pl.BlockSpec(memory_space=pltpu.VMEM),
            ),
            scratch_shapes=scratch,
            compiler_params=pltpu.CompilerParams(collective_id=0, has_side_effects=True),
            name="shallow_water",
        )(fields, friction, wet_mask, owner_table)

    in_specs = (P(None, "groups", axis), P("groups", axis), P("groups", axis), P("groups", None))
    out_specs = (P(None, "groups", axis), P("groups", axis))
    return jax.shard_map(body, mesh=mesh, in_specs=in_specs, out_specs=out_specs, check_vma=False)
```

```python
import functools

import jax
import jax.numpy as jnp
from jax import lax
from jax.experimental import pallas as pl
from jax.experimental.pallas import tpu as pltpu
from jax.sharding import PartitionSpec as P

STEPS = 2
PAD = 8
CHUNK = 64
MESSAGE = 32
LANES = 128

gravity_half = 0.5
depth_floor = 0.25
flux_factor = 0.1
time_step = 0.25


def advance(state, wet, damping, east, west, south, north):
    h, p, q = state
    inverse = 1.0 / jnp.maximum(h, depth_floor)
    u = p * inverse
    v = q * inverse
    pressure = gravity_half * h * h
    cross = q * u
    flux_p = p * u + pressure
    flux_q = q * v + pressure

    def gather(cell, flux_east, flux_south):
        quarter = 0.25 * cell
        along = flux_factor * flux_east
        down = flux_factor * flux_south
        return (east(quarter - along) + west(quarter + along)) + (
            south(quarter - down) + north(quarter + down)
        )

    return (
        wet * gather(h, p, q),
        damping * gather(p, flux_p, cross),
        damping * gather(q, cross, flux_q),
    )


def masks(openness):
    wet = jnp.where(openness > 0.0, 1.0, 0.0)
    return wet, wet / (1.0 + time_step * openness)


def kernel(
    axis,
    count,
    fields_ref,
    friction_ref,
    wet_ref,
    owner_ref,
    out_fields,
    out_depth,
    state,
    fric,
    mask,
    owner,
    first,
    inbox,
    back,
    turn,
    mine,
    other,
    packed,
    halo_left,
    halo_right,
    edge,
    edge_turn,
    edge_first,
    edge_in,
    edge_back,
    edge_give,
    edge_mine,
    edge_other,
    edge_final,
    edge_wide,
    load_sem,
    raw_send,
    relay_send,
    in_recv,
    back_send,
    back_recv,
    swap_send,
    swap_recv,
    halo_send,
    halo_recv,
):
    rows, cols = friction_ref.shape
    tile = cols
    tile_rows = rows // tile
    messages = rows // MESSAGE
    extra = messages
    MESH = pl.DeviceIdType.MESH

    me = lax.axis_index(axis)
    odd = me % 2
    position = me % 8
    chip = position // 2
    middle = ((chip + 1) // 2) % 2
    toward = me + 2 - 4 * (chip // 2)
    outward = 2 * me - toward
    sibling = me + 1 - 2 * odd
    is_middle = middle == 1
    is_end = middle == 0

    last = jnp.where(me == count - 1, 1, 0)
    lead_left = jnp.where(position == 0, 0, 1 - odd)
    follow_left = jnp.where(me == 0, 0, 1 - lead_left)
    lead_right = jnp.where(position == 7, 1, 1 - odd) * (1 - last)
    follow_right = (1 - last) * (1 - lead_right)

    loads = [
        pltpu.make_async_copy(
            fields_ref.at[plane], state.at[plane, pl.ds(PAD, rows), :], load_sem.at[plane]
        )
        for plane in range(3)
    ]
    loads.append(pltpu.make_async_copy(friction_ref, fric.at[pl.ds(PAD, rows), :], load_sem.at[3]))
    loads.append(pltpu.make_async_copy(wet_ref, mask.at[pl.ds(PAD, rows), :], load_sem.at[4]))
    loads.append(pltpu.make_async_copy(owner_ref, owner, load_sem.at[5]))
    for load in loads:
        load.start()

    barrier = pltpu.get_barrier_semaphore()

    def greet(peer):
        pl.semaphore_signal(barrier, inc=1, device_id={axis: peer}, device_id_type=MESH)

    @pl.when(is_middle)
    def _():
        greet(outward)
        greet(toward)

    @pl.when(follow_left == 1)
    def _():
        greet(me - 1)

    @pl.when(follow_right == 1)
    def _():
        greet(me + 1)

    zero_rows = jnp.zeros((PAD, cols), jnp.float32)
    for start in (0, PAD + rows):
        for plane in range(3):
            state[plane, start : start + PAD, :] = zero_rows
        fric[start : start + PAD, :] = zero_rows
        mask[start : start + PAD, :] = jnp.zeros((PAD, cols), jnp.int32)
    edge[...] = jnp.zeros_like(edge)
    edge_turn[...] = jnp.zeros_like(edge_turn)
    edge_final[...] = jnp.zeros_like(edge_final)

    def differs(tile_row, bit):
        own = owner[tile_row, me]
        return (own // 2 ** bit + me // 2 ** bit) % 2

    def remote(src, dst, send, recv, peer):
        return pltpu.make_async_remote_copy(
            src_ref=src,
            dst_ref=dst,
            send_sem=send,
            recv_sem=recv,
            device_id={axis: peer},
            device_id_type=MESH,
        )

    def span(m):
        return pl.ds(pl.multiple_of(m * MESSAGE, MESSAGE), MESSAGE)

    def raw(m, slot):
        return remote(
            first.at[span(m), :], inbox.at[slot, span(m), :], raw_send.at[m], in_recv.at[slot, m], toward
        )

    def relay(m):
        return remote(
            inbox.at[0, span(m), :], inbox.at[2, span(m), :], relay_send.at[m], in_recv.at[2, m], toward
        )

    def give(m):
        return remote(turn.at[span(m), :], back.at[span(m), :], back_send.at[m], back_recv.at[m], outward)

    def swap(m):
        return remote(mine.at[span(m), :], other.at[span(m), :], swap_send.at[m], swap_recv.at[m], sibling)

    def edge_raw(slot):
        return remote(edge_first, edge_in.at[slot], raw_send.at[extra], in_recv.at[slot, extra], toward)

    edge_relay = remote(
        edge_in.at[0], edge_in.at[2], relay_send.at[extra], in_recv.at[2, extra], toward
    )
    edge_return = remote(edge_give, edge_back, back_send.at[extra], back_recv.at[extra], outward)
    edge_swap = remote(edge_mine, edge_other, swap_send.at[extra], swap_recv.at[extra], sibling)

    halo_to_left = remote(
        packed.at[pl.ds(0, 8), :], halo_right, halo_send.at[0], halo_recv.at[0], me - 1
    )
    halo_to_right = remote(
        packed.at[pl.ds(8, 8), :], halo_left, halo_send.at[1], halo_recv.at[1], me + 1
    )

    def shift(axis_number, amount, size):
        return lambda a: pltpu.roll(a, amount % size, axis_number)

    def compute(i):
        height = CHUNK + 2 * PAD
        at = pl.multiple_of(i * CHUNK, CHUNK)
        where = pl.ds(at, height)
        openness = mask[where, :].astype(jnp.float32) * fric[where, :]
        wet, damping = masks(openness)
        values = tuple(state[plane, where, :] * wet for plane in range(3))
        for _ in range(STEPS):
            values = advance(
                values,
                wet,
                damping,
                shift(1, -1, cols),
                shift(1, 1, cols),
                shift(0, -1, height),
                shift(0, 1, height),
            )
        here = pl.ds(at, CHUNK)
        first[here, :] = values[0][PAD : PAD + CHUNK]
        for plane in range(3):
            out_fields[plane, here, :] = values[plane][PAD : PAD + CHUNK]

    for load in loads:
        load.wait()

    compute(0)
    pl.semaphore_wait(barrier, 1 + lead_left + lead_right)
    for part in range(CHUNK // MESSAGE):
        raw(part, middle).start()

    lane = lax.broadcasted_iota(jnp.int32, (LANES, LANES), 1)

    @pl.loop(0, rows // LANES)
    def _(block):
        where = pl.ds(pl.multiple_of(PAD + block * LANES, PAD), LANES)
        result = jnp.zeros((LANES, LANES), jnp.float32)
        for side, low in enumerate((0, cols - LANES)):
            cut = pl.ds(low, LANES)
            openness = mask[where, cut].astype(jnp.float32) * fric[where, cut]
            wet, _ = masks(openness)
            planes = [state[plane, where, cut] * wet for plane in range(3)] + [openness]
            for number, values in enumerate(planes):
                for inner in range(2):
                    source = LANES - 2 - 2 * inner if side else 2 * inner
                    target = 16 * inner + 8 * side + 2 * number
                    moved = pltpu.roll(values, (target - source) % LANES, 1)
                    result = jnp.where((lane >= target) & (lane < target + 2), moved, result)
        packed[:, pl.ds(pl.multiple_of(block * LANES, LANES), LANES)] = result.T[0:32]

    @pl.when(lead_left == 1)
    def _():
        halo_to_left.start()

    @pl.when(lead_right == 1)
    def _():
        halo_to_right.start()

    @pl.loop(1, rows // CHUNK)
    def _(i):
        compute(i)
        for part in range(CHUNK // MESSAGE):
            raw(i * (CHUNK // MESSAGE) + part, middle).start()

    @pl.when(follow_right == 1)
    def _():
        halo_to_left.wait_recv()
        halo_to_right.start()

    @pl.when(follow_left == 1)
    def _():
        halo_to_right.wait_recv()
        halo_to_left.start()

    @pl.when(lead_right == 1)
    def _():
        halo_to_left.wait_recv()

    @pl.when(lead_left == 1)
    def _():
        halo_to_right.wait_recv()

    for number in range(4):
        pair = pl.ds(2 * number, 2)
        edge[number, 0:2, :] = jnp.where(me > 0, halo_left[pair, :], 0.0)
        edge[number, 2:4, :] = packed[pl.ds(2 * number, 2), :]
        edge[number, 4:6, :] = packed[pl.ds(16 + 2 * number, 2), :]
        edge[number, 8:10, :] = packed[pl.ds(24 + 2 * number, 2), :]
        edge[number, 10:12, :] = packed[pl.ds(8 + 2 * number, 2), :]
        edge[number, 12:14, :] = jnp.where(me < count - 1, halo_right[pair, :], 0.0)

    place = lax.broadcasted_iota(jnp.int32, (16, rows), 1)
    wet, damping = masks(edge[3])
    values = tuple(edge[plane] for plane in range(3))
    for _ in range(STEPS):
        values = advance(
            values,
            wet,
            damping,
            shift(0, -1, 16),
            shift(0, 1, 16),
            lambda a: jnp.where(place == rows - 1, 0.0, pltpu.roll(a, rows - 1, 1)),
            lambda a: jnp.where(place == 0, 0.0, pltpu.roll(a, 1, 1)),
        )
    for plane in range(3):
        edge_turn[16 * plane : 16 * plane + 16, :] = values[plane]
    for tile_row in range(tile_rows):
        cut = pl.ds(tile_row * tile, tile)
        edge_first[4 * tile_row : 4 * tile_row + 2, :] = edge_turn[2:4, cut]
        edge_first[4 * tile_row + 2 : 4 * tile_row + 4, :] = edge_turn[10:12, cut]
    edge_raw(middle).start()

    @pl.when(is_middle)
    def _():
        @pl.loop(0, messages - 2)
        def _(m):
            raw(m, 0).wait_recv()
            relay(m).start()

        edge_raw(0).wait_recv()
        edge_relay.start()
        for m in range(messages - 2, messages):
            raw(m, 0).wait_recv()
            relay(m).start()

    @pl.loop(0, rows // LANES)
    def _(block):
        where = pl.ds(pl.multiple_of(block * LANES, LANES), LANES)
        turned = edge_turn[:, where].T
        for plane in range(3):
            on_left = pltpu.roll(turned, (-16 * plane - 2) % LANES, 1)
            cut = pl.ds(0, LANES)
            out_fields[plane, where, cut] = jnp.where(
                lane < 2, on_left, out_fields[plane, where, cut]
            )
            on_right = pltpu.roll(turned, (LANES - 2 - 16 * plane - 10) % LANES, 1)
            cut = pl.ds(cols - LANES, LANES)
            out_fields[plane, where, cut] = jnp.where(
                lane >= LANES - 2, on_right, out_fields[plane, where, cut]
            )

    moves = [differs(tile_row, 1) + 2 * differs(tile_row, 2) for tile_row in range(tile_rows)]
    flips = [differs(tile_row, 0) for tile_row in range(tile_rows)]

    def for_end(by, own, near, far):
        return jnp.where(by == 3, far, jnp.where(by == 2, near, own))

    def for_middle(by, own, end, near, far):
        return jnp.where(by == 3, near, jnp.where(by == 2, far, jnp.where(by == 1, end, own)))

    def of_row(pair, m, shape):
        value = pair[-1]
        for tile_row in reversed(range(tile_rows - 1)):
            value = jnp.where(m < (tile_row + 1) * (tile // MESSAGE), pair[tile_row], value)
        return jnp.full(shape, value, jnp.int32)

    def settle(m):
        where = span(m)
        by = of_row(moves, m, (MESSAGE, cols))

        @pl.when(is_middle)
        def _():
            raw(m, 1).wait_recv()
            relay(m).wait_recv()
            own = first[where, :]
            near = inbox[1, where, :]
            far = inbox[2, where, :]
            turn[where, :] = for_end(by, own, near, far)
            give(m).start()
            mine[where, :] = for_middle(by, own, inbox[0, where, :], near, far)

        @pl.when(is_end)
        def _():
            give(m).wait_recv()
            mine[where, :] = jnp.where(by == 0, first[where, :], back[where, :])

        swap(m).start()

    line = lax.broadcasted_iota(jnp.int32, (8, cols), 0)

    def by_line(pair):
        value = jnp.full((8, cols), pair[-1], jnp.int32)
        for tile_row in reversed(range(tile_rows - 1)):
            value = jnp.where(line < 4 * (tile_row + 1), pair[tile_row], value)
        return value

    @pl.loop(0, messages - 2)
    def _(m):
        settle(m)

    edge_by = by_line(moves)

    @pl.when(is_middle)
    def _():
        edge_raw(1).wait_recv()
        edge_relay.wait_recv()
        own = edge_first[...]
        near = edge_in[1]
        far = edge_in[2]
        edge_give[...] = for_end(edge_by, own, near, far)
        edge_return.start()
        edge_mine[...] = for_middle(edge_by, own, edge_in[0], near, far)

    @pl.when(is_end)
    def _():
        edge_return.wait_recv()
        edge_mine[...] = jnp.where(edge_by == 0, edge_first[...], edge_back[...])

    edge_swap.start()
    for m in range(messages - 2, messages):
        settle(m)

    edge_swap.wait_recv()
    edge_final[0:8, :] = jnp.where(by_line(flips) == 1, edge_other[...], edge_mine[...])
    for tile_row in range(tile_rows):
        for block in range(tile // LANES):
            turned = edge_final[:, block * LANES : (block + 1) * LANES].T
            where = pl.ds(tile_row * tile + block * LANES, LANES)
            edge_wide[where, 0:LANES] = pltpu.roll(turned, (-4 * tile_row) % LANES, 1)
            edge_wide[where, cols - LANES : cols] = pltpu.roll(
                turned, (LANES - 2 - 4 * tile_row - 2) % LANES, 1
            )

    column = lax.broadcasted_iota(jnp.int32, (MESSAGE, cols), 1)
    inside = (column >= 2) & (column < cols - 2)

    @pl.loop(0, messages)
    def _(m):
        swap(m).wait_recv()
        where = span(m)
        taken = of_row(flips, m, (MESSAGE, cols)) == 1
        value = jnp.where(taken, other[where, :], mine[where, :])
        out_depth[where, :] = jnp.where(inside, value, edge_wide[where, :])

    @pl.when((lead_left == 1) | (follow_left == 1))
    def _():
        halo_to_left.wait_send()

    @pl.when((lead_right == 1) | (follow_right == 1))
    def _():
        halo_to_right.wait_send()

    edge_raw(middle).wait_send()
    edge_swap.wait_send()

    @pl.loop(0, messages)
    def _(m):
        raw(m, middle).wait_send()
        swap(m).wait_send()

    @pl.when(is_middle)
    def _():
        edge_relay.wait_send()
        edge_return.wait_send()

        @pl.loop(0, messages)
        def _(m):
            relay(m).wait_send()
            give(m).wait_send()


def solution(mesh):
    axis = "gx"
    count = mesh.shape[axis]

    def body(fields, friction, wet_mask, owner_table):
        rows, cols = friction.shape
        padded = rows + 2 * PAD
        slots = rows // MESSAGE + 1
        f32 = jnp.float32
        whole = pltpu.VMEM((rows, cols), f32)
        small = pltpu.VMEM((8, cols), f32)
        scratch = [
            pltpu.VMEM((3, padded, cols), f32),
            pltpu.VMEM((padded, cols), f32),
            pltpu.VMEM((padded, cols), jnp.int32),
            pltpu.SMEM(owner_table.shape, jnp.int32),
            whole,
            pltpu.VMEM((3, rows, cols), f32),
            whole,
            whole,
            whole,
            whole,
            pltpu.VMEM((32, rows), f32),
            pltpu.VMEM((8, rows), f32),
            pltpu.VMEM((8, rows), f32),
            pltpu.VMEM((4, 16, rows), f32),
            pltpu.VMEM((LANES, rows), f32),
            small,
            pltpu.VMEM((3, 8, cols), f32),
            small,
            small,
            small,
            small,
            pltpu.VMEM((LANES, cols), f32),
            whole,
            pltpu.SemaphoreType.DMA((6,)),
            pltpu.SemaphoreType.DMA((slots,)),
            pltpu.SemaphoreType.DMA((slots,)),
            pltpu.SemaphoreType.DMA((3, slots)),
            pltpu.SemaphoreType.DMA((slots,)),
            pltpu.SemaphoreType.DMA((slots,)),
            pltpu.SemaphoreType.DMA((slots,)),
            pltpu.SemaphoreType.DMA((slots,)),
            pltpu.SemaphoreType.DMA((2,)),
            pltpu.SemaphoreType.DMA((2,)),
        ]
        arrays = [
            pltpu.with_memory_space_constraint(array, pltpu.HBM)
            for array in (fields, friction, wet_mask, owner_table)
        ]
        return pl.pallas_call(
            functools.partial(kernel, axis, count),
            out_shape=(
                jax.ShapeDtypeStruct(fields.shape, f32),
                jax.ShapeDtypeStruct(friction.shape, f32),
            ),
            in_specs=[pl.BlockSpec(memory_space=pltpu.HBM)] * 4,
            out_specs=(
                pl.BlockSpec(memory_space=pltpu.VMEM),
                pl.BlockSpec(memory_space=pltpu.VMEM),
            ),
            scratch_shapes=scratch,
            compiler_params=pltpu.CompilerParams(
                collective_id=0, has_side_effects=True, vmem_limit_bytes=32 * 2**20
            ),
            name="shallow_water",
        )(*arrays)

    in_specs = (P(None, "groups", axis), P("groups", axis), P("groups", axis), P("groups", None))
    out_specs = (P(None, "groups", axis), P("groups", axis))
    return jax.shard_map(body, mesh=mesh, in_specs=in_specs, out_specs=out_specs, check_vma=False)
```

```python
import functools

import jax
import jax.numpy as jnp
from jax import lax
from jax.experimental import pallas as pl
from jax.experimental.pallas import tpu as pltpu
from jax.sharding import PartitionSpec as P

STEPS = 2
PAD = 8
CHUNK = 64
MESSAGE = 32
LAG = 4
BLOCKS = 4
LANES = 128

gravity_half = 0.5
depth_floor = 0.25
flux_factor = 0.1
time_step = 0.25


def advance(state, wet, damping, east, west, south, north):
    h, p, q = state
    inverse = 1.0 / jnp.maximum(h, depth_floor)
    u = p * inverse
    v = q * inverse
    pressure = gravity_half * h * h
    cross = q * u
    flux_p = p * u + pressure
    flux_q = q * v + pressure

    def gather(cell, flux_east, flux_south):
        quarter = 0.25 * cell
        along = flux_factor * flux_east
        down = flux_factor * flux_south
        return (east(quarter - along) + west(quarter + along)) + (
            south(quarter - down) + north(quarter + down)
        )

    return (
        wet * gather(h, p, q),
        damping * gather(p, flux_p, cross),
        damping * gather(q, cross, flux_q),
    )


def masks(openness):
    wet = jnp.where(openness > 0.0, 1.0, 0.0)
    return wet, wet / (1.0 + time_step * openness)


def kernel(
    axis,
    count,
    fields_ref,
    friction_ref,
    wet_ref,
    owner_ref,
    out_fields,
    out_depth,
    state,
    fric,
    mask,
    owner,
    first,
    inbox,
    back,
    turn,
    near_out,
    far_out,
    mine,
    other,
    packed,
    halo_left,
    halo_right,
    edge,
    edge_turn,
    edge_first,
    edge_in,
    edge_back,
    edge_give,
    edge_mine,
    edge_other,
    edge_final,
    edge_wide,
    load_sem,
    table_sem,
    raw_send,
    relay_send,
    in_recv,
    back_send,
    back_recv,
    swap_send,
    swap_recv,
    halo_send,
    halo_recv,
    hello,
):
    rows, cols = friction_ref.shape
    tile = cols
    tile_rows = rows // tile
    messages = rows // MESSAGE
    half = messages // 2
    chunks = rows // CHUNK
    extra = messages
    MESH = pl.DeviceIdType.MESH

    me = lax.axis_index(axis)
    odd = me % 2
    position = me % 8
    chip = position // 2
    middle = ((chip + 1) // 2) % 2
    toward = me + 2 - 4 * (chip // 2)
    outward = 2 * me - toward
    sibling = me + 1 - 2 * odd
    is_first = chip == 0
    is_third = chip == 2
    swapped = chip // 3
    is_middle = middle == 1
    is_end = middle == 0

    last = jnp.where(me == count - 1, 1, 0)
    lead_left = jnp.where(position == 0, 0, 1 - odd)
    follow_left = jnp.where(me == 0, 0, 1 - lead_left)
    lead_right = jnp.where(position == 7, 1, 1 - odd) * (1 - last)
    follow_right = (1 - last) * (1 - lead_right)

    height = rows // BLOCKS

    def load(number):
        block = lax.rem(number + swapped, BLOCKS)
        start = pl.multiple_of(block * height, height)
        here = pl.ds(start, height)
        there = pl.ds(start + PAD, height)
        copies = [
            pltpu.make_async_copy(
                fields_ref.at[plane, here, :],
                state.at[plane, there, :],
                load_sem.at[number, plane],
            )
            for plane in range(3)
        ]
        copies.append(
            pltpu.make_async_copy(friction_ref.at[here, :], fric.at[there, :], load_sem.at[number, 3])
        )
        copies.append(
            pltpu.make_async_copy(wet_ref.at[here, :], mask.at[there, :], load_sem.at[number, 4])
        )
        return copies

    def await_load(number):
        for copy in load(number):
            copy.wait()

    table = pltpu.make_async_copy(owner_ref, owner, table_sem)
    for number in range(BLOCKS):
        for copy in load(number):
            copy.start()
    table.start()

    barrier = pltpu.get_barrier_semaphore()

    def greet(peer):
        pl.semaphore_signal(barrier, inc=1, device_id={axis: peer}, device_id_type=MESH)

    @pl.when(is_middle)
    def _():
        greet(outward)
        greet(toward)

    @pl.when(is_third)
    def _():
        greet(me - 4)

    @pl.when(follow_left == 1)
    def _():
        greet(me - 1)

    @pl.when(follow_right == 1)
    def _():
        greet(me + 1)

    zero_rows = jnp.zeros((PAD, cols), jnp.float32)
    for start in (0, PAD + rows):
        for plane in range(3):
            state[plane, start : start + PAD, :] = zero_rows
        fric[start : start + PAD, :] = zero_rows
        mask[start : start + PAD, :] = jnp.zeros((PAD, cols), jnp.int32)
    edge[...] = jnp.zeros_like(edge)
    edge_turn[...] = jnp.zeros_like(edge_turn)
    edge_final[...] = jnp.zeros_like(edge_final)

    def differs(tile_row, bit):
        own = owner[tile_row, me]
        return (own // 2 ** bit + me // 2 ** bit) % 2

    def remote(src, dst, send, recv, peer):
        return pltpu.make_async_remote_copy(
            src_ref=src,
            dst_ref=dst,
            send_sem=send,
            recv_sem=recv,
            device_id={axis: peer},
            device_id_type=MESH,
        )

    def span(m):
        return pl.ds(pl.multiple_of(m * MESSAGE, MESSAGE), MESSAGE)

    def raw(m, slot):
        return remote(
            first.at[span(m), :], inbox.at[slot, span(m), :], raw_send.at[m], in_recv.at[slot, m], toward
        )

    def relay(m):
        return remote(
            inbox.at[0, span(m), :], inbox.at[2, span(m), :], relay_send.at[m], in_recv.at[2, m], toward
        )

    def give(m):
        return remote(turn.at[span(m), :], back.at[span(m), :], back_send.at[m], back_recv.at[m], outward)

    def give_raw(m):
        return remote(
            first.at[span(m), :], back.at[span(m), :], back_send.at[m], back_recv.at[m], outward
        )

    def near_direct(m):
        return remote(
            near_out.at[span(m), :], inbox.at[1, span(m), :], raw_send.at[m], in_recv.at[1, m], me - 2
        )

    def far_direct(m):
        return remote(
            far_out.at[span(m), :], inbox.at[2, span(m), :], relay_send.at[m], in_recv.at[2, m], me - 4
        )

    def swap(m):
        return remote(mine.at[span(m), :], other.at[span(m), :], swap_send.at[m], swap_recv.at[m], sibling)

    def edge_raw(slot):
        return remote(edge_first, edge_in.at[slot], raw_send.at[extra], in_recv.at[slot, extra], toward)

    edge_relay = remote(
        edge_in.at[0], edge_in.at[2], relay_send.at[extra], in_recv.at[2, extra], toward
    )
    edge_return = remote(edge_give, edge_back, back_send.at[extra], back_recv.at[extra], outward)
    edge_swap = remote(edge_mine, edge_other, swap_send.at[extra], swap_recv.at[extra], sibling)

    halo_to_left = remote(
        packed.at[pl.ds(0, 8), :], halo_right, halo_send.at[0], halo_recv.at[0], me - 1
    )
    halo_to_right = remote(
        packed.at[pl.ds(8, 8), :], halo_left, halo_send.at[1], halo_recv.at[1], me + 1
    )

    def shift(axis_number, amount, size):
        return lambda a: pltpu.roll(a, amount % size, axis_number)

    def compute(i):
        reach = CHUNK + 2 * PAD
        at = pl.multiple_of(i * CHUNK, CHUNK)
        where = pl.ds(at, reach)
        openness = mask[where, :].astype(jnp.float32) * fric[where, :]
        wet, damping = masks(openness)
        values = tuple(state[plane, where, :] * wet for plane in range(3))
        for _ in range(STEPS):
            values = advance(
                values,
                wet,
                damping,
                shift(1, -1, cols),
                shift(1, 1, cols),
                shift(0, -1, reach),
                shift(0, 1, reach),
            )
        here = pl.ds(at, CHUNK)
        first[here, :] = values[0][PAD : PAD + CHUNK]
        for plane in range(3):
            out_fields[plane, here, :] = values[plane][PAD : PAD + CHUNK]

    def for_end(by, own, near, far):
        return jnp.where(by == 3, far, jnp.where(by == 2, near, own))

    def for_middle(by, own, end, near, far):
        return jnp.where(by == 3, near, jnp.where(by == 2, far, jnp.where(by == 1, end, own)))

    def of_row(pair, m, shape):
        value = pair[-1]
        for tile_row in reversed(range(tile_rows - 1)):
            value = jnp.where(m < (tile_row + 1) * (tile // MESSAGE), pair[tile_row], value)
        return jnp.full(shape, value, jnp.int32)

    def send_chunk(number):
        for part in range(CHUNK // MESSAGE):
            raw(number * (CHUNK // MESSAGE) + part, middle).start()

    def chunk_at(j):
        return lax.rem(j + swapped * (chunks // 2), chunks)

    await_load(0)

    @pl.when(swapped == 1)
    def _():
        await_load(1)

    compute(chunk_at(0))
    pl.semaphore_wait(barrier, 1 + lead_left + lead_right + jnp.where(is_first, 1, 0))
    send_chunk(chunk_at(0))

    @pl.when(is_first)
    def _():
        for peer in (me + 2, me + 4):
            pl.semaphore_signal(hello, inc=1, device_id={axis: peer}, device_id_type=MESH)

    @pl.when(swapped == 0)
    def _():
        await_load(1)

    for number in range(2, BLOCKS):
        await_load(number)
    table.wait()
    moves = [differs(tile_row, 1) + 2 * differs(tile_row, 2) for tile_row in range(tile_rows)]
    flips = [differs(tile_row, 0) for tile_row in range(tile_rows)]

    lane = lax.broadcasted_iota(jnp.int32, (LANES, LANES), 1)

    @pl.loop(0, rows // LANES)
    def _(block):
        where = pl.ds(pl.multiple_of(PAD + block * LANES, PAD), LANES)
        result = jnp.zeros((LANES, LANES), jnp.float32)
        for side, low in enumerate((0, cols - LANES)):
            cut = pl.ds(low, LANES)
            openness = mask[where, cut].astype(jnp.float32) * fric[where, cut]
            wet, _ = masks(openness)
            planes = [state[plane, where, cut] * wet for plane in range(3)] + [openness]
            for number, values in enumerate(planes):
                for inner in range(2):
                    source = LANES - 2 - 2 * inner if side else 2 * inner
                    target = 16 * inner + 8 * side + 2 * number
                    moved = pltpu.roll(values, (target - source) % LANES, 1)
                    result = jnp.where((lane >= target) & (lane < target + 2), moved, result)
        packed[:, pl.ds(pl.multiple_of(block * LANES, LANES), LANES)] = result.T[0:32]

    @pl.when(lead_left == 1)
    def _():
        halo_to_left.start()

    @pl.when(lead_right == 1)
    def _():
        halo_to_right.start()

    @pl.loop(1, chunks)
    def _(j):
        compute(chunk_at(j))

        @pl.when((chip != 2) | (j < chunks // 2))
        def _():
            send_chunk(chunk_at(j))

    @pl.when(follow_right == 1)
    def _():
        halo_to_left.wait_recv()
        halo_to_right.start()

    @pl.when(follow_left == 1)
    def _():
        halo_to_right.wait_recv()
        halo_to_left.start()

    @pl.when(is_third)
    def _():
        @pl.loop(half, messages)
        def _(m):
            raw(m, 0).wait_recv()
            where = span(m)
            by = of_row(moves, m, (MESSAGE, cols))
            near_out[where, :] = jnp.where(by == 3, first[where, :], inbox[0, where, :])
            near_direct(m).start()

    @pl.when(chip == 1)
    def _():
        pl.semaphore_wait(hello, 1)

        @pl.loop(half, messages)
        def _(m):
            give_raw(m).start()

    @pl.when(lead_right == 1)
    def _():
        halo_to_left.wait_recv()

    @pl.when(lead_left == 1)
    def _():
        halo_to_right.wait_recv()

    for number in range(4):
        pair = pl.ds(2 * number, 2)
        edge[number, 0:2, :] = jnp.where(me > 0, halo_left[pair, :], 0.0)
        edge[number, 2:4, :] = packed[pl.ds(2 * number, 2), :]
        edge[number, 4:6, :] = packed[pl.ds(16 + 2 * number, 2), :]
        edge[number, 8:10, :] = packed[pl.ds(24 + 2 * number, 2), :]
        edge[number, 10:12, :] = packed[pl.ds(8 + 2 * number, 2), :]
        edge[number, 12:14, :] = jnp.where(me < count - 1, halo_right[pair, :], 0.0)

    place = lax.broadcasted_iota(jnp.int32, (16, rows), 1)
    wet, damping = masks(edge[3])
    values = tuple(edge[plane] for plane in range(3))
    for _ in range(STEPS):
        values = advance(
            values,
            wet,
            damping,
            shift(0, -1, 16),
            shift(0, 1, 16),
            lambda a: jnp.where(place == rows - 1, 0.0, pltpu.roll(a, rows - 1, 1)),
            lambda a: jnp.where(place == 0, 0.0, pltpu.roll(a, 1, 1)),
        )
    for plane in range(3):
        edge_turn[16 * plane : 16 * plane + 16, :] = values[plane]
    for tile_row in range(tile_rows):
        cut = pl.ds(tile_row * tile, tile)
        edge_first[4 * tile_row : 4 * tile_row + 2, :] = edge_turn[2:4, cut]
        edge_first[4 * tile_row + 2 : 4 * tile_row + 4, :] = edge_turn[10:12, cut]
    edge_raw(middle).start()

    def settle_second(m, late):
        where = span(m)
        by = of_row(moves, m, (MESSAGE, cols))
        raw(m, 1).wait_recv()
        own = first[where, :]
        end = inbox[0, where, :]
        near = inbox[1, where, :]
        if late:
            mine[where, :] = jnp.where(by >= 2, near, jnp.where(by == 1, end, own))
        else:
            relay(m).wait_recv()
            far = inbox[2, where, :]
            turn[where, :] = for_end(by, own, near, far)
            give(m).start()
            mine[where, :] = for_middle(by, own, end, near, far)
        swap(m).start()

    def pass_on(m):
        raw(m, 0).wait_recv()
        relay(m).start()

    @pl.when(is_third)
    def _():
        @pl.loop(0, half)
        def _(m):
            pass_on(m)

        edge_raw(0).wait_recv()
        edge_relay.start()
        pl.semaphore_wait(hello, 1)

        @pl.loop(half, messages)
        def _(m):
            where = span(m)
            by = of_row(moves, m, (MESSAGE, cols))
            far_out[where, :] = jnp.where(by == 2, first[where, :], inbox[0, where, :])
            far_direct(m).start()

    @pl.when(chip == 1)
    def _():
        for m in range(LAG):
            pass_on(m)

        @pl.loop(0, half)
        def _(m):
            settle_second(m, False)
            pass_on(m + LAG)

        for m in range(half + LAG, messages):
            pass_on(m)
        edge_raw(0).wait_recv()
        edge_relay.start()

    @pl.loop(0, rows // LANES)
    def _(block):
        where = pl.ds(pl.multiple_of(block * LANES, LANES), LANES)
        turned = edge_turn[:, where].T
        for plane in range(3):
            on_left = pltpu.roll(turned, (-16 * plane - 2) % LANES, 1)
            cut = pl.ds(0, LANES)
            out_fields[plane, where, cut] = jnp.where(
                lane < 2, on_left, out_fields[plane, where, cut]
            )
            on_right = pltpu.roll(turned, (LANES - 2 - 16 * plane - 10) % LANES, 1)
            cut = pl.ds(cols - LANES, LANES)
            out_fields[plane, where, cut] = jnp.where(
                lane >= LANES - 2, on_right, out_fields[plane, where, cut]
            )

    def settle(m, late):
        where = span(m)
        by = of_row(moves, m, (MESSAGE, cols))

        @pl.when(is_third)
        def _():
            raw(m, 1).wait_recv()
            relay(m).wait_recv()
            own = first[where, :]
            near = inbox[1, where, :]
            far = inbox[2, where, :]
            turn[where, :] = for_end(by, own, near, far)
            give(m).start()
            mine[where, :] = for_middle(by, own, inbox[0, where, :], near, far)

        @pl.when(is_end)
        def _():
            give(m).wait_recv()

        @pl.when(is_first)
        def _():
            taken = back[where, :]
            if late:
                relay(m).wait_recv()
                taken = jnp.where(by >= 2, inbox[2, where, :], taken)
            mine[where, :] = jnp.where(by == 0, first[where, :], taken)

        @pl.when(chip == 3)
        def _():
            mine[where, :] = jnp.where(by == 0, first[where, :], back[where, :])

        swap(m).start()

    line = lax.broadcasted_iota(jnp.int32, (8, cols), 0)

    def by_line(pair):
        value = jnp.full((8, cols), pair[-1], jnp.int32)
        for tile_row in reversed(range(tile_rows - 1)):
            value = jnp.where(line < 4 * (tile_row + 1), pair[tile_row], value)
        return value

    @pl.when(chip != 1)
    def _():
        @pl.loop(0, half)
        def _(m):
            settle(m, False)

    edge_by = by_line(moves)

    @pl.when(is_middle)
    def _():
        edge_raw(1).wait_recv()
        edge_relay.wait_recv()
        own = edge_first[...]
        near = edge_in[1]
        far = edge_in[2]
        edge_give[...] = for_end(edge_by, own, near, far)
        edge_return.start()
        edge_mine[...] = for_middle(edge_by, own, edge_in[0], near, far)

    @pl.when(is_end)
    def _():
        edge_return.wait_recv()
        edge_mine[...] = jnp.where(edge_by == 0, edge_first[...], edge_back[...])

    edge_swap.start()

    @pl.when(chip != 1)
    def _():
        @pl.loop(half, messages)
        def _(m):
            settle(m, True)

    @pl.when(chip == 1)
    def _():
        @pl.loop(half, messages)
        def _(m):
            settle_second(m, True)

    edge_swap.wait_recv()
    edge_final[0:8, :] = jnp.where(by_line(flips) == 1, edge_other[...], edge_mine[...])
    for tile_row in range(tile_rows):
        for block in range(tile // LANES):
            turned = edge_final[:, block * LANES : (block + 1) * LANES].T
            where = pl.ds(tile_row * tile + block * LANES, LANES)
            edge_wide[where, 0:LANES] = pltpu.roll(turned, (-4 * tile_row) % LANES, 1)
            edge_wide[where, cols - LANES : cols] = pltpu.roll(
                turned, (LANES - 2 - 4 * tile_row - 2) % LANES, 1
            )

    column = lax.broadcasted_iota(jnp.int32, (MESSAGE, cols), 1)
    inside = (column >= 2) & (column < cols - 2)

    @pl.loop(0, messages)
    def _(m):
        swap(m).wait_recv()
        where = span(m)
        taken = of_row(flips, m, (MESSAGE, cols)) == 1
        value = jnp.where(taken, other[where, :], mine[where, :])
        out_depth[where, :] = jnp.where(inside, value, edge_wide[where, :])

    @pl.when((lead_left == 1) | (follow_left == 1))
    def _():
        halo_to_left.wait_send()

    @pl.when((lead_right == 1) | (follow_right == 1))
    def _():
        halo_to_right.wait_send()

    edge_raw(middle).wait_send()
    edge_swap.wait_send()

    @pl.loop(0, messages)
    def _(m):
        raw(m, middle).wait_send()
        swap(m).wait_send()

    @pl.when(is_middle)
    def _():
        edge_relay.wait_send()
        edge_return.wait_send()

        @pl.loop(0, messages)
        def _(m):
            relay(m).wait_send()
            give(m).wait_send()


def solution(mesh):
    axis = "gx"
    count = mesh.shape[axis]

    def body(fields, friction, wet_mask, owner_table):
        rows, cols = friction.shape
        padded = rows + 2 * PAD
        slots = rows // MESSAGE + 1
        f32 = jnp.float32
        whole = pltpu.VMEM((rows, cols), f32)
        small = pltpu.VMEM((8, cols), f32)
        scratch = [
            pltpu.VMEM((3, padded, cols), f32),
            pltpu.VMEM((padded, cols), f32),
            pltpu.VMEM((padded, cols), jnp.int32),
            pltpu.SMEM(owner_table.shape, jnp.int32),
            whole,
            pltpu.VMEM((3, rows, cols), f32),
            whole,
            whole,
            whole,
            whole,
            whole,
            whole,
            pltpu.VMEM((32, rows), f32),
            pltpu.VMEM((8, rows), f32),
            pltpu.VMEM((8, rows), f32),
            pltpu.VMEM((4, 16, rows), f32),
            pltpu.VMEM((LANES, rows), f32),
            small,
            pltpu.VMEM((3, 8, cols), f32),
            small,
            small,
            small,
            small,
            pltpu.VMEM((LANES, cols), f32),
            whole,
            pltpu.SemaphoreType.DMA((BLOCKS, 5)),
            pltpu.SemaphoreType.DMA,
            pltpu.SemaphoreType.DMA((slots,)),
            pltpu.SemaphoreType.DMA((slots,)),
            pltpu.SemaphoreType.DMA((3, slots)),
            pltpu.SemaphoreType.DMA((slots,)),
            pltpu.SemaphoreType.DMA((slots,)),
            pltpu.SemaphoreType.DMA((slots,)),
            pltpu.SemaphoreType.DMA((slots,)),
            pltpu.SemaphoreType.DMA((2,)),
            pltpu.SemaphoreType.DMA((2,)),
            pltpu.SemaphoreType.REGULAR,
        ]
        arrays = [
            pltpu.with_memory_space_constraint(array, pltpu.HBM)
            for array in (fields, friction, wet_mask, owner_table)
        ]
        return pl.pallas_call(
            functools.partial(kernel, axis, count),
            out_shape=(
                jax.ShapeDtypeStruct(fields.shape, f32),
                jax.ShapeDtypeStruct(friction.shape, f32),
            ),
            in_specs=[pl.BlockSpec(memory_space=pltpu.HBM)] * 4,
            out_specs=(
                pl.BlockSpec(memory_space=pltpu.VMEM),
                pl.BlockSpec(memory_space=pltpu.VMEM),
            ),
            scratch_shapes=scratch,
            compiler_params=pltpu.CompilerParams(
                collective_id=0, has_side_effects=True, vmem_limit_bytes=32 * 2**20
            ),
            name="shallow_water",
        )(*arrays)

    in_specs = (P(None, "groups", axis), P("groups", axis), P("groups", axis), P("groups", None))
    out_specs = (P(None, "groups", axis), P("groups", axis))
    return jax.shard_map(body, mesh=mesh, in_specs=in_specs, out_specs=out_specs, check_vma=False)
```

```python
import functools

import jax
import jax.numpy as jnp
from jax import lax
from jax.experimental import pallas as pl
from jax.experimental.pallas import tpu as pltpu
from jax.sharding import PartitionSpec as P

STEPS = 2
PAD = 8
CHUNK = 64
MESSAGE = 32
LAG = 4
BLOCKS = 4
LANES = 128

gravity_half = 0.5
depth_floor = 0.25
flux_factor = 0.1
time_step = 0.25


def advance(state, wet, damping, east, west, south, north):
    h, p, q = state
    inverse = 1.0 / jnp.maximum(h, depth_floor)
    u = p * inverse
    v = q * inverse
    pressure = gravity_half * h * h
    cross = q * u
    flux_p = p * u + pressure
    flux_q = q * v + pressure

    def gather(cell, flux_east, flux_south):
        quarter = 0.25 * cell
        along = flux_factor * flux_east
        down = flux_factor * flux_south
        return (east(quarter - along) + west(quarter + along)) + (
            south(quarter - down) + north(quarter + down)
        )

    return (
        wet * gather(h, p, q),
        damping * gather(p, flux_p, cross),
        damping * gather(q, cross, flux_q),
    )


def masks(openness):
    wet = jnp.where(openness > 0.0, 1.0, 0.0)
    return wet, wet / (1.0 + time_step * openness)


def kernel(
    axis,
    count,
    fields_ref,
    friction_ref,
    wet_ref,
    owner_ref,
    out_fields,
    out_depth,
    state,
    fric,
    mask,
    owner,
    first,
    inbox,
    back,
    turn,
    near_out,
    far_out,
    mine,
    other,
    packed,
    halo_left,
    halo_right,
    edge,
    edge_turn,
    edge_first,
    edge_in,
    edge_back,
    edge_give,
    edge_mine,
    edge_other,
    edge_final,
    edge_wide,
    load_sem,
    table_sem,
    raw_send,
    relay_send,
    in_recv,
    back_send,
    back_recv,
    swap_send,
    swap_recv,
    halo_send,
    halo_recv,
    hello,
):
    rows, cols = friction_ref.shape
    tile = cols
    tile_rows = rows // tile
    messages = rows // MESSAGE
    half = messages // 2
    chunks = rows // CHUNK
    extra = messages
    MESH = pl.DeviceIdType.MESH

    me = lax.axis_index(axis)
    odd = me % 2
    position = me % 8
    chip = position // 2
    middle = ((chip + 1) // 2) % 2
    toward = me + 2 - 4 * (chip // 2)
    outward = 2 * me - toward
    sibling = me + 1 - 2 * odd
    is_first = chip == 0
    is_third = chip == 2
    is_middle = middle == 1
    is_end = middle == 0

    last = jnp.where(me == count - 1, 1, 0)
    parity = (me // 8) % 2
    lead_left = jnp.where(position == 0, parity, jnp.where(position == 6, 1, 0))
    lead_left = jnp.where(me == 0, 0, lead_left)
    follow_left = jnp.where(me == 0, 0, 1 - lead_left)
    lead_right = jnp.where(position == 7, parity, jnp.where(position == 5, 0, 1)) * (1 - last)
    follow_right = (1 - last) * (1 - lead_right)

    height = rows // BLOCKS

    def load(number):
        here = pl.ds(number * height, height)
        there = pl.ds(number * height + PAD, height)
        copies = [
            pltpu.make_async_copy(
                fields_ref.at[plane, here, :],
                state.at[plane, there, :],
                load_sem.at[number, plane],
            )
            for plane in range(3)
        ]
        copies.append(
            pltpu.make_async_copy(friction_ref.at[here, :], fric.at[there, :], load_sem.at[number, 3])
        )
        copies.append(
            pltpu.make_async_copy(wet_ref.at[here, :], mask.at[there, :], load_sem.at[number, 4])
        )
        return copies

    def await_load(number):
        for copy in load(number):
            copy.wait()

    table = pltpu.make_async_copy(owner_ref, owner, table_sem)
    for number in range(BLOCKS):
        for copy in load(number):
            copy.start()
    table.start()

    barrier = pltpu.get_barrier_semaphore()

    def greet(peer):
        pl.semaphore_signal(barrier, inc=1, device_id={axis: peer}, device_id_type=MESH)

    @pl.when(is_middle)
    def _():
        greet(outward)
        greet(toward)

    @pl.when(is_third)
    def _():
        greet(me - 4)

    @pl.when(follow_left == 1)
    def _():
        greet(me - 1)

    @pl.when(follow_right == 1)
    def _():
        greet(me + 1)

    zero_rows = jnp.zeros((PAD, cols), jnp.float32)
    for start in (0, PAD + rows):
        for plane in range(3):
            state[plane, start : start + PAD, :] = zero_rows
        fric[start : start + PAD, :] = zero_rows
        mask[start : start + PAD, :] = jnp.zeros((PAD, cols), jnp.int32)
    edge[...] = jnp.zeros_like(edge)
    edge_turn[...] = jnp.zeros_like(edge_turn)
    edge_final[...] = jnp.zeros_like(edge_final)

    def differs(tile_row, bit):
        own = owner[tile_row, me]
        return (own // 2 ** bit + me // 2 ** bit) % 2

    def remote(src, dst, send, recv, peer):
        return pltpu.make_async_remote_copy(
            src_ref=src,
            dst_ref=dst,
            send_sem=send,
            recv_sem=recv,
            device_id={axis: peer},
            device_id_type=MESH,
        )

    def span(m):
        return pl.ds(pl.multiple_of(m * MESSAGE, MESSAGE), MESSAGE)

    def raw(m, slot):
        return remote(
            first.at[span(m), :], inbox.at[slot, span(m), :], raw_send.at[m], in_recv.at[slot, m], toward
        )

    def relay(m):
        return remote(
            inbox.at[0, span(m), :], inbox.at[2, span(m), :], relay_send.at[m], in_recv.at[2, m], toward
        )

    def give(m):
        return remote(turn.at[span(m), :], back.at[span(m), :], back_send.at[m], back_recv.at[m], outward)

    def give_raw(m):
        return remote(
            first.at[span(m), :], back.at[span(m), :], back_send.at[m], back_recv.at[m], outward
        )

    def near_direct(m):
        return remote(
            near_out.at[span(m), :], inbox.at[1, span(m), :], raw_send.at[m], in_recv.at[1, m], me - 2
        )

    def far_direct(m):
        return remote(
            far_out.at[span(m), :], inbox.at[2, span(m), :], relay_send.at[m], in_recv.at[2, m], me - 4
        )

    def swap(m):
        return remote(mine.at[span(m), :], other.at[span(m), :], swap_send.at[m], swap_recv.at[m], sibling)

    def edge_raw(slot):
        return remote(edge_first, edge_in.at[slot], raw_send.at[extra], in_recv.at[slot, extra], toward)

    edge_relay = remote(
        edge_in.at[0], edge_in.at[2], relay_send.at[extra], in_recv.at[2, extra], toward
    )
    edge_return = remote(edge_give, edge_back, back_send.at[extra], back_recv.at[extra], outward)
    edge_swap = remote(edge_mine, edge_other, swap_send.at[extra], swap_recv.at[extra], sibling)

    halo_to_left = remote(
        packed.at[pl.ds(0, 8), :], halo_right, halo_send.at[0], halo_recv.at[0], me - 1
    )
    halo_to_right = remote(
        packed.at[pl.ds(8, 8), :], halo_left, halo_send.at[1], halo_recv.at[1], me + 1
    )

    def shift(axis_number, amount, size):
        return lambda a: pltpu.roll(a, amount % size, axis_number)

    def compute(i):
        reach = CHUNK + 2 * PAD
        at = pl.multiple_of(i * CHUNK, CHUNK)
        where = pl.ds(at, reach)
        openness = mask[where, :].astype(jnp.float32) * fric[where, :]
        wet, damping = masks(openness)
        values = tuple(state[plane, where, :] * wet for plane in range(3))
        for _ in range(STEPS):
            values = advance(
                values,
                wet,
                damping,
                shift(1, -1, cols),
                shift(1, 1, cols),
                shift(0, -1, reach),
                shift(0, 1, reach),
            )
        here = pl.ds(at, CHUNK)
        first[here, :] = values[0][PAD : PAD + CHUNK]
        for plane in range(3):
            out_fields[plane, here, :] = values[plane][PAD : PAD + CHUNK]

    def for_end(by, own, near, far):
        return jnp.where(by == 3, far, jnp.where(by == 2, near, own))

    def for_middle(by, own, end, near, far):
        return jnp.where(by == 3, near, jnp.where(by == 2, far, jnp.where(by == 1, end, own)))

    def of_row(pair, m, shape):
        value = pair[-1]
        for tile_row in reversed(range(tile_rows - 1)):
            value = jnp.where(m < (tile_row + 1) * (tile // MESSAGE), pair[tile_row], value)
        return jnp.full(shape, value, jnp.int32)

    def send_chunk(number):
        for part in range(CHUNK // MESSAGE):
            raw(number * (CHUNK // MESSAGE) + part, middle).start()

    await_load(0)
    compute(0)
    pl.semaphore_wait(barrier, 1 + lead_left + lead_right + jnp.where(is_first, 1, 0))
    send_chunk(0)

    @pl.when(is_first)
    def _():
        for peer in (me + 2, me + 4):
            pl.semaphore_signal(hello, inc=1, device_id={axis: peer}, device_id_type=MESH)

    for number in range(1, BLOCKS):
        await_load(number)
    table.wait()
    moves = [differs(tile_row, 1) + 2 * differs(tile_row, 2) for tile_row in range(tile_rows)]
    flips = [differs(tile_row, 0) for tile_row in range(tile_rows)]

    lane = lax.broadcasted_iota(jnp.int32, (LANES, LANES), 1)

    @pl.loop(0, rows // LANES)
    def _(block):
        where = pl.ds(pl.multiple_of(PAD + block * LANES, PAD), LANES)
        result = jnp.zeros((LANES, LANES), jnp.float32)
        for side, low in enumerate((0, cols - LANES)):
            cut = pl.ds(low, LANES)
            openness = mask[where, cut].astype(jnp.float32) * fric[where, cut]
            wet, _ = masks(openness)
            planes = [state[plane, where, cut] * wet for plane in range(3)] + [openness]
            for number, values in enumerate(planes):
                for inner in range(2):
                    source = LANES - 2 - 2 * inner if side else 2 * inner
                    target = 16 * inner + 8 * side + 2 * number
                    moved = pltpu.roll(values, (target - source) % LANES, 1)
                    result = jnp.where((lane >= target) & (lane < target + 2), moved, result)
        packed[:, pl.ds(pl.multiple_of(block * LANES, LANES), LANES)] = result.T[0:32]

    @pl.when(lead_left == 1)
    def _():
        halo_to_left.start()

    @pl.when(lead_right == 1)
    def _():
        halo_to_right.start()

    @pl.loop(1, chunks)
    def _(j):
        compute(j)

        @pl.when((chip != 2) | (j < chunks // 2))
        def _():
            send_chunk(j)

    @pl.when(follow_right == 1)
    def _():
        halo_to_left.wait_recv()
        halo_to_right.start()

    @pl.when(follow_left == 1)
    def _():
        halo_to_right.wait_recv()
        halo_to_left.start()

    def pass_on(m):
        raw(m, 0).wait_recv()
        relay(m).start()

    @pl.when(is_third)
    def _():
        @pl.loop(0, half)
        def _(m):
            pass_on(m)

        @pl.loop(half, messages)
        def _(m):
            raw(m, 0).wait_recv()
            where = span(m)
            by = of_row(moves, m, (MESSAGE, cols))
            near_out[where, :] = jnp.where(by == 3, first[where, :], inbox[0, where, :])
            near_direct(m).start()

    @pl.when(chip == 1)
    def _():
        pl.semaphore_wait(hello, 1)

        @pl.loop(half, messages)
        def _(m):
            give_raw(m).start()

    @pl.when(lead_right == 1)
    def _():
        halo_to_left.wait_recv()

    @pl.when(lead_left == 1)
    def _():
        halo_to_right.wait_recv()

    for number in range(4):
        pair = pl.ds(2 * number, 2)
        edge[number, 0:2, :] = jnp.where(me > 0, halo_left[pair, :], 0.0)
        edge[number, 2:4, :] = packed[pl.ds(2 * number, 2), :]
        edge[number, 4:6, :] = packed[pl.ds(16 + 2 * number, 2), :]
        edge[number, 8:10, :] = packed[pl.ds(24 + 2 * number, 2), :]
        edge[number, 10:12, :] = packed[pl.ds(8 + 2 * number, 2), :]
        edge[number, 12:14, :] = jnp.where(me < count - 1, halo_right[pair, :], 0.0)

    place = lax.broadcasted_iota(jnp.int32, (16, rows), 1)
    wet, damping = masks(edge[3])
    values = tuple(edge[plane] for plane in range(3))
    for _ in range(STEPS):
        values = advance(
            values,
            wet,
            damping,
            shift(0, -1, 16),
            shift(0, 1, 16),
            lambda a: jnp.where(place == rows - 1, 0.0, pltpu.roll(a, rows - 1, 1)),
            lambda a: jnp.where(place == 0, 0.0, pltpu.roll(a, 1, 1)),
        )
    for plane in range(3):
        edge_turn[16 * plane : 16 * plane + 16, :] = values[plane]
    for tile_row in range(tile_rows):
        cut = pl.ds(tile_row * tile, tile)
        edge_first[4 * tile_row : 4 * tile_row + 2, :] = edge_turn[2:4, cut]
        edge_first[4 * tile_row + 2 : 4 * tile_row + 4, :] = edge_turn[10:12, cut]
    edge_raw(middle).start()

    def settle_second(m, late):
        where = span(m)
        by = of_row(moves, m, (MESSAGE, cols))
        raw(m, 1).wait_recv()
        own = first[where, :]
        end = inbox[0, where, :]
        near = inbox[1, where, :]
        if late:
            mine[where, :] = jnp.where(by >= 2, near, jnp.where(by == 1, end, own))
        else:
            relay(m).wait_recv()
            far = inbox[2, where, :]
            turn[where, :] = for_end(by, own, near, far)
            give(m).start()
            mine[where, :] = for_middle(by, own, end, near, far)
        swap(m).start()

    @pl.when(is_third)
    def _():
        edge_raw(0).wait_recv()
        edge_relay.start()
        pl.semaphore_wait(hello, 1)

        @pl.loop(half, messages)
        def _(m):
            where = span(m)
            by = of_row(moves, m, (MESSAGE, cols))
            far_out[where, :] = jnp.where(by == 2, first[where, :], inbox[0, where, :])
            far_direct(m).start()

    @pl.when(chip == 1)
    def _():
        for m in range(LAG):
            pass_on(m)

        @pl.loop(0, half)
        def _(m):
            settle_second(m, False)
            pass_on(m + LAG)

        for m in range(half + LAG, messages):
            pass_on(m)
        edge_raw(0).wait_recv()
        edge_relay.start()

    @pl.loop(0, rows // LANES)
    def _(block):
        where = pl.ds(pl.multiple_of(block * LANES, LANES), LANES)
        turned = edge_turn[:, where].T
        for plane in range(3):
            on_left = pltpu.roll(turned, (-16 * plane - 2) % LANES, 1)
            cut = pl.ds(0, LANES)
            out_fields[plane, where, cut] = jnp.where(
                lane < 2, on_left, out_fields[plane, where, cut]
            )
            on_right = pltpu.roll(turned, (LANES - 2 - 16 * plane - 10) % LANES, 1)
            cut = pl.ds(cols - LANES, LANES)
            out_fields[plane, where, cut] = jnp.where(
                lane >= LANES - 2, on_right, out_fields[plane, where, cut]
            )

    def settle(m, late):
        where = span(m)
        by = of_row(moves, m, (MESSAGE, cols))

        @pl.when(is_third)
        def _():
            raw(m, 1).wait_recv()
            relay(m).wait_recv()
            own = first[where, :]
            near = inbox[1, where, :]
            far = inbox[2, where, :]
            turn[where, :] = for_end(by, own, near, far)
            give(m).start()
            mine[where, :] = for_middle(by, own, inbox[0, where, :], near, far)

        @pl.when(is_end)
        def _():
            give(m).wait_recv()

        @pl.when(is_first)
        def _():
            taken = back[where, :]
            if late:
                relay(m).wait_recv()
                taken = jnp.where(by >= 2, inbox[2, where, :], taken)
            mine[where, :] = jnp.where(by == 0, first[where, :], taken)

        @pl.when(chip == 3)
        def _():
            mine[where, :] = jnp.where(by == 0, first[where, :], back[where, :])

        swap(m).start()

    line = lax.broadcasted_iota(jnp.int32, (8, cols), 0)

    def by_line(pair):
        value = jnp.full((8, cols), pair[-1], jnp.int32)
        for tile_row in reversed(range(tile_rows - 1)):
            value = jnp.where(line < 4 * (tile_row + 1), pair[tile_row], value)
        return value

    @pl.when(chip != 1)
    def _():
        @pl.loop(0, half)
        def _(m):
            settle(m, False)

    edge_by = by_line(moves)

    def settle_edges():
        @pl.when(is_middle)
        def _():
            edge_raw(1).wait_recv()
            edge_relay.wait_recv()
            own = edge_first[...]
            near = edge_in[1]
            far = edge_in[2]
            edge_give[...] = for_end(edge_by, own, near, far)
            edge_return.start()
            edge_mine[...] = for_middle(edge_by, own, edge_in[0], near, far)

        @pl.when(is_end)
        def _():
            edge_return.wait_recv()
            edge_mine[...] = jnp.where(edge_by == 0, edge_first[...], edge_back[...])

        edge_swap.start()

    @pl.when(chip < 2)
    def _():
        settle_edges()

    @pl.when(chip != 1)
    def _():
        @pl.loop(half, messages)
        def _(m):
            settle(m, True)

    @pl.when(chip == 1)
    def _():
        @pl.loop(half, messages)
        def _(m):
            settle_second(m, True)

    @pl.when(chip >= 2)
    def _():
        settle_edges()

    edge_swap.wait_recv()
    edge_final[0:8, :] = jnp.where(by_line(flips) == 1, edge_other[...], edge_mine[...])
    for tile_row in range(tile_rows):
        for block in range(tile // LANES):
            turned = edge_final[:, block * LANES : (block + 1) * LANES].T
            where = pl.ds(tile_row * tile + block * LANES, LANES)
            edge_wide[where, 0:LANES] = pltpu.roll(turned, (-4 * tile_row) % LANES, 1)
            edge_wide[where, cols - LANES : cols] = pltpu.roll(
                turned, (LANES - 2 - 4 * tile_row - 2) % LANES, 1
            )

    column = lax.broadcasted_iota(jnp.int32, (MESSAGE, cols), 1)
    inside = (column >= 2) & (column < cols - 2)

    @pl.loop(0, messages)
    def _(m):
        swap(m).wait_recv()
        where = span(m)
        taken = of_row(flips, m, (MESSAGE, cols)) == 1
        value = jnp.where(taken, other[where, :], mine[where, :])
        out_depth[where, :] = jnp.where(inside, value, edge_wide[where, :])

    @pl.when((lead_left == 1) | (follow_left == 1))
    def _():
        halo_to_left.wait_send()

    @pl.when((lead_right == 1) | (follow_right == 1))
    def _():
        halo_to_right.wait_send()

    edge_raw(middle).wait_send()
    edge_swap.wait_send()

    @pl.loop(0, messages)
    def _(m):
        raw(m, middle).wait_send()
        swap(m).wait_send()

    @pl.when(is_middle)
    def _():
        edge_relay.wait_send()
        edge_return.wait_send()

        @pl.loop(0, messages)
        def _(m):
            relay(m).wait_send()
            give(m).wait_send()


def solution(mesh):
    axis = "gx"
    count = mesh.shape[axis]

    def body(fields, friction, wet_mask, owner_table):
        rows, cols = friction.shape
        padded = rows + 2 * PAD
        slots = rows // MESSAGE + 1
        f32 = jnp.float32
        whole = pltpu.VMEM((rows, cols), f32)
        small = pltpu.VMEM((8, cols), f32)
        scratch = [
            pltpu.VMEM((3, padded, cols), f32),
            pltpu.VMEM((padded, cols), f32),
            pltpu.VMEM((padded, cols), jnp.int32),
            pltpu.SMEM(owner_table.shape, jnp.int32),
            whole,
            pltpu.VMEM((3, rows, cols), f32),
            whole,
            whole,
            whole,
            whole,
            whole,
            whole,
            pltpu.VMEM((32, rows), f32),
            pltpu.VMEM((8, rows), f32),
            pltpu.VMEM((8, rows), f32),
            pltpu.VMEM((4, 16, rows), f32),
            pltpu.VMEM((LANES, rows), f32),
            small,
            pltpu.VMEM((3, 8, cols), f32),
            small,
            small,
            small,
            small,
            pltpu.VMEM((LANES, cols), f32),
            whole,
            pltpu.SemaphoreType.DMA((BLOCKS, 5)),
            pltpu.SemaphoreType.DMA,
            pltpu.SemaphoreType.DMA((slots,)),
            pltpu.SemaphoreType.DMA((slots,)),
            pltpu.SemaphoreType.DMA((3, slots)),
            pltpu.SemaphoreType.DMA((slots,)),
            pltpu.SemaphoreType.DMA((slots,)),
            pltpu.SemaphoreType.DMA((slots,)),
            pltpu.SemaphoreType.DMA((slots,)),
            pltpu.SemaphoreType.DMA((2,)),
            pltpu.SemaphoreType.DMA((2,)),
            pltpu.SemaphoreType.REGULAR,
        ]
        arrays = [
            pltpu.with_memory_space_constraint(array, pltpu.HBM)
            for array in (fields, friction, wet_mask, owner_table)
        ]
        return pl.pallas_call(
            functools.partial(kernel, axis, count),
            out_shape=(
                jax.ShapeDtypeStruct(fields.shape, f32),
                jax.ShapeDtypeStruct(friction.shape, f32),
            ),
            in_specs=[pl.BlockSpec(memory_space=pltpu.HBM)] * 4,
            out_specs=(
                pl.BlockSpec(memory_space=pltpu.VMEM),
                pl.BlockSpec(memory_space=pltpu.VMEM),
            ),
            scratch_shapes=scratch,
            compiler_params=pltpu.CompilerParams(
                collective_id=0, has_side_effects=True, vmem_limit_bytes=32 * 2**20
            ),
            name="shallow_water",
        )(*arrays)

    in_specs = (P(None, "groups", axis), P("groups", axis), P("groups", axis), P("groups", None))
    out_specs = (P(None, "groups", axis), P("groups", axis))
    return jax.shard_map(body, mesh=mesh, in_specs=in_specs, out_specs=out_specs, check_vma=False)
```

```python
import functools

import jax
import jax.numpy as jnp
from jax import lax
from jax.experimental import pallas as pl
from jax.experimental.pallas import tpu as pltpu
from jax.sharding import PartitionSpec as P

STEPS = 2
PAD = 8
CHUNK = 64
MESSAGE = 32
LAG = 8
AHEAD = 6
DIRECT = 4
FIRST = 128
LANES = 128

gravity_half = 0.5
depth_floor = 0.25
flux_factor = 0.1
time_step = 0.25


def advance(state, wet, damping, east, west, south, north):
    h, p, q = state
    inverse = 1.0 / jnp.maximum(h, depth_floor)
    u = p * inverse
    v = q * inverse
    pressure = gravity_half * h * h
    cross = q * u
    flux_p = p * u + pressure
    flux_q = q * v + pressure

    def gather(cell, flux_east, flux_south):
        quarter = 0.25 * cell
        along = flux_factor * flux_east
        down = flux_factor * flux_south
        return (east(quarter - along) + west(quarter + along)) + (
            south(quarter - down) + north(quarter + down)
        )

    return (
        wet * gather(h, p, q),
        damping * gather(p, flux_p, cross),
        damping * gather(q, cross, flux_q),
    )


def masks(openness):
    wet = jnp.where(openness > 0.0, 1.0, 0.0)
    return wet, wet / (1.0 + time_step * openness)


def kernel(
    axis,
    count,
    fields_ref,
    friction_ref,
    wet_ref,
    owner_ref,
    out_fields,
    out_depth,
    state,
    fric,
    mask,
    owner,
    first,
    inbox,
    back,
    turn,
    near_out,
    far_out,
    mine,
    other,
    packed,
    halo_left,
    halo_right,
    edge,
    edge_turn,
    edge_first,
    edge_in,
    edge_back,
    edge_give,
    edge_near,
    edge_mine,
    edge_other,
    edge_final,
    edge_wide,
    load_sem,
    table_sem,
    raw_send,
    relay_send,
    in_recv,
    back_send,
    swap_send,
    swap_recv,
    halo_send,
    halo_recv,
    hello,
):
    rows, cols = friction_ref.shape
    tile = cols
    tile_rows = rows // tile
    messages = rows // MESSAGE
    split = messages - DIRECT
    chunks = rows // CHUNK
    extra = messages
    MESH = pl.DeviceIdType.MESH

    me = lax.axis_index(axis)
    odd = me % 2
    position = me % 8
    chip = position // 2
    middle = ((chip + 1) // 2) % 2
    toward = me + 2 - 4 * (chip // 2)
    outward = 2 * me - toward
    sibling = me + 1 - 2 * odd
    keeper = me - position + 1
    is_keeper = position == 1
    is_leaf = position == 0
    is_third = chip == 2
    is_middle = middle == 1
    is_end = middle == 0

    last = jnp.where(me == count - 1, 1, 0)
    parity = (me // 8) % 2
    lead_left = jnp.where(position == 0, parity, jnp.where(position == 6, 1, 0))
    lead_left = jnp.where(me == 0, 0, lead_left)
    follow_left = jnp.where(me == 0, 0, 1 - lead_left)
    lead_right = jnp.where(position == 7, parity, jnp.where(position == 5, 0, 1)) * (1 - last)
    follow_right = (1 - last) * (1 - lead_right)

    def load(number):
        start, size = ((0, FIRST), (FIRST, rows - FIRST))[number]
        here = pl.ds(start, size)
        there = pl.ds(start + PAD, size)
        return [
            pltpu.make_async_copy(
                fields_ref.at[:, here, :], state.at[:, there, :], load_sem.at[number, 0]
            ),
            pltpu.make_async_copy(friction_ref.at[here, :], fric.at[there, :], load_sem.at[number, 1]),
            pltpu.make_async_copy(wet_ref.at[here, :], mask.at[there, :], load_sem.at[number, 2]),
        ]

    def await_load(number):
        for copy in load(number):
            copy.wait()

    table = pltpu.make_async_copy(owner_ref, owner, table_sem)
    for number in range(2):
        for copy in load(number):
            copy.start()
    table.start()

    barrier = pltpu.get_barrier_semaphore()

    def greet(peer):
        pl.semaphore_signal(barrier, inc=1, device_id={axis: peer}, device_id_type=MESH)

    @pl.when(is_middle)
    def _():
        greet(outward)
        greet(toward)

    @pl.when(is_third)
    def _():
        greet(keeper)

    @pl.when(follow_left == 1)
    def _():
        greet(me - 1)

    @pl.when(follow_right == 1)
    def _():
        greet(me + 1)

    zero_rows = jnp.zeros((PAD, cols), jnp.float32)
    for start in (0, PAD + rows):
        for plane in range(3):
            state[plane, start : start + PAD, :] = zero_rows
        fric[start : start + PAD, :] = zero_rows
        mask[start : start + PAD, :] = jnp.zeros((PAD, cols), jnp.int32)
    edge[...] = jnp.zeros_like(edge)
    edge_turn[...] = jnp.zeros_like(edge_turn)
    edge_final[...] = jnp.zeros_like(edge_final)

    def differs(tile_row, bit):
        own = owner[tile_row, me]
        return (own // 2 ** bit + me // 2 ** bit) % 2

    def remote(src, dst, send, recv, peer):
        return pltpu.make_async_remote_copy(
            src_ref=src,
            dst_ref=dst,
            send_sem=send,
            recv_sem=recv,
            device_id={axis: peer},
            device_id_type=MESH,
        )

    def span(m):
        return pl.ds(pl.multiple_of(m * MESSAGE, MESSAGE), MESSAGE)

    def raw(m, slot):
        return remote(
            first.at[span(m), :], inbox.at[slot, span(m), :], raw_send.at[0], in_recv.at[slot, m], toward
        )

    def relay(m):
        return remote(
            inbox.at[0, span(m), :], inbox.at[2, span(m), :], relay_send.at[0], in_recv.at[2, m], toward
        )

    plane_slot = jnp.where(chip == 1, odd, 0)
    receiver = jnp.where(chip == 1, keeper, outward)

    def give(m, source, slot):
        return remote(
            source.at[span(m), :],
            back.at[slot, span(m), :],
            back_send.at[0],
            in_recv.at[slot, m],
            receiver,
        )

    def near_direct(m):
        return remote(
            near_out.at[span(m), :], inbox.at[1, span(m), :], raw_send.at[0], in_recv.at[1, m], me - 2
        )

    def far_direct(m, core):
        return remote(
            far_out.at[span(m), :],
            inbox.at[1 + core, span(m), :],
            relay_send.at[0],
            in_recv.at[2, m - (1 - core) * split],
            keeper,
        )

    def pass_back(m, slot):
        return remote(
            near_out.at[span(m), :], other.at[span(m), :], swap_send.at[0], swap_recv.at[slot], sibling
        )

    def swap(m, slot):
        return remote(
            mine.at[span(m), :], other.at[span(m), :], swap_send.at[0], swap_recv.at[slot], sibling
        )

    def edge_raw(slot):
        return remote(edge_first, edge_in.at[slot], raw_send.at[1], in_recv.at[slot, extra], toward)

    edge_relay = remote(
        edge_in.at[0], edge_in.at[2], relay_send.at[1], in_recv.at[2, extra], toward
    )

    def edge_return(slot):
        return remote(
            edge_give, edge_back.at[slot], back_send.at[1], in_recv.at[slot, extra], receiver
        )

    edge_pass = remote(edge_near, edge_other, swap_send.at[1], swap_recv.at[1], sibling)
    edge_swap = remote(edge_mine, edge_other, swap_send.at[1], swap_recv.at[1], sibling)

    halo_to_left = remote(
        packed.at[pl.ds(0, 16), :], halo_right, halo_send.at[0], halo_recv.at[0], me - 1
    )
    halo_to_right = remote(
        packed.at[pl.ds(16, 16), :], halo_left, halo_send.at[1], halo_recv.at[1], me + 1
    )

    def shift(axis_number, amount, size):
        return lambda a: pltpu.roll(a, amount % size, axis_number)

    def compute(i):
        reach = CHUNK + 2 * PAD
        at = pl.multiple_of(i * CHUNK, CHUNK)
        where = pl.ds(at, reach)
        openness = mask[where, :].astype(jnp.float32) * fric[where, :]
        wet, damping = masks(openness)
        values = tuple(state[plane, where, :] * wet for plane in range(3))
        for _ in range(STEPS):
            values = advance(
                values,
                wet,
                damping,
                shift(1, -1, cols),
                shift(1, 1, cols),
                shift(0, -1, reach),
                shift(0, 1, reach),
            )
        here = pl.ds(at, CHUNK)
        first[here, :] = values[0][PAD : PAD + CHUNK]
        for plane in range(3):
            out_fields[plane, here, :] = values[plane][PAD : PAD + CHUNK]

    def for_end(by, own, near, far):
        return jnp.where(by == 3, far, jnp.where(by == 2, near, own))

    def for_middle(by, own, end, near, far):
        return jnp.where(by == 3, near, jnp.where(by == 2, far, jnp.where(by == 1, end, own)))

    def of_row(pair, m, shape):
        value = pair[-1]
        for tile_row in reversed(range(tile_rows - 1)):
            value = jnp.where(m < (tile_row + 1) * (tile // MESSAGE), pair[tile_row], value)
        return jnp.full(shape, value, jnp.int32)

    def send_chunk(number):
        for part in range(CHUNK // MESSAGE):
            raw(number * (CHUNK // MESSAGE) + part, middle).start()

    @pl.when(is_keeper)
    def _():
        pl.semaphore_wait(barrier, 3 + lead_left + lead_right)
        for ahead in range(1, 5):
            pl.semaphore_signal(hello, inc=1, device_id={axis: me + ahead}, device_id_type=MESH)

    await_load(0)
    compute(0)

    @pl.when(position != 1)
    def _():
        pl.semaphore_wait(barrier, 1 + lead_left + lead_right)

    send_chunk(0)
    await_load(1)
    table.wait()
    moves = [differs(tile_row, 1) + 2 * differs(tile_row, 2) for tile_row in range(tile_rows)]
    flips = [differs(tile_row, 0) for tile_row in range(tile_rows)]

    compute(1)
    send_chunk(1)

    lane = lax.broadcasted_iota(jnp.int32, (LANES, LANES), 1)

    @pl.loop(0, rows // LANES)
    def _(block):
        where = pl.ds(pl.multiple_of(PAD + block * LANES, PAD), LANES)
        result = jnp.zeros((LANES, LANES), jnp.float32)
        for side, low in enumerate((0, cols - LANES)):
            cut = pl.ds(low, LANES)
            openness = mask[where, cut].astype(jnp.float32) * fric[where, cut]
            wet = jnp.where(openness > 0.0, 1.0, 0.0)
            planes = [state[plane, where, cut] * wet for plane in range(3)] + [openness]
            for number, values in enumerate(planes):
                source = (LANES - 4) * side
                target = 16 * side + 4 * number
                moved = pltpu.roll(values, (target - source) % LANES, 1)
                result = jnp.where(lane >= target, moved, result)
        packed[:, pl.ds(pl.multiple_of(block * LANES, LANES), LANES)] = result.T[0:32]

    @pl.when(lead_left == 1)
    def _():
        halo_to_left.start()

    @pl.when(lead_right == 1)
    def _():
        halo_to_right.start()

    @pl.loop(2, chunks)
    def _(j):
        compute(j)

        @pl.when((chip != 2) | (j < split * MESSAGE // CHUNK))
        def _():
            send_chunk(j)

    @pl.when(follow_right == 1)
    def _():
        halo_to_left.wait_recv()
        halo_to_right.start()

    @pl.when(follow_left == 1)
    def _():
        halo_to_right.wait_recv()
        halo_to_left.start()

    def pass_on(m):
        raw(m, 0).wait_recv()
        relay(m).start()

    @pl.when(is_third)
    def _():
        @pl.loop(0, split)
        def _(m):
            pass_on(m)

        @pl.loop(split, messages)
        def _(m):
            raw(m, 0).wait_recv()
            where = span(m)
            by = of_row(moves, m, (MESSAGE, cols))
            near_out[where, :] = jnp.where(by == 3, first[where, :], inbox[0, where, :])
            near_direct(m).start()

    @pl.when(chip == 1)
    def _():
        pl.semaphore_wait(hello, 1)

        @pl.loop(split, messages)
        def _(m):
            give(m, first, plane_slot).start()

    @pl.when(lead_right == 1)
    def _():
        halo_to_left.wait_recv()

    @pl.when(lead_left == 1)
    def _():
        halo_to_right.wait_recv()

    for number in range(4):
        base = 4 * number
        edge[number, 0:2, :] = jnp.where(me > 0, halo_left[base + 2 : base + 4, :], 0.0)
        edge[number, 2:6, :] = packed[base : base + 4, :]
        edge[number, 8:12, :] = packed[16 + base : 20 + base, :]
        edge[number, 12:14, :] = jnp.where(me < count - 1, halo_right[base : base + 2, :], 0.0)

    place = lax.broadcasted_iota(jnp.int32, (16, rows), 1)
    wet, damping = masks(edge[3])
    values = tuple(edge[plane] for plane in range(3))
    for _ in range(STEPS):
        values = advance(
            values,
            wet,
            damping,
            shift(0, -1, 16),
            shift(0, 1, 16),
            lambda a: jnp.where(place == rows - 1, 0.0, pltpu.roll(a, rows - 1, 1)),
            lambda a: jnp.where(place == 0, 0.0, pltpu.roll(a, 1, 1)),
        )
    for plane in range(3):
        edge_turn[16 * plane : 16 * plane + 16, :] = values[plane]
    for tile_row in range(tile_rows):
        cut = pl.ds(tile_row * tile, tile)
        edge_first[4 * tile_row : 4 * tile_row + 2, :] = edge_turn[2:4, cut]
        edge_first[4 * tile_row + 2 : 4 * tile_row + 4, :] = edge_turn[10:12, cut]
    edge_raw(middle).start()

    line = lax.broadcasted_iota(jnp.int32, (8, cols), 0)

    def by_line(pair):
        value = jnp.full((8, cols), pair[-1], jnp.int32)
        for tile_row in reversed(range(tile_rows - 1)):
            value = jnp.where(line < 4 * (tile_row + 1), pair[tile_row], value)
        return value

    edge_by = by_line(moves)

    def return_second(m):
        where = span(m)
        by = of_row(moves, m, (MESSAGE, cols))
        raw(m, 1).wait_recv()
        relay(m).wait_recv()
        turn[where, :] = for_end(by, first[where, :], inbox[1, where, :], inbox[2, where, :])
        give(m, turn, plane_slot).start()

    def settle_second(m, late):
        where = span(m)
        by = of_row(moves, m, (MESSAGE, cols))
        if late:
            raw(m, 1).wait_recv()
        own = first[where, :]
        end = inbox[0, where, :]
        near = inbox[1, where, :]
        if late:
            mine[where, :] = jnp.where(by >= 2, near, jnp.where(by == 1, end, own))
        else:
            mine[where, :] = for_middle(by, own, end, near, inbox[2, where, :])
        swap(m, m - split + 2 if late else 0).start()

    @pl.when(is_third)
    def _():
        edge_raw(0).wait_recv()
        edge_relay.start()
        pl.semaphore_wait(hello, 1)

        @pl.loop(split, messages)
        def _(m):
            where = span(m)
            by = of_row(moves, m, (MESSAGE, cols))
            far_out[where, :] = jnp.where(by == 2, first[where, :], inbox[0, where, :])
            far_direct(m, odd).start()

    def edge_returns():
        edge_raw(1).wait_recv()
        edge_relay.wait_recv()
        edge_give[...] = for_end(edge_by, edge_first[...], edge_in[1], edge_in[2])
        edge_return(plane_slot).start()

    def edge_relays():
        edge_raw(0).wait_recv()
        edge_relay.start()

    @pl.when((chip == 1) & (odd == 0))
    def _():
        @pl.loop(0, AHEAD)
        def _(m):
            return_second(m)

        @pl.loop(0, split - AHEAD)
        def _(m):
            pass_on(m)
            return_second(m + AHEAD)

        @pl.loop(split - AHEAD, split)
        def _(m):
            pass_on(m)

        edge_returns()

        @pl.loop(split, messages)
        def _(m):
            pass_on(m)

        edge_relays()

    @pl.when((chip == 1) & (odd == 1))
    def _():
        @pl.loop(0, LAG)
        def _(m):
            pass_on(m)

        @pl.loop(0, messages - LAG)
        def _(m):
            return_second(m)
            pass_on(m + LAG)

        @pl.loop(messages - LAG, split)
        def _(m):
            return_second(m)

        edge_relays()
        edge_returns()

    @pl.when(chip == 1)
    def _():
        @pl.loop(0, split)
        def _(m):
            settle_second(m, False)

    def patch_fields():
        @pl.loop(0, rows // LANES)
        def _(block):
            where = pl.ds(pl.multiple_of(block * LANES, LANES), LANES)
            turned = edge_turn[:, where].T
            for plane in range(3):
                on_left = pltpu.roll(turned, (-16 * plane - 2) % LANES, 1)
                cut = pl.ds(0, LANES)
                out_fields[plane, where, cut] = jnp.where(
                    lane < 2, on_left, out_fields[plane, where, cut]
                )
                on_right = pltpu.roll(turned, (LANES - 2 - 16 * plane - 10) % LANES, 1)
                cut = pl.ds(cols - LANES, LANES)
                out_fields[plane, where, cut] = jnp.where(
                    lane >= LANES - 2, on_right, out_fields[plane, where, cut]
                )

    @pl.when(is_end)
    def _():
        patch_fields()

    def settle(m, late):
        where = span(m)
        by = of_row(moves, m, (MESSAGE, cols))
        slot = m - split + 2 if late else 0

        @pl.when(is_third)
        def _():
            raw(m, 1).wait_recv()
            relay(m).wait_recv()
            own = first[where, :]
            near = inbox[1, where, :]
            far = inbox[2, where, :]
            turn[where, :] = for_end(by, own, near, far)
            give(m, turn, 0).start()
            mine[where, :] = for_middle(by, own, inbox[0, where, :], near, far)
            swap(m, slot).start()

        @pl.when(is_leaf)
        def _():
            mine[where, :] = first[where, :]
            swap(m, slot).start()

        @pl.when(is_keeper)
        def _():
            flipped = of_row(flips, m, (MESSAGE, cols)) == 1
            parts = []
            for core in range(2):
                give(m, turn, core).wait_recv()
                part = back[core, where, :]
                if late:
                    far_direct(m, core).wait_recv()
                    part = jnp.where(by >= 2, inbox[1 + core, where, :], part)
                parts.append(part)
            settled = jnp.where(by == 0, first[where, :], parts[1])
            near_out[where, :] = jnp.where(flipped, settled, parts[0])
            pass_back(m, slot).start()
            mine[where, :] = jnp.where(flipped, parts[0], settled)

        @pl.when(chip == 3)
        def _():
            give(m, turn, 0).wait_recv()
            mine[where, :] = jnp.where(by == 0, first[where, :], back[0, where, :])
            swap(m, slot).start()

    @pl.when(chip != 1)
    def _():
        @pl.loop(0, split)
        def _(m):
            settle(m, False)

    def settle_edges():
        @pl.when(is_third)
        def _():
            edge_returns()

        @pl.when(is_middle)
        def _():
            edge_mine[...] = for_middle(
                edge_by, edge_first[...], edge_in[0], edge_in[1], edge_in[2]
            )
            edge_swap.start()

        @pl.when(is_leaf)
        def _():
            edge_mine[...] = edge_first[...]
            edge_swap.start()

        @pl.when(is_keeper)
        def _():
            for core in range(2):
                edge_return(core).wait_recv()
            flipped = by_line(flips) == 1
            settled = jnp.where(edge_by == 0, edge_first[...], edge_back[1])
            edge_near[...] = jnp.where(flipped, settled, edge_back[0])
            edge_pass.start()
            edge_mine[...] = jnp.where(flipped, edge_back[0], settled)

        @pl.when(chip == 3)
        def _():
            edge_return(0).wait_recv()
            edge_mine[...] = jnp.where(edge_by == 0, edge_first[...], edge_back[0])
            edge_swap.start()

    @pl.when(chip < 2)
    def _():
        settle_edges()

    @pl.when(chip != 1)
    def _():
        @pl.loop(split, messages)
        def _(m):
            settle(m, True)

    @pl.when(chip == 1)
    def _():
        @pl.loop(split, messages)
        def _(m):
            settle_second(m, True)

    @pl.when(chip >= 2)
    def _():
        settle_edges()

    @pl.when(is_middle)
    def _():
        patch_fields()

    edge_swap.wait_recv()
    choices = []
    for tile_row in range(tile_rows):
        still = jnp.where(moves[tile_row] == 0, 1, 0)
        flipped = flips[tile_row]
        from_leaf = flipped * still
        choice = jnp.where(is_keeper, from_leaf, flipped)
        choices.append(jnp.where(is_leaf, 1 - (1 - flipped) * still, choice))
    edge_final[0:8, :] = jnp.where(by_line(choices) == 1, edge_other[...], edge_mine[...])
    for tile_row in range(tile_rows):
        for block in range(tile // LANES):
            turned = edge_final[:, block * LANES : (block + 1) * LANES].T
            where = pl.ds(tile_row * tile + block * LANES, LANES)
            edge_wide[where, 0:LANES] = pltpu.roll(turned, (-4 * tile_row) % LANES, 1)
            edge_wide[where, cols - LANES : cols] = pltpu.roll(
                turned, (LANES - 2 - 4 * tile_row - 2) % LANES, 1
            )

    column = lax.broadcasted_iota(jnp.int32, (MESSAGE, cols), 1)
    inside = (column >= 2) & (column < cols - 2)

    early_rows = pl.ds(0, split * MESSAGE)
    remote(
        mine.at[early_rows, :], other.at[early_rows, :], swap_send.at[0], swap_recv.at[0], sibling
    ).wait_recv()

    @pl.loop(0, messages)
    def _(m):
        @pl.when(m >= split)
        def _():
            swap(m, m - split + 2).wait_recv()

        where = span(m)
        taken = of_row(choices, m, (MESSAGE, cols)) == 1
        value = jnp.where(taken, other[where, :], mine[where, :])
        out_depth[where, :] = jnp.where(inside, value, edge_wide[where, :])

    @pl.when((lead_left == 1) | (follow_left == 1))
    def _():
        halo_to_left.wait_send()

    @pl.when((lead_right == 1) | (follow_right == 1))
    def _():
        halo_to_right.wait_send()

    edge_raw(middle).wait_send()
    edge_swap.wait_send()

    remote(first, inbox.at[0], raw_send.at[0], in_recv.at[0, 0], toward).wait_send()
    remote(mine, other, swap_send.at[0], swap_recv.at[0], sibling).wait_send()

    @pl.when(is_middle)
    def _():
        edge_relay.wait_send()
        edge_return(plane_slot).wait_send()
        remote(inbox.at[0], inbox.at[2], relay_send.at[0], in_recv.at[2, 0], toward).wait_send()
        remote(turn, back.at[0], back_send.at[0], in_recv.at[0, 0], outward).wait_send()


def solution(mesh):
    axis = "gx"
    count = mesh.shape[axis]

    def body(fields, friction, wet_mask, owner_table):
        rows, cols = friction.shape
        padded = rows + 2 * PAD
        slots = rows // MESSAGE + 1
        f32 = jnp.float32
        whole = pltpu.VMEM((rows, cols), f32)
        small = pltpu.VMEM((8, cols), f32)
        scratch = [
            pltpu.VMEM((3, padded, cols), f32),
            pltpu.VMEM((padded, cols), f32),
            pltpu.VMEM((padded, cols), jnp.int32),
            pltpu.SMEM(owner_table.shape, jnp.int32),
            whole,
            pltpu.VMEM((3, rows, cols), f32),
            pltpu.VMEM((2, rows, cols), f32),
            whole,
            whole,
            whole,
            whole,
            whole,
            pltpu.VMEM((32, rows), f32),
            pltpu.VMEM((16, rows), f32),
            pltpu.VMEM((16, rows), f32),
            pltpu.VMEM((4, 16, rows), f32),
            pltpu.VMEM((LANES, rows), f32),
            small,
            pltpu.VMEM((3, 8, cols), f32),
            pltpu.VMEM((2, 8, cols), f32),
            small,
            small,
            small,
            small,
            pltpu.VMEM((LANES, cols), f32),
            whole,
            pltpu.SemaphoreType.DMA((2, 3)),
            pltpu.SemaphoreType.DMA,
            pltpu.SemaphoreType.DMA((2,)),
            pltpu.SemaphoreType.DMA((2,)),
            pltpu.SemaphoreType.DMA((3, slots)),
            pltpu.SemaphoreType.DMA((2,)),
            pltpu.SemaphoreType.DMA((2,)),
            pltpu.SemaphoreType.DMA((2 + DIRECT,)),
            pltpu.SemaphoreType.DMA((2,)),
            pltpu.SemaphoreType.DMA((2,)),
            pltpu.SemaphoreType.REGULAR,
        ]
        arrays = [
            pltpu.with_memory_space_constraint(array, pltpu.HBM)
            for array in (fields, friction, wet_mask, owner_table)
        ]
        return pl.pallas_call(
            functools.partial(kernel, axis, count),
            out_shape=(
                jax.ShapeDtypeStruct(fields.shape, f32),
                jax.ShapeDtypeStruct(friction.shape, f32),
            ),
            in_specs=[pl.BlockSpec(memory_space=pltpu.HBM)] * 4,
            out_specs=(
                pl.BlockSpec(memory_space=pltpu.VMEM),
                pl.BlockSpec(memory_space=pltpu.VMEM),
            ),
            scratch_shapes=scratch,
            compiler_params=pltpu.CompilerParams(
                collective_id=0, has_side_effects=True, vmem_limit_bytes=32 * 2**20
            ),
            name="shallow_water",
        )(*arrays)

    in_specs = (P(None, "groups", axis), P("groups", axis), P("groups", axis), P("groups", None))
    out_specs = (P(None, "groups", axis), P("groups", axis))
    return jax.shard_map(body, mesh=mesh, in_specs=in_specs, out_specs=out_specs, check_vma=False)
```

```python
import functools

import jax
import jax.numpy as jnp
from jax import lax
from jax.experimental import pallas as pl
from jax.experimental.pallas import tpu as pltpu
from jax.sharding import PartitionSpec as P

STEPS = 2
PAD = 8
CHUNK = 64
MESSAGE = 32
LAG = 8
AHEAD = 8
DIRECT = 4
FIRST = 80
LANES = 128

gravity_half = 0.5
depth_floor = 0.25
flux_factor = 0.1
time_step = 0.25


def advance(state, wet, damping, east, west, south, north):
    h, p, q = state
    inverse = 1.0 / jnp.maximum(h, depth_floor)
    u = p * inverse
    v = q * inverse
    pressure = gravity_half * h * h
    cross = q * u
    flux_p = p * u + pressure
    flux_q = q * v + pressure

    def gather(cell, flux_east, flux_south):
        quarter = 0.25 * cell
        along = flux_factor * flux_east
        down = flux_factor * flux_south
        return (east(quarter - along) + west(quarter + along)) + (
            south(quarter - down) + north(quarter + down)
        )

    return (
        wet * gather(h, p, q),
        damping * gather(p, flux_p, cross),
        damping * gather(q, cross, flux_q),
    )


def masks(openness):
    wet = jnp.where(openness > 0.0, 1.0, 0.0)
    return wet, wet / (1.0 + time_step * openness)


def kernel(
    axis,
    count,
    fields_ref,
    friction_ref,
    wet_ref,
    owner_ref,
    out_fields,
    out_depth,
    state,
    fric,
    mask,
    owner,
    first,
    inbox,
    back,
    turn,
    near_out,
    far_out,
    mine,
    other,
    packed,
    halo_left,
    halo_right,
    edge,
    edge_turn,
    edge_first,
    edge_in,
    edge_back,
    edge_give,
    edge_near,
    edge_far,
    edge_mine,
    edge_other,
    edge_final,
    edge_wide,
    load_sem,
    table_sem,
    raw_send,
    relay_send,
    in_recv,
    back_send,
    swap_send,
    swap_recv,
    halo_send,
    halo_recv,
    hello,
):
    rows, cols = friction_ref.shape
    tile = cols
    tile_rows = rows // tile
    messages = rows // MESSAGE
    split = messages - DIRECT
    chunks = rows // CHUNK
    extra = messages
    MESH = pl.DeviceIdType.MESH

    me = lax.axis_index(axis)
    odd = me % 2
    position = me % 8
    chip = position // 2
    middle = ((chip + 1) // 2) % 2
    toward = me + 2 - 4 * (chip // 2)
    outward = 2 * me - toward
    sibling = me + 1 - 2 * odd
    keeper = me - position + 1
    is_keeper = position == 1
    is_leaf = position == 0
    is_third = chip == 2
    is_middle = middle == 1
    is_end = middle == 0

    last = jnp.where(me == count - 1, 1, 0)
    parity = (me // 8) % 2
    lead_left = jnp.where(position == 0, parity, jnp.where(position == 6, 1, 0))
    lead_left = jnp.where(me == 0, 0, lead_left)
    follow_left = jnp.where(me == 0, 0, 1 - lead_left)
    lead_right = jnp.where(position == 7, parity, jnp.where(position == 5, 0, 1)) * (1 - last)
    follow_right = (1 - last) * (1 - lead_right)

    def load(number):
        start, size = ((0, FIRST), (FIRST, rows - FIRST))[number]
        here = pl.ds(start, size)
        there = pl.ds(start + PAD, size)
        return [
            pltpu.make_async_copy(
                fields_ref.at[:, here, :], state.at[:, there, :], load_sem.at[number, 0]
            ),
            pltpu.make_async_copy(friction_ref.at[here, :], fric.at[there, :], load_sem.at[number, 1]),
            pltpu.make_async_copy(wet_ref.at[here, :], mask.at[there, :], load_sem.at[number, 2]),
        ]

    def await_load(number):
        for copy in load(number):
            copy.wait()

    table = pltpu.make_async_copy(owner_ref, owner, table_sem)
    for number in range(2):
        for copy in load(number):
            copy.start()
    table.start()

    barrier = pltpu.get_barrier_semaphore()

    def greet(peer):
        pl.semaphore_signal(barrier, inc=1, device_id={axis: peer}, device_id_type=MESH)

    @pl.when(is_middle)
    def _():
        greet(outward)
        greet(toward)

    @pl.when(is_third)
    def _():
        greet(keeper)

    @pl.when(follow_left == 1)
    def _():
        greet(me - 1)

    @pl.when(follow_right == 1)
    def _():
        greet(me + 1)

    zero_rows = jnp.zeros((PAD, cols), jnp.float32)
    for start in (0, PAD + rows):
        for plane in range(3):
            state[plane, start : start + PAD, :] = zero_rows
        fric[start : start + PAD, :] = zero_rows
        mask[start : start + PAD, :] = jnp.zeros((PAD, cols), jnp.int32)
    edge[...] = jnp.zeros_like(edge)
    edge_turn[...] = jnp.zeros_like(edge_turn)
    edge_final[...] = jnp.zeros_like(edge_final)

    def differs(tile_row, bit):
        own = owner[tile_row, me]
        return (own // 2 ** bit + me // 2 ** bit) % 2

    def remote(src, dst, send, recv, peer):
        return pltpu.make_async_remote_copy(
            src_ref=src,
            dst_ref=dst,
            send_sem=send,
            recv_sem=recv,
            device_id={axis: peer},
            device_id_type=MESH,
        )

    def span(m):
        return pl.ds(pl.multiple_of(m * MESSAGE, MESSAGE), MESSAGE)

    def raw(m, slot):
        return remote(
            first.at[span(m), :], inbox.at[slot, span(m), :], raw_send.at[0], in_recv.at[slot, m], toward
        )

    def relay(m):
        return remote(
            inbox.at[0, span(m), :], inbox.at[2, span(m), :], relay_send.at[0], in_recv.at[2, m], toward
        )

    plane_slot = jnp.where(chip == 1, odd, 0)
    receiver = jnp.where(chip == 1, keeper, outward)

    def give(m, source, slot):
        return remote(
            source.at[span(m), :],
            back.at[slot, span(m), :],
            back_send.at[0],
            in_recv.at[slot, m],
            receiver,
        )

    def near_direct(m):
        return remote(
            near_out.at[span(m), :], inbox.at[1, span(m), :], raw_send.at[0], in_recv.at[1, m], me - 2
        )

    def far_direct(m, core):
        return remote(
            far_out.at[span(m), :],
            inbox.at[1 + core, span(m), :],
            relay_send.at[0],
            in_recv.at[2, m - (1 - core) * split],
            keeper,
        )

    def pass_back(m, slot):
        return remote(
            near_out.at[span(m), :], other.at[span(m), :], swap_send.at[0], swap_recv.at[slot], sibling
        )

    def swap(m, slot):
        return remote(
            mine.at[span(m), :], other.at[span(m), :], swap_send.at[0], swap_recv.at[slot], sibling
        )

    def edge_raw(slot):
        return remote(edge_first, edge_in.at[slot], raw_send.at[1], in_recv.at[slot, extra], toward)

    edge_relay = remote(
        edge_in.at[0], edge_in.at[2], relay_send.at[1], in_recv.at[2, extra], toward
    )

    def edge_return(slot, source):
        return remote(source, edge_back.at[slot], back_send.at[1], in_recv.at[slot, extra], receiver)

    edge_near_direct = remote(
        edge_near, edge_in.at[1], raw_send.at[1], in_recv.at[1, extra], me - 2
    )

    def edge_far_direct(core):
        return remote(
            edge_far,
            edge_in.at[1 + core],
            relay_send.at[1],
            in_recv.at[2, extra - (1 - core) * split],
            keeper,
        )

    edge_pass = remote(edge_near, edge_other, swap_send.at[1], swap_recv.at[1], sibling)
    edge_swap = remote(edge_mine, edge_other, swap_send.at[1], swap_recv.at[1], sibling)

    halo_to_left = remote(
        packed.at[pl.ds(0, 16), :], halo_right, halo_send.at[0], halo_recv.at[0], me - 1
    )
    halo_to_right = remote(
        packed.at[pl.ds(16, 16), :], halo_left, halo_send.at[1], halo_recv.at[1], me + 1
    )

    def shift(axis_number, amount, size):
        return lambda a: pltpu.roll(a, amount % size, axis_number)

    def compute(i):
        reach = CHUNK + 2 * PAD
        at = pl.multiple_of(i * CHUNK, CHUNK)
        where = pl.ds(at, reach)
        openness = mask[where, :].astype(jnp.float32) * fric[where, :]
        wet, damping = masks(openness)
        values = tuple(state[plane, where, :] * wet for plane in range(3))
        for _ in range(STEPS):
            values = advance(
                values,
                wet,
                damping,
                shift(1, -1, cols),
                shift(1, 1, cols),
                shift(0, -1, reach),
                shift(0, 1, reach),
            )
        here = pl.ds(at, CHUNK)
        first[here, :] = values[0][PAD : PAD + CHUNK]
        for plane in range(3):
            out_fields[plane, here, :] = values[plane][PAD : PAD + CHUNK]

    def for_end(by, own, near, far):
        return jnp.where(by == 3, far, jnp.where(by == 2, near, own))

    def for_middle(by, own, end, near, far):
        return jnp.where(by == 3, near, jnp.where(by == 2, far, jnp.where(by == 1, end, own)))

    def of_row(pair, m, shape):
        value = pair[-1]
        for tile_row in reversed(range(tile_rows - 1)):
            value = jnp.where(m < (tile_row + 1) * (tile // MESSAGE), pair[tile_row], value)
        return jnp.full(shape, value, jnp.int32)

    def send_chunk(number):
        for part in range(CHUNK // MESSAGE):
            raw(number * (CHUNK // MESSAGE) + part, middle).start()

    @pl.when(is_keeper)
    def _():
        pl.semaphore_wait(barrier, 3 + lead_left + lead_right)
        for ahead in range(1, 5):
            pl.semaphore_signal(hello, inc=1, device_id={axis: me + ahead}, device_id_type=MESH)

    await_load(0)
    compute(0)

    @pl.when(position != 1)
    def _():
        pl.semaphore_wait(barrier, 1 + lead_left + lead_right)

    send_chunk(0)
    await_load(1)
    table.wait()
    moves = [differs(tile_row, 1) + 2 * differs(tile_row, 2) for tile_row in range(tile_rows)]
    flips = [differs(tile_row, 0) for tile_row in range(tile_rows)]

    compute(1)
    send_chunk(1)

    lane = lax.broadcasted_iota(jnp.int32, (LANES, LANES), 1)

    @pl.loop(0, rows // LANES)
    def _(block):
        where = pl.ds(pl.multiple_of(PAD + block * LANES, PAD), LANES)
        result = jnp.zeros((LANES, LANES), jnp.float32)
        for side, low in enumerate((0, cols - LANES)):
            cut = pl.ds(low, LANES)
            openness = mask[where, cut].astype(jnp.float32) * fric[where, cut]
            wet = jnp.where(openness > 0.0, 1.0, 0.0)
            planes = [state[plane, where, cut] * wet for plane in range(3)] + [openness]
            for number, values in enumerate(planes):
                source = (LANES - 4) * side
                target = 16 * side + 4 * number
                moved = pltpu.roll(values, (target - source) % LANES, 1)
                result = jnp.where(lane >= target, moved, result)
        packed[:, pl.ds(pl.multiple_of(block * LANES, LANES), LANES)] = result.T[0:32]

    @pl.when(lead_left == 1)
    def _():
        halo_to_left.start()

    @pl.when(lead_right == 1)
    def _():
        halo_to_right.start()

    @pl.loop(2, chunks)
    def _(j):
        compute(j)

        @pl.when((chip != 2) | (j < split * MESSAGE // CHUNK))
        def _():
            send_chunk(j)

    @pl.when(follow_right == 1)
    def _():
        halo_to_left.wait_recv()
        halo_to_right.start()

    @pl.when(follow_left == 1)
    def _():
        halo_to_right.wait_recv()
        halo_to_left.start()

    def pass_on(m):
        raw(m, 0).wait_recv()
        relay(m).start()

    @pl.when(is_third)
    def _():
        @pl.loop(0, split)
        def _(m):
            pass_on(m)

        @pl.loop(split, messages)
        def _(m):
            raw(m, 0).wait_recv()
            where = span(m)
            by = of_row(moves, m, (MESSAGE, cols))
            near_out[where, :] = jnp.where(by == 3, first[where, :], inbox[0, where, :])
            near_direct(m).start()

    @pl.when(chip == 1)
    def _():
        pl.semaphore_wait(hello, 1)

        @pl.loop(split, messages)
        def _(m):
            give(m, first, plane_slot).start()

    @pl.when(lead_right == 1)
    def _():
        halo_to_left.wait_recv()

    @pl.when(lead_left == 1)
    def _():
        halo_to_right.wait_recv()

    for number in range(4):
        base = 4 * number
        edge[number, 0:2, :] = jnp.where(me > 0, halo_left[base + 2 : base + 4, :], 0.0)
        edge[number, 2:6, :] = packed[base : base + 4, :]
        edge[number, 8:12, :] = packed[16 + base : 20 + base, :]
        edge[number, 12:14, :] = jnp.where(me < count - 1, halo_right[base : base + 2, :], 0.0)

    place = lax.broadcasted_iota(jnp.int32, (16, rows), 1)
    wet, damping = masks(edge[3])
    values = tuple(edge[plane] for plane in range(3))
    for _ in range(STEPS):
        values = advance(
            values,
            wet,
            damping,
            shift(0, -1, 16),
            shift(0, 1, 16),
            lambda a: jnp.where(place == rows - 1, 0.0, pltpu.roll(a, rows - 1, 1)),
            lambda a: jnp.where(place == 0, 0.0, pltpu.roll(a, 1, 1)),
        )
    for plane in range(3):
        edge_turn[16 * plane : 16 * plane + 16, :] = values[plane]
    for tile_row in range(tile_rows):
        cut = pl.ds(tile_row * tile, tile)
        edge_first[4 * tile_row : 4 * tile_row + 2, :] = edge_turn[2:4, cut]
        edge_first[4 * tile_row + 2 : 4 * tile_row + 4, :] = edge_turn[10:12, cut]

    @pl.when(chip != 2)
    def _():
        edge_raw(middle).start()

    @pl.when(chip == 1)
    def _():
        edge_return(plane_slot, edge_first).start()

    line = lax.broadcasted_iota(jnp.int32, (8, cols), 0)

    def by_line(pair):
        value = jnp.full((8, cols), pair[-1], jnp.int32)
        for tile_row in reversed(range(tile_rows - 1)):
            value = jnp.where(line < 4 * (tile_row + 1), pair[tile_row], value)
        return value

    edge_by = by_line(moves)

    def return_second(m):
        where = span(m)
        by = of_row(moves, m, (MESSAGE, cols))
        raw(m, 1).wait_recv()
        relay(m).wait_recv()
        turn[where, :] = for_end(by, first[where, :], inbox[1, where, :], inbox[2, where, :])
        give(m, turn, plane_slot).start()

    def settle_second(m, late):
        where = span(m)
        by = of_row(moves, m, (MESSAGE, cols))
        if late:
            raw(m, 1).wait_recv()
        own = first[where, :]
        end = inbox[0, where, :]
        near = inbox[1, where, :]
        if late:
            mine[where, :] = jnp.where(by >= 2, near, jnp.where(by == 1, end, own))
        else:
            mine[where, :] = for_middle(by, own, end, near, inbox[2, where, :])
        swap(m, m - split + 2 if late else 0).start()

    @pl.when(is_third)
    def _():
        edge_raw(0).wait_recv()
        edge_near[...] = jnp.where(edge_by == 3, edge_first[...], edge_in[0])
        edge_near_direct.start()
        pl.semaphore_wait(hello, 1)
        edge_far[...] = jnp.where(edge_by == 2, edge_first[...], edge_in[0])
        edge_far_direct(odd).start()

        @pl.loop(split, messages)
        def _(m):
            where = span(m)
            by = of_row(moves, m, (MESSAGE, cols))
            far_out[where, :] = jnp.where(by == 2, first[where, :], inbox[0, where, :])
            far_direct(m, odd).start()

    def edge_relays():
        edge_raw(0).wait_recv()
        edge_relay.start()

    @pl.when((chip == 1) & (odd == 0))
    def _():
        @pl.loop(0, AHEAD)
        def _(m):
            return_second(m)

        @pl.loop(0, split - AHEAD)
        def _(m):
            pass_on(m)
            return_second(m + AHEAD)

        @pl.loop(split - AHEAD, messages)
        def _(m):
            pass_on(m)

        edge_relays()

    @pl.when((chip == 1) & (odd == 1))
    def _():
        @pl.loop(0, LAG)
        def _(m):
            pass_on(m)

        @pl.loop(0, messages - LAG)
        def _(m):
            return_second(m)
            pass_on(m + LAG)

        @pl.loop(messages - LAG, split)
        def _(m):
            return_second(m)

        edge_relays()

    @pl.when(chip == 1)
    def _():
        @pl.loop(0, split)
        def _(m):
            settle_second(m, False)

    def patch_fields():
        @pl.loop(0, rows // LANES)
        def _(block):
            where = pl.ds(pl.multiple_of(block * LANES, LANES), LANES)
            turned = edge_turn[:, where].T
            for plane in range(3):
                on_left = pltpu.roll(turned, (-16 * plane - 2) % LANES, 1)
                cut = pl.ds(0, LANES)
                out_fields[plane, where, cut] = jnp.where(
                    lane < 2, on_left, out_fields[plane, where, cut]
                )
                on_right = pltpu.roll(turned, (LANES - 2 - 16 * plane - 10) % LANES, 1)
                cut = pl.ds(cols - LANES, LANES)
                out_fields[plane, where, cut] = jnp.where(
                    lane >= LANES - 2, on_right, out_fields[plane, where, cut]
                )

    @pl.when(is_end)
    def _():
        patch_fields()

    def settle(m, late):
        where = span(m)
        by = of_row(moves, m, (MESSAGE, cols))
        slot = m - split + 2 if late else 0

        @pl.when(is_third)
        def _():
            raw(m, 1).wait_recv()
            relay(m).wait_recv()
            own = first[where, :]
            near = inbox[1, where, :]
            far = inbox[2, where, :]
            turn[where, :] = for_end(by, own, near, far)
            give(m, turn, 0).start()
            mine[where, :] = for_middle(by, own, inbox[0, where, :], near, far)
            swap(m, slot).start()

        @pl.when(is_leaf)
        def _():
            mine[where, :] = first[where, :]
            swap(m, slot).start()

        @pl.when(is_keeper)
        def _():
            flipped = of_row(flips, m, (MESSAGE, cols)) == 1
            parts = []
            for core in range(2):
                give(m, turn, core).wait_recv()
                part = back[core, where, :]
                if late:
                    far_direct(m, core).wait_recv()
                    part = jnp.where(by >= 2, inbox[1 + core, where, :], part)
                parts.append(part)
            settled = jnp.where(by == 0, first[where, :], parts[1])
            near_out[where, :] = jnp.where(flipped, settled, parts[0])
            pass_back(m, slot).start()
            mine[where, :] = jnp.where(flipped, parts[0], settled)

        @pl.when(chip == 3)
        def _():
            give(m, turn, 0).wait_recv()
            mine[where, :] = jnp.where(by == 0, first[where, :], back[0, where, :])
            swap(m, slot).start()

    @pl.when(chip != 1)
    def _():
        @pl.loop(0, split)
        def _(m):
            settle(m, False)

    def settle_edges():
        @pl.when(is_third)
        def _():
            edge_raw(1).wait_recv()
            edge_relay.wait_recv()
            own = edge_first[...]
            near = edge_in[1]
            far = edge_in[2]
            edge_give[...] = for_end(edge_by, own, near, far)
            edge_return(0, edge_give).start()
            edge_mine[...] = for_middle(edge_by, own, edge_in[0], near, far)
            edge_swap.start()

        @pl.when(chip == 1)
        def _():
            edge_raw(1).wait_recv()
            end_or_own = jnp.where(edge_by == 1, edge_in[0], edge_first[...])
            edge_mine[...] = jnp.where(edge_by >= 2, edge_in[1], end_or_own)
            edge_swap.start()

        @pl.when(is_leaf)
        def _():
            edge_mine[...] = edge_first[...]
            edge_swap.start()

        @pl.when(is_keeper)
        def _():
            parts = []
            for core in range(2):
                edge_return(core, edge_give).wait_recv()
                edge_far_direct(core).wait_recv()
                parts.append(jnp.where(edge_by >= 2, edge_in[1 + core], edge_back[core]))
            flipped = by_line(flips) == 1
            settled = jnp.where(edge_by == 0, edge_first[...], parts[1])
            edge_near[...] = jnp.where(flipped, settled, parts[0])
            edge_pass.start()
            edge_mine[...] = jnp.where(flipped, parts[0], settled)

        @pl.when(chip == 3)
        def _():
            edge_return(0, edge_give).wait_recv()
            edge_mine[...] = jnp.where(edge_by == 0, edge_first[...], edge_back[0])
            edge_swap.start()

    @pl.when(chip < 2)
    def _():
        settle_edges()

    @pl.when(chip != 1)
    def _():
        @pl.loop(split, messages)
        def _(m):
            settle(m, True)

    @pl.when(chip == 1)
    def _():
        @pl.loop(split, messages)
        def _(m):
            settle_second(m, True)

    @pl.when(chip >= 2)
    def _():
        settle_edges()

    @pl.when(is_middle)
    def _():
        patch_fields()

    edge_swap.wait_recv()
    choices = []
    for tile_row in range(tile_rows):
        still = jnp.where(moves[tile_row] == 0, 1, 0)
        flipped = flips[tile_row]
        from_leaf = flipped * still
        choice = jnp.where(is_keeper, from_leaf, flipped)
        choices.append(jnp.where(is_leaf, 1 - (1 - flipped) * still, choice))
    edge_final[0:8, :] = jnp.where(by_line(choices) == 1, edge_other[...], edge_mine[...])
    for tile_row in range(tile_rows):
        for block in range(tile // LANES):
            turned = edge_final[:, block * LANES : (block + 1) * LANES].T
            where = pl.ds(tile_row * tile + block * LANES, LANES)
            edge_wide[where, 0:LANES] = pltpu.roll(turned, (-4 * tile_row) % LANES, 1)
            edge_wide[where, cols - LANES : cols] = pltpu.roll(
                turned, (LANES - 2 - 4 * tile_row - 2) % LANES, 1
            )

    column = lax.broadcasted_iota(jnp.int32, (MESSAGE, cols), 1)
    inside = (column >= 2) & (column < cols - 2)

    early_rows = pl.ds(0, split * MESSAGE)
    remote(
        mine.at[early_rows, :], other.at[early_rows, :], swap_send.at[0], swap_recv.at[0], sibling
    ).wait_recv()

    @pl.loop(0, messages)
    def _(m):
        @pl.when(m >= split)
        def _():
            swap(m, m - split + 2).wait_recv()

        where = span(m)
        taken = of_row(choices, m, (MESSAGE, cols)) == 1
        value = jnp.where(taken, other[where, :], mine[where, :])
        out_depth[where, :] = jnp.where(inside, value, edge_wide[where, :])

    @pl.when((lead_left == 1) | (follow_left == 1))
    def _():
        halo_to_left.wait_send()

    @pl.when((lead_right == 1) | (follow_right == 1))
    def _():
        halo_to_right.wait_send()

    edge_raw(middle).wait_send()
    edge_swap.wait_send()

    remote(first, inbox.at[0], raw_send.at[0], in_recv.at[0, 0], toward).wait_send()
    remote(mine, other, swap_send.at[0], swap_recv.at[0], sibling).wait_send()

    @pl.when(is_middle)
    def _():
        edge_relay.wait_send()
        edge_return(plane_slot, edge_give).wait_send()
        remote(inbox.at[0], inbox.at[2], relay_send.at[0], in_recv.at[2, 0], toward).wait_send()
        remote(turn, back.at[0], back_send.at[0], in_recv.at[0, 0], outward).wait_send()


def flush(fields_ref, depth_ref, out_fields, out_depth, sem):
    copies = [
        pltpu.make_async_copy(depth_ref, out_depth, sem.at[3]),
    ] + [
        pltpu.make_async_copy(fields_ref.at[plane], out_fields.at[plane], sem.at[plane])
        for plane in range(3)
    ]
    for copy in copies:
        copy.start()
    for copy in copies:
        copy.wait()


def solution(mesh):
    axis = "gx"
    count = mesh.shape[axis]

    def body(fields, friction, wet_mask, owner_table):
        rows, cols = friction.shape
        padded = rows + 2 * PAD
        slots = rows // MESSAGE + 1
        f32 = jnp.float32
        whole = pltpu.VMEM((rows, cols), f32)
        small = pltpu.VMEM((8, cols), f32)
        scratch = [
            pltpu.VMEM((3, padded, cols), f32),
            pltpu.VMEM((padded, cols), f32),
            pltpu.VMEM((padded, cols), jnp.int32),
            pltpu.SMEM(owner_table.shape, jnp.int32),
            whole,
            pltpu.VMEM((3, rows, cols), f32),
            pltpu.VMEM((2, rows, cols), f32),
            whole,
            whole,
            whole,
            whole,
            whole,
            pltpu.VMEM((32, rows), f32),
            pltpu.VMEM((16, rows), f32),
            pltpu.VMEM((16, rows), f32),
            pltpu.VMEM((4, 16, rows), f32),
            pltpu.VMEM((LANES, rows), f32),
            small,
            pltpu.VMEM((3, 8, cols), f32),
            pltpu.VMEM((2, 8, cols), f32),
            small,
            small,
            small,
            small,
            small,
            pltpu.VMEM((LANES, cols), f32),
            whole,
            pltpu.SemaphoreType.DMA((2, 3)),
            pltpu.SemaphoreType.DMA,
            pltpu.SemaphoreType.DMA((2,)),
            pltpu.SemaphoreType.DMA((2,)),
            pltpu.SemaphoreType.DMA((3, slots)),
            pltpu.SemaphoreType.DMA((2,)),
            pltpu.SemaphoreType.DMA((2,)),
            pltpu.SemaphoreType.DMA((2 + DIRECT,)),
            pltpu.SemaphoreType.DMA((2,)),
            pltpu.SemaphoreType.DMA((2,)),
            pltpu.SemaphoreType.REGULAR,
        ]
        arrays = [
            pltpu.with_memory_space_constraint(array, pltpu.HBM)
            for array in (fields, friction, wet_mask, owner_table)
        ]
        results = pl.pallas_call(
            functools.partial(kernel, axis, count),
            out_shape=(
                jax.ShapeDtypeStruct(fields.shape, f32),
                jax.ShapeDtypeStruct(friction.shape, f32),
            ),
            in_specs=[pl.BlockSpec(memory_space=pltpu.HBM)] * 4,
            out_specs=(
                pl.BlockSpec(memory_space=pltpu.VMEM),
                pl.BlockSpec(memory_space=pltpu.VMEM),
            ),
            scratch_shapes=scratch,
            compiler_params=pltpu.CompilerParams(
                collective_id=0, has_side_effects=True, vmem_limit_bytes=32 * 2**20
            ),
            name="shallow_water",
        )(*arrays)
        return pl.pallas_call(
            flush,
            out_shape=(
                jax.ShapeDtypeStruct(fields.shape, f32),
                jax.ShapeDtypeStruct(friction.shape, f32),
            ),
            in_specs=[pl.BlockSpec(memory_space=pltpu.VMEM)] * 2,
            out_specs=(
                pl.BlockSpec(memory_space=pltpu.HBM),
                pl.BlockSpec(memory_space=pltpu.HBM),
            ),
            scratch_shapes=[pltpu.SemaphoreType.DMA((4,))],
            compiler_params=pltpu.CompilerParams(vmem_limit_bytes=32 * 2**20),
            name="flush",
        )(*results)

    in_specs = (P(None, "groups", axis), P("groups", axis), P("groups", axis), P("groups", None))
    out_specs = (P(None, "groups", axis), P("groups", axis))
    return jax.shard_map(body, mesh=mesh, in_specs=in_specs, out_specs=out_specs, check_vma=False)
```

```python
import functools

import jax
import jax.numpy as jnp
from jax import lax
from jax.experimental import pallas as pl
from jax.experimental.pallas import tpu as pltpu
from jax.sharding import PartitionSpec as P

STEPS = 2
PAD = 8
CHUNK = 64
MESSAGE = 32
LAG = 8
AHEAD = 8
DIRECT = 4
FIRST = 80
LANES = 128

gravity_half = 0.5
depth_floor = 0.25
flux_factor = 0.1
time_step = 0.25


def advance(state, wet, damping, east, west, south, north):
    h, p, q = state
    inverse = 1.0 / jnp.maximum(h, depth_floor)
    u = p * inverse
    v = q * inverse
    pressure = gravity_half * h * h
    cross = q * u
    flux_p = p * u + pressure
    flux_q = q * v + pressure

    def gather(cell, flux_east, flux_south):
        quarter = 0.25 * cell
        along = flux_factor * flux_east
        down = flux_factor * flux_south
        return (east(quarter - along) + west(quarter + along)) + (
            south(quarter - down) + north(quarter + down)
        )

    return (
        wet * gather(h, p, q),
        damping * gather(p, flux_p, cross),
        damping * gather(q, cross, flux_q),
    )


def masks(openness):
    wet = jnp.where(openness > 0.0, 1.0, 0.0)
    return wet, wet / (1.0 + time_step * openness)


def kernel(
    axis,
    count,
    fields_ref,
    friction_ref,
    wet_ref,
    owner_ref,
    out_fields,
    out_depth,
    state,
    fric,
    mask,
    owner,
    first,
    inbox,
    back,
    turn,
    near_out,
    far_out,
    mine,
    other,
    packed,
    outer,
    halo_left,
    halo_right,
    edge,
    edge_turn,
    edge_first,
    edge_in,
    edge_back,
    edge_give,
    edge_near,
    edge_far,
    edge_mine,
    edge_other,
    edge_final,
    edge_wide,
    load_sem,
    table_sem,
    raw_send,
    relay_send,
    in_recv,
    back_send,
    swap_send,
    swap_recv,
    halo_send,
    halo_recv,
    hello,
):
    rows, cols = friction_ref.shape
    tile = cols
    tile_rows = rows // tile
    messages = rows // MESSAGE
    split = messages - DIRECT
    chunks = rows // CHUNK
    extra = messages
    MESH = pl.DeviceIdType.MESH

    me = lax.axis_index(axis)
    odd = me % 2
    position = me % 8
    chip = position // 2
    middle = ((chip + 1) // 2) % 2
    toward = me + 2 - 4 * (chip // 2)
    outward = 2 * me - toward
    sibling = me + 1 - 2 * odd
    keeper = me - position + 1
    is_keeper = position == 1
    is_leaf = position == 0
    is_third = chip == 2
    is_middle = middle == 1
    is_end = middle == 0

    last = jnp.where(me == count - 1, 1, 0)
    parity = (me // 8) % 2
    lead_left = jnp.where(position == 0, parity, jnp.where(position == 6, 1, 0))
    lead_left = jnp.where(me == 0, 0, lead_left)
    follow_left = jnp.where(me == 0, 0, 1 - lead_left)
    lead_right = jnp.where(position == 7, parity, jnp.where(position == 5, 0, 1)) * (1 - last)
    follow_right = (1 - last) * (1 - lead_right)

    def load(number):
        start, size = ((0, FIRST), (FIRST, rows - FIRST))[number]
        here = pl.ds(start, size)
        there = pl.ds(start + PAD, size)
        return [
            pltpu.make_async_copy(
                fields_ref.at[:, here, :], state.at[:, there, :], load_sem.at[number, 0]
            ),
            pltpu.make_async_copy(friction_ref.at[here, :], fric.at[there, :], load_sem.at[number, 1]),
            pltpu.make_async_copy(wet_ref.at[here, :], mask.at[there, :], load_sem.at[number, 2]),
        ]

    def await_load(number):
        for copy in load(number):
            copy.wait()

    table = pltpu.make_async_copy(owner_ref, owner, table_sem)
    for copy in load(0):
        copy.start()

    barrier = pltpu.get_barrier_semaphore()

    def greet(peer):
        pl.semaphore_signal(barrier, inc=1, device_id={axis: peer}, device_id_type=MESH)

    @pl.when(is_middle)
    def _():
        greet(outward)
        greet(toward)

    @pl.when(is_third)
    def _():
        greet(keeper)

    @pl.when(follow_left == 1)
    def _():
        greet(me - 1)

    @pl.when(follow_right == 1)
    def _():
        greet(me + 1)

    zero_rows = jnp.zeros((PAD, cols), jnp.float32)
    for start in (0, PAD + rows):
        for plane in range(3):
            state[plane, start : start + PAD, :] = zero_rows
        fric[start : start + PAD, :] = zero_rows
        mask[start : start + PAD, :] = jnp.zeros((PAD, cols), jnp.int32)
    for copy in load(1):
        copy.start()
    table.start()
    edge[...] = jnp.zeros_like(edge)
    edge_turn[...] = jnp.zeros_like(edge_turn)
    edge_final[...] = jnp.zeros_like(edge_final)

    def differs(tile_row, bit):
        own = owner[tile_row, me]
        return (own // 2 ** bit + me // 2 ** bit) % 2

    def remote(src, dst, send, recv, peer):
        return pltpu.make_async_remote_copy(
            src_ref=src,
            dst_ref=dst,
            send_sem=send,
            recv_sem=recv,
            device_id={axis: peer},
            device_id_type=MESH,
        )

    def span(m):
        return pl.ds(pl.multiple_of(m * MESSAGE, MESSAGE), MESSAGE)

    def raw(m, slot):
        return remote(
            first.at[span(m), :], inbox.at[slot, span(m), :], raw_send.at[0], in_recv.at[slot, m], toward
        )

    def relay(m):
        return remote(
            inbox.at[0, span(m), :], inbox.at[2, span(m), :], relay_send.at[0], in_recv.at[2, m], toward
        )

    plane_slot = jnp.where(chip == 1, odd, 0)
    receiver = jnp.where(chip == 1, keeper, outward)

    def give(m, source, slot):
        return remote(
            source.at[span(m), :],
            back.at[slot, span(m), :],
            back_send.at[0],
            in_recv.at[slot, m],
            receiver,
        )

    def near_direct(m):
        return remote(
            near_out.at[span(m), :], inbox.at[1, span(m), :], raw_send.at[0], in_recv.at[1, m], me - 2
        )

    def far_direct(m, core):
        return remote(
            far_out.at[span(m), :],
            inbox.at[1 + core, span(m), :],
            relay_send.at[0],
            in_recv.at[2, m - (1 - core) * split],
            keeper,
        )

    def pass_back(m, slot):
        return remote(
            near_out.at[span(m), :], other.at[span(m), :], swap_send.at[0], swap_recv.at[slot], sibling
        )

    def swap(m, slot):
        return remote(
            mine.at[span(m), :], other.at[span(m), :], swap_send.at[0], swap_recv.at[slot], sibling
        )

    def edge_raw(slot):
        return remote(edge_first, edge_in.at[slot], raw_send.at[1], in_recv.at[slot, extra], toward)

    edge_relay = remote(
        edge_in.at[0], edge_in.at[2], relay_send.at[1], in_recv.at[2, extra], toward
    )

    def edge_return(slot, source):
        return remote(source, edge_back.at[slot], back_send.at[1], in_recv.at[slot, extra], receiver)

    edge_near_direct = remote(
        edge_near, edge_in.at[1], raw_send.at[1], in_recv.at[1, extra], me - 2
    )

    def edge_far_direct(core):
        return remote(
            edge_far,
            edge_in.at[1 + core],
            relay_send.at[1],
            in_recv.at[2, extra - (1 - core) * split],
            keeper,
        )

    edge_pass = remote(edge_near, edge_other, swap_send.at[1], swap_recv.at[1], sibling)
    edge_swap = remote(edge_mine, edge_other, swap_send.at[1], swap_recv.at[1], sibling)

    halo_to_left = remote(
        outer.at[pl.ds(0, 8), :], halo_right, halo_send.at[0], halo_recv.at[0], me - 1
    )
    halo_to_right = remote(
        outer.at[pl.ds(8, 8), :], halo_left, halo_send.at[1], halo_recv.at[1], me + 1
    )

    def shift(axis_number, amount, size):
        return lambda a: pltpu.roll(a, amount % size, axis_number)

    def compute(at, size):
        reach = size + 2 * PAD
        where = pl.ds(at, reach)
        openness = mask[where, :].astype(jnp.float32) * fric[where, :]
        wet, damping = masks(openness)
        values = tuple(state[plane, where, :] * wet for plane in range(3))
        for _ in range(STEPS):
            values = advance(
                values,
                wet,
                damping,
                shift(1, -1, cols),
                shift(1, 1, cols),
                shift(0, -1, reach),
                shift(0, 1, reach),
            )
        here = pl.ds(at, size)
        first[here, :] = values[0][PAD : PAD + size]
        for plane in range(3):
            out_fields[plane, here, :] = values[plane][PAD : PAD + size]

    def for_end(by, own, near, far):
        return jnp.where(by == 3, far, jnp.where(by == 2, near, own))

    def for_middle(by, own, end, near, far):
        return jnp.where(by == 3, near, jnp.where(by == 2, far, jnp.where(by == 1, end, own)))

    def of_row(pair, m, shape):
        value = pair[-1]
        for tile_row in reversed(range(tile_rows - 1)):
            value = jnp.where(m < (tile_row + 1) * (tile // MESSAGE), pair[tile_row], value)
        return jnp.full(shape, value, jnp.int32)

    def send_chunk(number):
        for part in range(CHUNK // MESSAGE):
            raw(number * (CHUNK // MESSAGE) + part, middle).start()

    @pl.when(is_keeper)
    def _():
        pl.semaphore_wait(barrier, 3 + lead_left + lead_right)
        for ahead in range(1, 5):
            pl.semaphore_signal(hello, inc=1, device_id={axis: me + ahead}, device_id_type=MESH)

    await_load(0)
    compute(0, MESSAGE)

    @pl.when(position != 1)
    def _():
        pl.semaphore_wait(barrier, 1 + lead_left + lead_right)

    raw(0, middle).start()
    for part in range(1, CHUNK // MESSAGE):
        compute(part * MESSAGE, MESSAGE)
        raw(part, middle).start()
    await_load(1)
    table.wait()
    moves = [differs(tile_row, 1) + 2 * differs(tile_row, 2) for tile_row in range(tile_rows)]
    flips = [differs(tile_row, 0) for tile_row in range(tile_rows)]

    compute(CHUNK, CHUNK)
    send_chunk(1)

    lane = lax.broadcasted_iota(jnp.int32, (LANES, LANES), 1)

    @pl.loop(0, rows // LANES)
    def _(block):
        where = pl.ds(pl.multiple_of(PAD + block * LANES, PAD), LANES)
        result = jnp.zeros((LANES, LANES), jnp.float32)
        for side, low in enumerate((0, cols - LANES)):
            cut = pl.ds(low, LANES)
            openness = mask[where, cut].astype(jnp.float32) * fric[where, cut]
            wet = jnp.where(openness > 0.0, 1.0, 0.0)
            planes = [state[plane, where, cut] * wet for plane in range(3)] + [openness]
            for number, values in enumerate(planes):
                source = (LANES - 4) * side
                target = 16 * side + 4 * number
                moved = pltpu.roll(values, (target - source) % LANES, 1)
                result = jnp.where(lane >= target, moved, result)
        turned = result.T[0:32]
        there = pl.ds(pl.multiple_of(block * LANES, LANES), LANES)
        packed[:, there] = turned
        for number in range(4):
            outer[2 * number : 2 * number + 2, there] = turned[4 * number : 4 * number + 2]
            outer[8 + 2 * number : 10 + 2 * number, there] = turned[18 + 4 * number : 20 + 4 * number]

    @pl.when(lead_left == 1)
    def _():
        halo_to_left.start()

    @pl.when(lead_right == 1)
    def _():
        halo_to_right.start()

    @pl.loop(2, chunks)
    def _(j):
        compute(pl.multiple_of(j * CHUNK, CHUNK), CHUNK)

        @pl.when((chip != 2) | (j < split * MESSAGE // CHUNK))
        def _():
            send_chunk(j)

    @pl.when(follow_right == 1)
    def _():
        halo_to_left.wait_recv()
        halo_to_right.start()

    @pl.when(follow_left == 1)
    def _():
        halo_to_right.wait_recv()
        halo_to_left.start()

    def pass_on(m):
        raw(m, 0).wait_recv()
        relay(m).start()

    @pl.when(is_third)
    def _():
        @pl.loop(0, split)
        def _(m):
            pass_on(m)

        @pl.loop(split, messages)
        def _(m):
            raw(m, 0).wait_recv()
            where = span(m)
            by = of_row(moves, m, (MESSAGE, cols))
            near_out[where, :] = jnp.where(by == 3, first[where, :], inbox[0, where, :])
            near_direct(m).start()

    @pl.when(chip == 1)
    def _():
        pl.semaphore_wait(hello, 1)

        @pl.loop(split, messages)
        def _(m):
            give(m, first, plane_slot).start()

    @pl.when(lead_right == 1)
    def _():
        halo_to_left.wait_recv()

    @pl.when(lead_left == 1)
    def _():
        halo_to_right.wait_recv()

    for number in range(4):
        base = 4 * number
        pair = pl.ds(2 * number, 2)
        edge[number, 0:2, :] = jnp.where(me > 0, halo_left[pair, :], 0.0)
        edge[number, 2:6, :] = packed[base : base + 4, :]
        edge[number, 8:12, :] = packed[16 + base : 20 + base, :]
        edge[number, 12:14, :] = jnp.where(me < count - 1, halo_right[pair, :], 0.0)

    place = lax.broadcasted_iota(jnp.int32, (16, rows), 1)
    wet, damping = masks(edge[3])
    values = tuple(edge[plane] for plane in range(3))
    for _ in range(STEPS):
        values = advance(
            values,
            wet,
            damping,
            shift(0, -1, 16),
            shift(0, 1, 16),
            lambda a: jnp.where(place == rows - 1, 0.0, pltpu.roll(a, rows - 1, 1)),
            lambda a: jnp.where(place == 0, 0.0, pltpu.roll(a, 1, 1)),
        )
    for plane in range(3):
        edge_turn[16 * plane : 16 * plane + 16, :] = values[plane]
    for tile_row in range(tile_rows):
        cut = pl.ds(tile_row * tile, tile)
        edge_first[4 * tile_row : 4 * tile_row + 2, :] = edge_turn[2:4, cut]
        edge_first[4 * tile_row + 2 : 4 * tile_row + 4, :] = edge_turn[10:12, cut]

    @pl.when(chip != 2)
    def _():
        edge_raw(middle).start()

    @pl.when(chip == 1)
    def _():
        edge_return(plane_slot, edge_first).start()

    line = lax.broadcasted_iota(jnp.int32, (8, cols), 0)

    def by_line(pair):
        value = jnp.full((8, cols), pair[-1], jnp.int32)
        for tile_row in reversed(range(tile_rows - 1)):
            value = jnp.where(line < 4 * (tile_row + 1), pair[tile_row], value)
        return value

    edge_by = by_line(moves)

    def return_second(m):
        where = span(m)
        by = of_row(moves, m, (MESSAGE, cols))
        raw(m, 1).wait_recv()
        relay(m).wait_recv()
        turn[where, :] = for_end(by, first[where, :], inbox[1, where, :], inbox[2, where, :])
        give(m, turn, plane_slot).start()

    def settle_second(m, late):
        where = span(m)
        by = of_row(moves, m, (MESSAGE, cols))
        if late:
            raw(m, 1).wait_recv()
        own = first[where, :]
        end = inbox[0, where, :]
        near = inbox[1, where, :]
        if late:
            mine[where, :] = jnp.where(by >= 2, near, jnp.where(by == 1, end, own))
        else:
            mine[where, :] = for_middle(by, own, end, near, inbox[2, where, :])
        swap(m, m - split + 2 if late else 0).start()

    @pl.when(is_third)
    def _():
        edge_raw(0).wait_recv()
        edge_near[...] = jnp.where(edge_by == 3, edge_first[...], edge_in[0])
        edge_near_direct.start()
        pl.semaphore_wait(hello, 1)
        edge_far[...] = jnp.where(edge_by == 2, edge_first[...], edge_in[0])
        edge_far_direct(odd).start()

        @pl.loop(split, messages)
        def _(m):
            where = span(m)
            by = of_row(moves, m, (MESSAGE, cols))
            far_out[where, :] = jnp.where(by == 2, first[where, :], inbox[0, where, :])
            far_direct(m, odd).start()

    def edge_relays():
        edge_raw(0).wait_recv()
        edge_relay.start()

    @pl.when((chip == 1) & (odd == 0))
    def _():
        @pl.loop(0, AHEAD)
        def _(m):
            return_second(m)

        @pl.loop(0, split - AHEAD)
        def _(m):
            pass_on(m)
            return_second(m + AHEAD)

        @pl.loop(split - AHEAD, messages - 2)
        def _(m):
            pass_on(m)

        edge_relays()
        for m in range(messages - 2, messages):
            pass_on(m)

    @pl.when((chip == 1) & (odd == 1))
    def _():
        @pl.loop(0, LAG)
        def _(m):
            pass_on(m)

        @pl.loop(0, messages - LAG)
        def _(m):
            return_second(m)
            pass_on(m + LAG)

        @pl.loop(messages - LAG, split)
        def _(m):
            return_second(m)

        edge_relays()

    @pl.when(chip == 1)
    def _():
        @pl.loop(0, split)
        def _(m):
            settle_second(m, False)

    def patch_fields():
        @pl.loop(0, rows // LANES)
        def _(block):
            where = pl.ds(pl.multiple_of(block * LANES, LANES), LANES)
            turned = edge_turn[:, where].T
            for plane in range(3):
                on_left = pltpu.roll(turned, (-16 * plane - 2) % LANES, 1)
                cut = pl.ds(0, LANES)
                out_fields[plane, where, cut] = jnp.where(
                    lane < 2, on_left, out_fields[plane, where, cut]
                )
                on_right = pltpu.roll(turned, (LANES - 2 - 16 * plane - 10) % LANES, 1)
                cut = pl.ds(cols - LANES, LANES)
                out_fields[plane, where, cut] = jnp.where(
                    lane >= LANES - 2, on_right, out_fields[plane, where, cut]
                )

    @pl.when(is_end)
    def _():
        patch_fields()

    def settle(m, late):
        where = span(m)
        by = of_row(moves, m, (MESSAGE, cols))
        slot = m - split + 2 if late else 0

        @pl.when(is_third)
        def _():
            raw(m, 1).wait_recv()
            relay(m).wait_recv()
            own = first[where, :]
            near = inbox[1, where, :]
            far = inbox[2, where, :]
            turn[where, :] = for_end(by, own, near, far)
            give(m, turn, 0).start()
            mine[where, :] = for_middle(by, own, inbox[0, where, :], near, far)
            swap(m, slot).start()

        @pl.when(is_leaf)
        def _():
            mine[where, :] = first[where, :]
            swap(m, slot).start()

        @pl.when(is_keeper)
        def _():
            flipped = of_row(flips, m, (MESSAGE, cols)) == 1
            parts = []
            for core in range(2):
                give(m, turn, core).wait_recv()
                part = back[core, where, :]
                if late:
                    far_direct(m, core).wait_recv()
                    part = jnp.where(by >= 2, inbox[1 + core, where, :], part)
                parts.append(part)
            settled = jnp.where(by == 0, first[where, :], parts[1])
            near_out[where, :] = jnp.where(flipped, settled, parts[0])
            pass_back(m, slot).start()
            mine[where, :] = jnp.where(flipped, parts[0], settled)

        @pl.when(chip == 3)
        def _():
            give(m, turn, 0).wait_recv()
            mine[where, :] = jnp.where(by == 0, first[where, :], back[0, where, :])
            swap(m, slot).start()

    @pl.when(chip != 1)
    def _():
        @pl.loop(0, split)
        def _(m):
            settle(m, False)

    def settle_edges():
        @pl.when(is_third)
        def _():
            edge_raw(1).wait_recv()
            edge_relay.wait_recv()
            own = edge_first[...]
            near = edge_in[1]
            far = edge_in[2]
            edge_give[...] = for_end(edge_by, own, near, far)
            edge_return(0, edge_give).start()
            edge_mine[...] = for_middle(edge_by, own, edge_in[0], near, far)
            edge_swap.start()

        @pl.when(chip == 1)
        def _():
            edge_raw(1).wait_recv()
            end_or_own = jnp.where(edge_by == 1, edge_in[0], edge_first[...])
            edge_mine[...] = jnp.where(edge_by >= 2, edge_in[1], end_or_own)
            edge_swap.start()

        @pl.when(is_leaf)
        def _():
            edge_mine[...] = edge_first[...]
            edge_swap.start()

        @pl.when(is_keeper)
        def _():
            parts = []
            for core in range(2):
                edge_return(core, edge_give).wait_recv()
                edge_far_direct(core).wait_recv()
                parts.append(jnp.where(edge_by >= 2, edge_in[1 + core], edge_back[core]))
            flipped = by_line(flips) == 1
            settled = jnp.where(edge_by == 0, edge_first[...], parts[1])
            edge_near[...] = jnp.where(flipped, settled, parts[0])
            edge_pass.start()
            edge_mine[...] = jnp.where(flipped, parts[0], settled)

        @pl.when(chip == 3)
        def _():
            edge_return(0, edge_give).wait_recv()
            edge_mine[...] = jnp.where(edge_by == 0, edge_first[...], edge_back[0])
            edge_swap.start()

    choices = []
    for tile_row in range(tile_rows):
        still = jnp.where(moves[tile_row] == 0, 1, 0)
        flipped = flips[tile_row]
        choice = jnp.where(is_keeper, flipped * still, flipped)
        choices.append(jnp.where(is_leaf, 1 - (1 - flipped) * still, choice))

    column = lax.broadcasted_iota(jnp.int32, (MESSAGE, cols), 1)
    inside = (column >= 2) & (column < cols - 2)

    def deliver(m):
        where = span(m)
        taken = of_row(choices, m, (MESSAGE, cols)) == 1
        value = jnp.where(taken, other[where, :], mine[where, :])
        out_depth[where, :] = jnp.where(inside, value, edge_wide[where, :])

    def deliver_early():
        edge_swap.wait_recv()
        edge_final[0:8, :] = jnp.where(by_line(choices) == 1, edge_other[...], edge_mine[...])
        for tile_row in range(tile_rows):
            for block in range(tile // LANES):
                turned = edge_final[:, block * LANES : (block + 1) * LANES].T
                where = pl.ds(tile_row * tile + block * LANES, LANES)
                edge_wide[where, 0:LANES] = pltpu.roll(turned, (-4 * tile_row) % LANES, 1)
                edge_wide[where, cols - LANES : cols] = pltpu.roll(
                    turned, (LANES - 2 - 4 * tile_row - 2) % LANES, 1
                )
        early_rows = pl.ds(0, split * MESSAGE)
        remote(
            mine.at[early_rows, :], other.at[early_rows, :], swap_send.at[0], swap_recv.at[0], sibling
        ).wait_recv()

        @pl.loop(0, split)
        def _(m):
            deliver(m)

    @pl.when(chip == 0)
    def _():
        settle_edges()
        deliver_early()

        @pl.loop(split, messages)
        def _(m):
            settle(m, True)

    @pl.when(chip == 1)
    def _():
        settle_edges()

        @pl.loop(split, messages)
        def _(m):
            settle_second(m, True)

        patch_fields()
        deliver_early()

    @pl.when(is_third)
    def _():
        @pl.loop(split, messages - 2)
        def _(m):
            settle(m, True)

        settle_edges()
        for m in range(messages - 2, messages):
            settle(m, True)
        patch_fields()
        deliver_early()

    @pl.when(chip == 3)
    def _():
        @pl.loop(split, messages - 2)
        def _(m):
            settle(m, True)

        settle_edges()
        for m in range(messages - 2, messages):
            settle(m, True)
        deliver_early()

    @pl.loop(split, messages)
    def _(m):
        swap(m, m - split + 2).wait_recv()
        deliver(m)

    @pl.when((lead_left == 1) | (follow_left == 1))
    def _():
        halo_to_left.wait_send()

    @pl.when((lead_right == 1) | (follow_right == 1))
    def _():
        halo_to_right.wait_send()

    edge_raw(middle).wait_send()
    edge_swap.wait_send()

    remote(first, inbox.at[0], raw_send.at[0], in_recv.at[0, 0], toward).wait_send()
    remote(mine, other, swap_send.at[0], swap_recv.at[0], sibling).wait_send()

    @pl.when(is_middle)
    def _():
        edge_relay.wait_send()
        edge_return(plane_slot, edge_give).wait_send()
        remote(inbox.at[0], inbox.at[2], relay_send.at[0], in_recv.at[2, 0], toward).wait_send()
        remote(turn, back.at[0], back_send.at[0], in_recv.at[0, 0], outward).wait_send()


def flush(fields_ref, depth_ref, out_fields, out_depth, sem):
    copies = [
        pltpu.make_async_copy(depth_ref, out_depth, sem.at[3]),
    ] + [
        pltpu.make_async_copy(fields_ref.at[plane], out_fields.at[plane], sem.at[plane])
        for plane in range(3)
    ]
    for copy in copies:
        copy.start()
    for copy in copies:
        copy.wait()


def solution(mesh):
    axis = "gx"
    count = mesh.shape[axis]

    def body(fields, friction, wet_mask, owner_table):
        rows, cols = friction.shape
        padded = rows + 2 * PAD
        slots = rows // MESSAGE + 1
        f32 = jnp.float32
        whole = pltpu.VMEM((rows, cols), f32)
        small = pltpu.VMEM((8, cols), f32)
        scratch = [
            pltpu.VMEM((3, padded, cols), f32),
            pltpu.VMEM((padded, cols), f32),
            pltpu.VMEM((padded, cols), jnp.int32),
            pltpu.SMEM(owner_table.shape, jnp.int32),
            whole,
            pltpu.VMEM((3, rows, cols), f32),
            pltpu.VMEM((2, rows, cols), f32),
            whole,
            whole,
            whole,
            whole,
            whole,
            pltpu.VMEM((32, rows), f32),
            pltpu.VMEM((16, rows), f32),
            pltpu.VMEM((8, rows), f32),
            pltpu.VMEM((8, rows), f32),
            pltpu.VMEM((4, 16, rows), f32),
            pltpu.VMEM((LANES, rows), f32),
            small,
            pltpu.VMEM((3, 8, cols), f32),
            pltpu.VMEM((2, 8, cols), f32),
            small,
            small,
            small,
            small,
            small,
            pltpu.VMEM((LANES, cols), f32),
            whole,
            pltpu.SemaphoreType.DMA((2, 3)),
            pltpu.SemaphoreType.DMA,
            pltpu.SemaphoreType.DMA((2,)),
            pltpu.SemaphoreType.DMA((2,)),
            pltpu.SemaphoreType.DMA((3, slots)),
            pltpu.SemaphoreType.DMA((2,)),
            pltpu.SemaphoreType.DMA((2,)),
            pltpu.SemaphoreType.DMA((2 + DIRECT,)),
            pltpu.SemaphoreType.DMA((2,)),
            pltpu.SemaphoreType.DMA((2,)),
            pltpu.SemaphoreType.REGULAR,
        ]
        arrays = [
            pltpu.with_memory_space_constraint(array, pltpu.HBM)
            for array in (fields, friction, wet_mask, owner_table)
        ]
        results = pl.pallas_call(
            functools.partial(kernel, axis, count),
            out_shape=(
                jax.ShapeDtypeStruct(fields.shape, f32),
                jax.ShapeDtypeStruct(friction.shape, f32),
            ),
            in_specs=[pl.BlockSpec(memory_space=pltpu.HBM)] * 4,
            out_specs=(
                pl.BlockSpec(memory_space=pltpu.VMEM),
                pl.BlockSpec(memory_space=pltpu.VMEM),
            ),
            scratch_shapes=scratch,
            compiler_params=pltpu.CompilerParams(
                collective_id=0, has_side_effects=True, vmem_limit_bytes=32 * 2**20
            ),
            name="shallow_water",
        )(*arrays)
        return pl.pallas_call(
            flush,
            out_shape=(
                jax.ShapeDtypeStruct(fields.shape, f32),
                jax.ShapeDtypeStruct(friction.shape, f32),
            ),
            in_specs=[pl.BlockSpec(memory_space=pltpu.VMEM)] * 2,
            out_specs=(
                pl.BlockSpec(memory_space=pltpu.HBM),
                pl.BlockSpec(memory_space=pltpu.HBM),
            ),
            scratch_shapes=[pltpu.SemaphoreType.DMA((4,))],
            compiler_params=pltpu.CompilerParams(vmem_limit_bytes=32 * 2**20),
            name="flush",
        )(*results)

    in_specs = (P(None, "groups", axis), P("groups", axis), P("groups", axis), P("groups", None))
    out_specs = (P(None, "groups", axis), P("groups", axis))
    return jax.shard_map(body, mesh=mesh, in_specs=in_specs, out_specs=out_specs, check_vma=False)
```

```python
import functools

import jax
import jax.numpy as jnp
from jax import lax
from jax.experimental import pallas as pl
from jax.experimental.pallas import tpu as pltpu
from jax.sharding import PartitionSpec as P

STEPS = 2
PAD = 8
CHUNK = 64
MESSAGE = 32
LAG = 8
AHEAD = 8
DIRECT = 4
FIRST = 80
LANES = 128

gravity_half = 0.5
depth_floor = 0.25
flux_factor = 0.1
time_step = 0.25


def advance(state, wet, damping, east, west, south, north):
    h, p, q = state
    inverse = 1.0 / jnp.maximum(h, depth_floor)
    u = p * inverse
    v = q * inverse
    pressure = gravity_half * h * h
    cross = q * u
    flux_p = p * u + pressure
    flux_q = q * v + pressure

    def gather(cell, flux_east, flux_south):
        quarter = 0.25 * cell
        along = flux_factor * flux_east
        down = flux_factor * flux_south
        return (east(quarter - along) + west(quarter + along)) + (
            south(quarter - down) + north(quarter + down)
        )

    return (
        wet * gather(h, p, q),
        damping * gather(p, flux_p, cross),
        damping * gather(q, cross, flux_q),
    )


def masks(openness):
    wet = jnp.where(openness > 0.0, 1.0, 0.0)
    return wet, wet / (1.0 + time_step * openness)


def kernel(
    axis,
    count,
    fields_ref,
    friction_ref,
    wet_ref,
    owner_ref,
    out_fields,
    out_depth,
    state,
    fric,
    mask,
    owner,
    first,
    inbox,
    back,
    turn,
    near_out,
    far_out,
    mine,
    other,
    packed,
    outer,
    halo_left,
    halo_right,
    edge,
    edge_turn,
    edge_first,
    edge_in,
    edge_back,
    edge_give,
    edge_near,
    edge_far,
    edge_mine,
    edge_other,
    edge_final,
    edge_wide,
    load_sem,
    table_sem,
    raw_send,
    relay_send,
    in_recv,
    back_send,
    swap_send,
    swap_recv,
    halo_send,
    halo_recv,
    hello,
):
    rows, cols = friction_ref.shape
    tile = cols
    tile_rows = rows // tile
    messages = rows // MESSAGE
    split = messages - DIRECT
    chunks = rows // CHUNK
    extra = messages
    MESH = pl.DeviceIdType.MESH

    me = lax.axis_index(axis)
    odd = me % 2
    position = me % 8
    chip = position // 2
    middle = ((chip + 1) // 2) % 2
    toward = me + 2 - 4 * (chip // 2)
    outward = 2 * me - toward
    sibling = me + 1 - 2 * odd
    keeper = me - position + 1
    is_keeper = position == 1
    is_leaf = position == 0
    is_third = chip == 2
    is_middle = middle == 1
    is_end = middle == 0

    last = jnp.where(me == count - 1, 1, 0)
    parity = (me // 8) % 2
    lead_left = jnp.where(position == 0, parity, jnp.where(position == 6, 1, 0))
    lead_left = jnp.where(me == 0, 0, lead_left)
    follow_left = jnp.where(me == 0, 0, 1 - lead_left)
    lead_right = jnp.where(position == 7, parity, jnp.where(position == 5, 0, 1)) * (1 - last)
    follow_right = (1 - last) * (1 - lead_right)

    def load(number):
        start, size = ((0, FIRST), (FIRST, rows - FIRST))[number]
        here = pl.ds(start, size)
        there = pl.ds(start + PAD, size)
        return [
            pltpu.make_async_copy(
                fields_ref.at[:, here, :], state.at[:, there, :], load_sem.at[number, 0]
            ),
            pltpu.make_async_copy(friction_ref.at[here, :], fric.at[there, :], load_sem.at[number, 1]),
            pltpu.make_async_copy(wet_ref.at[here, :], mask.at[there, :], load_sem.at[number, 2]),
        ]

    def await_load(number):
        for copy in load(number):
            copy.wait()

    table = pltpu.make_async_copy(owner_ref, owner, table_sem)
    for copy in load(0):
        copy.start()

    barrier = pltpu.get_barrier_semaphore()

    def greet(peer):
        pl.semaphore_signal(barrier, inc=1, device_id={axis: peer}, device_id_type=MESH)

    @pl.when(is_middle)
    def _():
        greet(outward)
        greet(toward)

    @pl.when(is_third)
    def _():
        greet(keeper)

    @pl.when(follow_left == 1)
    def _():
        greet(me - 1)

    @pl.when(follow_right == 1)
    def _():
        greet(me + 1)

    zero_rows = jnp.zeros((PAD, cols), jnp.float32)
    for start in (0, PAD + rows):
        for plane in range(3):
            state[plane, start : start + PAD, :] = zero_rows
        fric[start : start + PAD, :] = zero_rows
        mask[start : start + PAD, :] = jnp.zeros((PAD, cols), jnp.int32)
    for copy in load(1):
        copy.start()
    table.start()
    edge[...] = jnp.zeros_like(edge)
    edge_turn[...] = jnp.zeros_like(edge_turn)
    edge_final[...] = jnp.zeros_like(edge_final)

    def differs(tile_row, bit):
        own = owner[tile_row, me]
        return (own // 2 ** bit + me // 2 ** bit) % 2

    def remote(src, dst, send, recv, peer):
        return pltpu.make_async_remote_copy(
            src_ref=src,
            dst_ref=dst,
            send_sem=send,
            recv_sem=recv,
            device_id={axis: peer},
            device_id_type=MESH,
        )

    def span(m):
        return pl.ds(pl.multiple_of(m * MESSAGE, MESSAGE), MESSAGE)

    def raw(m, slot):
        return remote(
            first.at[span(m), :], inbox.at[slot, span(m), :], raw_send.at[0], in_recv.at[slot, m], toward
        )

    def relay(m):
        return remote(
            inbox.at[0, span(m), :], inbox.at[2, span(m), :], relay_send.at[0], in_recv.at[2, m], toward
        )

    plane_slot = jnp.where(chip == 1, odd, 0)
    receiver = jnp.where(chip == 1, keeper, outward)

    def give(m, source, slot):
        return remote(
            source.at[span(m), :],
            back.at[slot, span(m), :],
            back_send.at[0],
            in_recv.at[slot, m],
            receiver,
        )

    def near_direct(m):
        return remote(
            near_out.at[span(m), :], inbox.at[1, span(m), :], raw_send.at[0], in_recv.at[1, m], me - 2
        )

    def far_direct(m, core):
        return remote(
            far_out.at[span(m), :],
            inbox.at[1 + core, span(m), :],
            relay_send.at[0],
            in_recv.at[2, m - (1 - core) * split],
            keeper,
        )

    def pass_back(m, slot):
        return remote(
            near_out.at[span(m), :], other.at[span(m), :], swap_send.at[0], swap_recv.at[slot], sibling
        )

    def swap(m, slot):
        return remote(
            mine.at[span(m), :], other.at[span(m), :], swap_send.at[0], swap_recv.at[slot], sibling
        )

    def edge_raw(slot):
        return remote(edge_first, edge_in.at[slot], raw_send.at[1], in_recv.at[slot, extra], toward)

    edge_relay = remote(
        edge_in.at[0], edge_in.at[2], relay_send.at[1], in_recv.at[2, extra], toward
    )

    def edge_return(slot, source):
        return remote(source, edge_back.at[slot], back_send.at[1], in_recv.at[slot, extra], receiver)

    edge_near_direct = remote(
        edge_near, edge_in.at[1], raw_send.at[1], in_recv.at[1, extra], me - 2
    )

    def edge_far_direct(core):
        return remote(
            edge_far,
            edge_in.at[1 + core],
            relay_send.at[1],
            in_recv.at[2, extra - (1 - core) * split],
            keeper,
        )

    edge_pass = remote(edge_near, edge_other, swap_send.at[1], swap_recv.at[1], sibling)
    edge_swap = remote(edge_mine, edge_other, swap_send.at[1], swap_recv.at[1], sibling)

    halo_to_left = remote(
        outer.at[pl.ds(0, 8), :], halo_right, halo_send.at[0], halo_recv.at[0], me - 1
    )
    halo_to_right = remote(
        outer.at[pl.ds(8, 8), :], halo_left, halo_send.at[1], halo_recv.at[1], me + 1
    )

    def shift(axis_number, amount, size):
        return lambda a: pltpu.roll(a, amount % size, axis_number)

    def compute(at, size):
        reach = size + 2 * PAD
        where = pl.ds(at, reach)
        openness = mask[where, :].astype(jnp.float32) * fric[where, :]
        wet, damping = masks(openness)
        values = tuple(state[plane, where, :] * wet for plane in range(3))
        for _ in range(STEPS):
            values = advance(
                values,
                wet,
                damping,
                shift(1, -1, cols),
                shift(1, 1, cols),
                shift(0, -1, reach),
                shift(0, 1, reach),
            )
        here = pl.ds(at, size)
        first[here, :] = values[0][PAD : PAD + size]
        for plane in range(3):
            out_fields[plane, here, :] = values[plane][PAD : PAD + size]

    def for_end(by, own, near, far):
        return jnp.where(by == 3, far, jnp.where(by == 2, near, own))

    def for_middle(by, own, end, near, far):
        return jnp.where(by == 3, near, jnp.where(by == 2, far, jnp.where(by == 1, end, own)))

    def of_row(pair, m, shape):
        value = pair[-1]
        for tile_row in reversed(range(tile_rows - 1)):
            value = jnp.where(m < (tile_row + 1) * (tile // MESSAGE), pair[tile_row], value)
        return jnp.full(shape, value, jnp.int32)

    def send_chunk(number):
        for part in range(CHUNK // MESSAGE):
            raw(number * (CHUNK // MESSAGE) + part, middle).start()

    @pl.when(is_keeper)
    def _():
        pl.semaphore_wait(barrier, 3 + lead_left + lead_right)
        for ahead in range(1, 5):
            pl.semaphore_signal(hello, inc=1, device_id={axis: me + ahead}, device_id_type=MESH)

    await_load(0)
    compute(0, MESSAGE)

    @pl.when(position != 1)
    def _():
        pl.semaphore_wait(barrier, 1 + lead_left + lead_right)

    raw(0, middle).start()
    for part in range(1, CHUNK // MESSAGE):
        compute(part * MESSAGE, MESSAGE)
        raw(part, middle).start()
    await_load(1)
    table.wait()
    moves = [differs(tile_row, 1) + 2 * differs(tile_row, 2) for tile_row in range(tile_rows)]
    flips = [differs(tile_row, 0) for tile_row in range(tile_rows)]

    compute(CHUNK, CHUNK)
    send_chunk(1)

    lane = lax.broadcasted_iota(jnp.int32, (LANES, LANES), 1)

    @pl.loop(0, rows // LANES)
    def _(block):
        where = pl.ds(pl.multiple_of(PAD + block * LANES, PAD), LANES)
        result = jnp.zeros((LANES, LANES), jnp.float32)
        for side, low in enumerate((0, cols - LANES)):
            cut = pl.ds(low, LANES)
            openness = mask[where, cut].astype(jnp.float32) * fric[where, cut]
            wet = jnp.where(openness > 0.0, 1.0, 0.0)
            planes = [state[plane, where, cut] * wet for plane in range(3)] + [openness]
            for number, values in enumerate(planes):
                source = (LANES - 4) * side
                target = 16 * side + 4 * number
                moved = pltpu.roll(values, (target - source) % LANES, 1)
                result = jnp.where(lane >= target, moved, result)
        turned = result.T[0:32]
        there = pl.ds(pl.multiple_of(block * LANES, LANES), LANES)
        packed[:, there] = turned
        for number in range(4):
            outer[2 * number : 2 * number + 2, there] = turned[4 * number : 4 * number + 2]
            outer[8 + 2 * number : 10 + 2 * number, there] = turned[18 + 4 * number : 20 + 4 * number]

    @pl.when(lead_left == 1)
    def _():
        halo_to_left.start()

    @pl.when(lead_right == 1)
    def _():
        halo_to_right.start()

    @pl.loop(2, chunks)
    def _(j):
        compute(pl.multiple_of(j * CHUNK, CHUNK), CHUNK)

        @pl.when((chip != 2) | (j < split * MESSAGE // CHUNK))
        def _():
            send_chunk(j)

    @pl.when(follow_right == 1)
    def _():
        halo_to_left.wait_recv()
        halo_to_right.start()

    @pl.when(follow_left == 1)
    def _():
        halo_to_right.wait_recv()
        halo_to_left.start()

    def pass_on(m):
        raw(m, 0).wait_recv()
        relay(m).start()

    @pl.when(is_third)
    def _():
        @pl.loop(0, split)
        def _(m):
            pass_on(m)

        @pl.loop(split, messages)
        def _(m):
            raw(m, 0).wait_recv()
            where = span(m)
            by = of_row(moves, m, (MESSAGE, cols))
            near_out[where, :] = jnp.where(by == 3, first[where, :], inbox[0, where, :])
            near_direct(m).start()

    @pl.when(chip == 1)
    def _():
        pl.semaphore_wait(hello, 1)

        @pl.loop(split, messages)
        def _(m):
            give(m, first, plane_slot).start()

    @pl.when(lead_right == 1)
    def _():
        halo_to_left.wait_recv()

    @pl.when(lead_left == 1)
    def _():
        halo_to_right.wait_recv()

    for number in range(4):
        base = 4 * number
        pair = pl.ds(2 * number, 2)
        edge[number, 0:2, :] = jnp.where(me > 0, halo_left[pair, :], 0.0)
        edge[number, 2:6, :] = packed[base : base + 4, :]
        edge[number, 8:12, :] = packed[16 + base : 20 + base, :]
        edge[number, 12:14, :] = jnp.where(me < count - 1, halo_right[pair, :], 0.0)

    place = lax.broadcasted_iota(jnp.int32, (16, rows), 1)
    wet, damping = masks(edge[3])
    values = tuple(edge[plane] for plane in range(3))
    for _ in range(STEPS):
        values = advance(
            values,
            wet,
            damping,
            shift(0, -1, 16),
            shift(0, 1, 16),
            lambda a: jnp.where(place == rows - 1, 0.0, pltpu.roll(a, rows - 1, 1)),
            lambda a: jnp.where(place == 0, 0.0, pltpu.roll(a, 1, 1)),
        )
    for plane in range(3):
        edge_turn[16 * plane : 16 * plane + 16, :] = values[plane]
    for tile_row in range(tile_rows):
        cut = pl.ds(tile_row * tile, tile)
        edge_first[4 * tile_row : 4 * tile_row + 2, :] = edge_turn[2:4, cut]
        edge_first[4 * tile_row + 2 : 4 * tile_row + 4, :] = edge_turn[10:12, cut]

    @pl.when(chip != 2)
    def _():
        edge_raw(middle).start()

    @pl.when(chip == 1)
    def _():
        edge_return(plane_slot, edge_first).start()

    line = lax.broadcasted_iota(jnp.int32, (8, cols), 0)

    def by_line(pair):
        value = jnp.full((8, cols), pair[-1], jnp.int32)
        for tile_row in reversed(range(tile_rows - 1)):
            value = jnp.where(line < 4 * (tile_row + 1), pair[tile_row], value)
        return value

    edge_by = by_line(moves)

    def return_second(m):
        where = span(m)
        by = of_row(moves, m, (MESSAGE, cols))
        raw(m, 1).wait_recv()
        relay(m).wait_recv()
        turn[where, :] = for_end(by, first[where, :], inbox[1, where, :], inbox[2, where, :])
        give(m, turn, plane_slot).start()

    def settle_second(m, late):
        where = span(m)
        by = of_row(moves, m, (MESSAGE, cols))
        if late:
            raw(m, 1).wait_recv()
        own = first[where, :]
        end = inbox[0, where, :]
        near = inbox[1, where, :]
        if late:
            mine[where, :] = jnp.where(by >= 2, near, jnp.where(by == 1, end, own))
        else:
            mine[where, :] = for_middle(by, own, end, near, inbox[2, where, :])
        swap(m, 2 if late else 0).start()

    @pl.when(is_third)
    def _():
        edge_raw(0).wait_recv()
        edge_near[...] = jnp.where(edge_by == 3, edge_first[...], edge_in[0])
        edge_near_direct.start()
        pl.semaphore_wait(hello, 1)
        edge_far[...] = jnp.where(edge_by == 2, edge_first[...], edge_in[0])
        edge_far_direct(odd).start()

        @pl.loop(split, messages)
        def _(m):
            where = span(m)
            by = of_row(moves, m, (MESSAGE, cols))
            far_out[where, :] = jnp.where(by == 2, first[where, :], inbox[0, where, :])
            far_direct(m, odd).start()

    def edge_relays():
        edge_raw(0).wait_recv()
        edge_relay.start()

    @pl.when((chip == 1) & (odd == 0))
    def _():
        @pl.loop(0, AHEAD)
        def _(m):
            return_second(m)

        @pl.loop(0, split - AHEAD)
        def _(m):
            pass_on(m)
            return_second(m + AHEAD)

        @pl.loop(split - AHEAD, messages - 2)
        def _(m):
            pass_on(m)

        edge_relays()
        for m in range(messages - 2, messages):
            pass_on(m)

    @pl.when((chip == 1) & (odd == 1))
    def _():
        @pl.loop(0, LAG)
        def _(m):
            pass_on(m)

        @pl.loop(0, messages - LAG)
        def _(m):
            return_second(m)
            pass_on(m + LAG)

        @pl.loop(messages - LAG, split)
        def _(m):
            return_second(m)

        edge_relays()

    @pl.when(chip == 1)
    def _():
        @pl.loop(0, split)
        def _(m):
            settle_second(m, False)

    def patch_fields():
        @pl.loop(0, rows // LANES)
        def _(block):
            where = pl.ds(pl.multiple_of(block * LANES, LANES), LANES)
            turned = edge_turn[:, where].T
            for plane in range(3):
                on_left = pltpu.roll(turned, (-16 * plane - 2) % LANES, 1)
                cut = pl.ds(0, LANES)
                out_fields[plane, where, cut] = jnp.where(
                    lane < 2, on_left, out_fields[plane, where, cut]
                )
                on_right = pltpu.roll(turned, (LANES - 2 - 16 * plane - 10) % LANES, 1)
                cut = pl.ds(cols - LANES, LANES)
                out_fields[plane, where, cut] = jnp.where(
                    lane >= LANES - 2, on_right, out_fields[plane, where, cut]
                )

    @pl.when(is_end)
    def _():
        patch_fields()

    def settle(m, late):
        where = span(m)
        by = of_row(moves, m, (MESSAGE, cols))
        slot = 2 if late else 0

        @pl.when(is_third)
        def _():
            raw(m, 1).wait_recv()
            relay(m).wait_recv()
            own = first[where, :]
            near = inbox[1, where, :]
            far = inbox[2, where, :]
            turn[where, :] = for_end(by, own, near, far)
            give(m, turn, 0).start()
            mine[where, :] = for_middle(by, own, inbox[0, where, :], near, far)
            swap(m, slot).start()

        @pl.when(is_leaf)
        def _():
            mine[where, :] = first[where, :]
            swap(m, slot).start()

        @pl.when(is_keeper)
        def _():
            flipped = of_row(flips, m, (MESSAGE, cols)) == 1
            parts = []
            for core in range(2):
                give(m, turn, core).wait_recv()
                part = back[core, where, :]
                if late:
                    far_direct(m, core).wait_recv()
                    part = jnp.where(by >= 2, inbox[1 + core, where, :], part)
                parts.append(part)
            settled = jnp.where(by == 0, first[where, :], parts[1])
            near_out[where, :] = jnp.where(flipped, settled, parts[0])
            pass_back(m, slot).start()
            mine[where, :] = jnp.where(flipped, parts[0], settled)

        @pl.when(chip == 3)
        def _():
            give(m, turn, 0).wait_recv()
            mine[where, :] = jnp.where(by == 0, first[where, :], back[0, where, :])
            swap(m, slot).start()

    @pl.when(chip != 1)
    def _():
        @pl.loop(0, split)
        def _(m):
            settle(m, False)

    def settle_edges():
        @pl.when(is_third)
        def _():
            edge_raw(1).wait_recv()
            edge_relay.wait_recv()
            own = edge_first[...]
            near = edge_in[1]
            far = edge_in[2]
            edge_give[...] = for_end(edge_by, own, near, far)
            edge_return(0, edge_give).start()
            edge_mine[...] = for_middle(edge_by, own, edge_in[0], near, far)
            edge_swap.start()

        @pl.when(chip == 1)
        def _():
            edge_raw(1).wait_recv()
            end_or_own = jnp.where(edge_by == 1, edge_in[0], edge_first[...])
            edge_mine[...] = jnp.where(edge_by >= 2, edge_in[1], end_or_own)
            edge_swap.start()

        @pl.when(is_leaf)
        def _():
            edge_mine[...] = edge_first[...]
            edge_swap.start()

        @pl.when(is_keeper)
        def _():
            parts = []
            for core in range(2):
                edge_return(core, edge_give).wait_recv()
                edge_far_direct(core).wait_recv()
                parts.append(jnp.where(edge_by >= 2, edge_in[1 + core], edge_back[core]))
            flipped = by_line(flips) == 1
            settled = jnp.where(edge_by == 0, edge_first[...], parts[1])
            edge_near[...] = jnp.where(flipped, settled, parts[0])
            edge_pass.start()
            edge_mine[...] = jnp.where(flipped, parts[0], settled)

        @pl.when(chip == 3)
        def _():
            edge_return(0, edge_give).wait_recv()
            edge_mine[...] = jnp.where(edge_by == 0, edge_first[...], edge_back[0])
            edge_swap.start()

    choices = []
    for tile_row in range(tile_rows):
        still = jnp.where(moves[tile_row] == 0, 1, 0)
        flipped = flips[tile_row]
        choice = jnp.where(is_keeper, flipped * still, flipped)
        choices.append(jnp.where(is_leaf, 1 - (1 - flipped) * still, choice))

    def deliver(m, size=MESSAGE):
        where = pl.ds(pl.multiple_of(m * MESSAGE, MESSAGE), size)
        column = lax.broadcasted_iota(jnp.int32, (size, cols), 1)
        inside = (column >= 2) & (column < cols - 2)
        taken = of_row(choices, m, (size, cols)) == 1
        value = jnp.where(taken, other[where, :], mine[where, :])
        out_depth[where, :] = jnp.where(inside, value, edge_wide[where, :])

    def deliver_early():
        edge_swap.wait_recv()
        edge_final[0:8, :] = jnp.where(by_line(choices) == 1, edge_other[...], edge_mine[...])
        for tile_row in range(tile_rows):
            for block in range(tile // LANES):
                turned = edge_final[:, block * LANES : (block + 1) * LANES].T
                where = pl.ds(tile_row * tile + block * LANES, LANES)
                edge_wide[where, 0:LANES] = pltpu.roll(turned, (-4 * tile_row) % LANES, 1)
                edge_wide[where, cols - LANES : cols] = pltpu.roll(
                    turned, (LANES - 2 - 4 * tile_row - 2) % LANES, 1
                )
        early_rows = pl.ds(0, split * MESSAGE)
        remote(
            mine.at[early_rows, :], other.at[early_rows, :], swap_send.at[0], swap_recv.at[0], sibling
        ).wait_recv()

        @pl.loop(0, split)
        def _(m):
            deliver(m)

    @pl.when(chip == 0)
    def _():
        settle_edges()
        deliver_early()

        @pl.loop(split, messages)
        def _(m):
            settle(m, True)

    @pl.when(chip == 1)
    def _():
        settle_edges()

        @pl.loop(split, messages)
        def _(m):
            settle_second(m, True)

        patch_fields()
        deliver_early()

    @pl.when(is_third)
    def _():
        @pl.loop(split, messages - 2)
        def _(m):
            settle(m, True)

        settle_edges()
        for m in range(messages - 2, messages):
            settle(m, True)
        patch_fields()
        deliver_early()

    @pl.when(chip == 3)
    def _():
        @pl.loop(split, messages - 2)
        def _(m):
            settle(m, True)

        settle_edges()
        for m in range(messages - 2, messages):
            settle(m, True)
        deliver_early()

    start = split * MESSAGE
    late_rows = pl.ds(start, rows - start)
    remote(
        mine.at[late_rows, :], other.at[late_rows, :], swap_send.at[0], swap_recv.at[2], sibling
    ).wait_recv()
    deliver(split, rows - start)

    @pl.when((lead_left == 1) | (follow_left == 1))
    def _():
        halo_to_left.wait_send()

    @pl.when((lead_right == 1) | (follow_right == 1))
    def _():
        halo_to_right.wait_send()

    edge_raw(middle).wait_send()
    edge_swap.wait_send()

    remote(first, inbox.at[0], raw_send.at[0], in_recv.at[0, 0], toward).wait_send()
    remote(mine, other, swap_send.at[0], swap_recv.at[0], sibling).wait_send()

    @pl.when(is_middle)
    def _():
        edge_relay.wait_send()
        edge_return(plane_slot, edge_give).wait_send()
        remote(inbox.at[0], inbox.at[2], relay_send.at[0], in_recv.at[2, 0], toward).wait_send()
        remote(turn, back.at[0], back_send.at[0], in_recv.at[0, 0], outward).wait_send()


def flush(fields_ref, depth_ref, out_fields, out_depth, sem):
    copies = [
        pltpu.make_async_copy(depth_ref, out_depth, sem.at[0]),
        pltpu.make_async_copy(fields_ref, out_fields, sem.at[1]),
    ]
    for copy in copies:
        copy.start()
    for copy in copies:
        copy.wait()


def solution(mesh):
    axis = "gx"
    count = mesh.shape[axis]

    def body(fields, friction, wet_mask, owner_table):
        rows, cols = friction.shape
        padded = rows + 2 * PAD
        slots = rows // MESSAGE + 1
        f32 = jnp.float32
        whole = pltpu.VMEM((rows, cols), f32)
        small = pltpu.VMEM((8, cols), f32)
        scratch = [
            pltpu.VMEM((3, padded, cols), f32),
            pltpu.VMEM((padded, cols), f32),
            pltpu.VMEM((padded, cols), jnp.int32),
            pltpu.SMEM(owner_table.shape, jnp.int32),
            whole,
            pltpu.VMEM((3, rows, cols), f32),
            pltpu.VMEM((2, rows, cols), f32),
            whole,
            whole,
            whole,
            whole,
            whole,
            pltpu.VMEM((32, rows), f32),
            pltpu.VMEM((16, rows), f32),
            pltpu.VMEM((8, rows), f32),
            pltpu.VMEM((8, rows), f32),
            pltpu.VMEM((4, 16, rows), f32),
            pltpu.VMEM((LANES, rows), f32),
            small,
            pltpu.VMEM((3, 8, cols), f32),
            pltpu.VMEM((2, 8, cols), f32),
            small,
            small,
            small,
            small,
            small,
            pltpu.VMEM((LANES, cols), f32),
            whole,
            pltpu.SemaphoreType.DMA((2, 3)),
            pltpu.SemaphoreType.DMA,
            pltpu.SemaphoreType.DMA((2,)),
            pltpu.SemaphoreType.DMA((2,)),
            pltpu.SemaphoreType.DMA((3, slots)),
            pltpu.SemaphoreType.DMA((2,)),
            pltpu.SemaphoreType.DMA((2,)),
            pltpu.SemaphoreType.DMA((3,)),
            pltpu.SemaphoreType.DMA((2,)),
            pltpu.SemaphoreType.DMA((2,)),
            pltpu.SemaphoreType.REGULAR,
        ]
        arrays = [
            pltpu.with_memory_space_constraint(array, pltpu.HBM)
            for array in (fields, friction, wet_mask, owner_table)
        ]
        results = pl.pallas_call(
            functools.partial(kernel, axis, count),
            out_shape=(
                jax.ShapeDtypeStruct(fields.shape, f32),
                jax.ShapeDtypeStruct(friction.shape, f32),
            ),
            in_specs=[pl.BlockSpec(memory_space=pltpu.HBM)] * 4,
            out_specs=(
                pl.BlockSpec(memory_space=pltpu.VMEM),
                pl.BlockSpec(memory_space=pltpu.VMEM),
            ),
            scratch_shapes=scratch,
            compiler_params=pltpu.CompilerParams(
                collective_id=0, has_side_effects=True, vmem_limit_bytes=32 * 2**20
            ),
            name="shallow_water",
        )(*arrays)
        return pl.pallas_call(
            flush,
            out_shape=(
                jax.ShapeDtypeStruct(fields.shape, f32),
                jax.ShapeDtypeStruct(friction.shape, f32),
            ),
            in_specs=[pl.BlockSpec(memory_space=pltpu.VMEM)] * 2,
            out_specs=(
                pl.BlockSpec(memory_space=pltpu.HBM),
                pl.BlockSpec(memory_space=pltpu.HBM),
            ),
            scratch_shapes=[pltpu.SemaphoreType.DMA((2,))],
            compiler_params=pltpu.CompilerParams(vmem_limit_bytes=32 * 2**20),
            name="flush",
        )(*results)

    in_specs = (P(None, "groups", axis), P("groups", axis), P("groups", axis), P("groups", None))
    out_specs = (P(None, "groups", axis), P("groups", axis))
    return jax.shard_map(body, mesh=mesh, in_specs=in_specs, out_specs=out_specs, check_vma=False)
```

```python
import functools

import jax
import jax.numpy as jnp
from jax import lax
from jax.experimental import pallas as pl
from jax.experimental.pallas import tpu as pltpu
from jax.sharding import PartitionSpec as P

STEPS = 2
PAD = 8
CHUNK = 64
MESSAGE = 32
LAG = 8
AHEAD = 10
DIRECT = 6
FIRST = 80
LANES = 128

gravity_half = 0.5
depth_floor = 0.25
flux_factor = 0.1
time_step = 0.25


def advance(state, wet, damping, east, west, south, north):
    h, p, q = state
    inverse = 1.0 / jnp.maximum(h, depth_floor)
    u = p * inverse
    v = q * inverse
    pressure = gravity_half * h * h
    cross = q * u
    flux_p = p * u + pressure
    flux_q = q * v + pressure

    def gather(cell, flux_east, flux_south):
        quarter = 0.25 * cell
        along = flux_factor * flux_east
        down = flux_factor * flux_south
        return (east(quarter - along) + west(quarter + along)) + (
            south(quarter - down) + north(quarter + down)
        )

    return (
        wet * gather(h, p, q),
        damping * gather(p, flux_p, cross),
        damping * gather(q, cross, flux_q),
    )


def masks(openness):
    wet = jnp.where(openness > 0.0, 1.0, 0.0)
    return wet, wet / (1.0 + time_step * openness)


def kernel(
    axis,
    count,
    fields_ref,
    friction_ref,
    wet_ref,
    owner_ref,
    out_fields,
    out_depth,
    state,
    fric,
    mask,
    owner,
    first,
    inbox,
    back,
    turn,
    near_out,
    far_out,
    mine,
    other,
    packed,
    outer,
    halo_left,
    halo_right,
    edge,
    edge_turn,
    edge_first,
    edge_in,
    edge_back,
    edge_give,
    edge_near,
    edge_far,
    edge_mine,
    edge_other,
    edge_final,
    edge_wide,
    load_sem,
    table_sem,
    raw_send,
    relay_send,
    in_recv,
    back_send,
    swap_send,
    swap_recv,
    halo_send,
    halo_recv,
    hello,
):
    rows, cols = friction_ref.shape
    tile = cols
    tile_rows = rows // tile
    messages = rows // MESSAGE
    split = messages - DIRECT
    chunks = rows // CHUNK
    extra = messages
    MESH = pl.DeviceIdType.MESH

    me = lax.axis_index(axis)
    odd = me % 2
    position = me % 8
    chip = position // 2
    middle = ((chip + 1) // 2) % 2
    toward = me + 2 - 4 * (chip // 2)
    outward = 2 * me - toward
    sibling = me + 1 - 2 * odd
    keeper = me - position + 1
    is_keeper = position == 1
    is_leaf = position == 0
    is_third = chip == 2
    is_middle = middle == 1
    is_end = middle == 0

    last = jnp.where(me == count - 1, 1, 0)
    parity = (me // 8) % 2
    lead_left = jnp.where(position == 0, parity, jnp.where(position == 6, 1, 0))
    lead_left = jnp.where(me == 0, 0, lead_left)
    follow_left = jnp.where(me == 0, 0, 1 - lead_left)
    lead_right = jnp.where(position == 7, parity, jnp.where(position == 5, 0, 1)) * (1 - last)
    follow_right = (1 - last) * (1 - lead_right)

    def load(number):
        start, size = ((0, FIRST), (FIRST, rows - FIRST))[number]
        here = pl.ds(start, size)
        there = pl.ds(start + PAD, size)
        return [
            pltpu.make_async_copy(
                fields_ref.at[:, here, :], state.at[:, there, :], load_sem.at[number, 0]
            ),
            pltpu.make_async_copy(friction_ref.at[here, :], fric.at[there, :], load_sem.at[number, 1]),
            pltpu.make_async_copy(wet_ref.at[here, :], mask.at[there, :], load_sem.at[number, 2]),
        ]

    def await_load(number):
        for copy in load(number):
            copy.wait()

    table = pltpu.make_async_copy(owner_ref, owner, table_sem)
    for copy in load(0):
        copy.start()

    barrier = pltpu.get_barrier_semaphore()

    def greet(peer):
        pl.semaphore_signal(barrier, inc=1, device_id={axis: peer}, device_id_type=MESH)

    @pl.when(is_middle)
    def _():
        greet(outward)
        greet(toward)

    @pl.when(is_third)
    def _():
        greet(keeper)

    @pl.when(follow_left == 1)
    def _():
        greet(me - 1)

    @pl.when(follow_right == 1)
    def _():
        greet(me + 1)

    zero_rows = jnp.zeros((PAD, cols), jnp.float32)
    for start in (0, PAD + rows):
        for plane in range(3):
            state[plane, start : start + PAD, :] = zero_rows
        fric[start : start + PAD, :] = zero_rows
        mask[start : start + PAD, :] = jnp.zeros((PAD, cols), jnp.int32)
    for copy in load(1):
        copy.start()
    table.start()
    edge[...] = jnp.zeros_like(edge)
    edge_turn[...] = jnp.zeros_like(edge_turn)
    edge_final[...] = jnp.zeros_like(edge_final)

    def differs(tile_row, bit):
        own = owner[tile_row, me]
        return (own // 2 ** bit + me // 2 ** bit) % 2

    def remote(src, dst, send, recv, peer):
        return pltpu.make_async_remote_copy(
            src_ref=src,
            dst_ref=dst,
            send_sem=send,
            recv_sem=recv,
            device_id={axis: peer},
            device_id_type=MESH,
        )

    def span(m):
        return pl.ds(pl.multiple_of(m * MESSAGE, MESSAGE), MESSAGE)

    def raw(m, slot):
        return remote(
            first.at[span(m), :], inbox.at[slot, span(m), :], raw_send.at[0], in_recv.at[slot, m], toward
        )

    def relay(m):
        return remote(
            inbox.at[0, span(m), :], inbox.at[2, span(m), :], relay_send.at[0], in_recv.at[2, m], toward
        )

    plane_slot = jnp.where(chip == 1, odd, 0)
    receiver = jnp.where(chip == 1, keeper, outward)

    def give(m, source, slot):
        return remote(
            source.at[span(m), :],
            back.at[slot, span(m), :],
            back_send.at[0],
            in_recv.at[slot, m],
            receiver,
        )

    def near_direct(m):
        return remote(
            near_out.at[span(m), :], inbox.at[1, span(m), :], raw_send.at[0], in_recv.at[1, m], me - 2
        )

    def far_direct(m, core):
        return remote(
            far_out.at[span(m), :],
            inbox.at[1 + core, span(m), :],
            relay_send.at[0],
            in_recv.at[2, m - (1 - core) * split],
            keeper,
        )

    def pass_back(m, slot):
        return remote(
            near_out.at[span(m), :], other.at[span(m), :], swap_send.at[0], swap_recv.at[slot], sibling
        )

    def swap(m, slot):
        return remote(
            mine.at[span(m), :], other.at[span(m), :], swap_send.at[0], swap_recv.at[slot], sibling
        )

    def edge_raw(slot):
        return remote(edge_first, edge_in.at[slot], raw_send.at[1], in_recv.at[slot, extra], toward)

    edge_relay = remote(
        edge_in.at[0], edge_in.at[2], relay_send.at[1], in_recv.at[2, extra], toward
    )

    def edge_return(slot, source):
        return remote(source, edge_back.at[slot], back_send.at[1], in_recv.at[slot, extra], receiver)

    edge_near_direct = remote(
        edge_near, edge_in.at[1], raw_send.at[1], in_recv.at[1, extra], me - 2
    )

    def edge_far_direct(core):
        return remote(
            edge_far,
            edge_in.at[1 + core],
            relay_send.at[1],
            in_recv.at[2, extra - (1 - core) * split],
            keeper,
        )

    edge_pass = remote(edge_near, edge_other, swap_send.at[1], swap_recv.at[1], sibling)
    edge_swap = remote(edge_mine, edge_other, swap_send.at[1], swap_recv.at[1], sibling)

    halo_to_left = remote(
        outer.at[pl.ds(0, 8), :], halo_right, halo_send.at[0], halo_recv.at[0], me - 1
    )
    halo_to_right = remote(
        outer.at[pl.ds(8, 8), :], halo_left, halo_send.at[1], halo_recv.at[1], me + 1
    )

    def shift(axis_number, amount, size):
        return lambda a: pltpu.roll(a, amount % size, axis_number)

    def compute(at, size):
        reach = size + 2 * PAD
        where = pl.ds(at, reach)
        openness = mask[where, :].astype(jnp.float32) * fric[where, :]
        wet, damping = masks(openness)
        values = tuple(state[plane, where, :] * wet for plane in range(3))
        for _ in range(STEPS):
            values = advance(
                values,
                wet,
                damping,
                shift(1, -1, cols),
                shift(1, 1, cols),
                shift(0, -1, reach),
                shift(0, 1, reach),
            )
        here = pl.ds(at, size)
        first[here, :] = values[0][PAD : PAD + size]
        for plane in range(3):
            out_fields[plane, here, :] = values[plane][PAD : PAD + size]

    def for_end(by, own, near, far):
        return jnp.where(by == 3, far, jnp.where(by == 2, near, own))

    def for_middle(by, own, end, near, far):
        return jnp.where(by == 3, near, jnp.where(by == 2, far, jnp.where(by == 1, end, own)))

    def of_row(pair, m, shape):
        value = pair[-1]
        for tile_row in reversed(range(tile_rows - 1)):
            value = jnp.where(m < (tile_row + 1) * (tile // MESSAGE), pair[tile_row], value)
        return jnp.full(shape, value, jnp.int32)

    def send_chunk(number):
        for part in range(CHUNK // MESSAGE):
            raw(number * (CHUNK // MESSAGE) + part, middle).start()

    @pl.when(is_keeper)
    def _():
        pl.semaphore_wait(barrier, 3 + lead_left + lead_right)
        for ahead in range(1, 5):
            pl.semaphore_signal(hello, inc=1, device_id={axis: me + ahead}, device_id_type=MESH)

    await_load(0)
    compute(0, MESSAGE)

    @pl.when(position != 1)
    def _():
        pl.semaphore_wait(barrier, 1 + lead_left + lead_right)

    raw(0, middle).start()
    for part in range(1, CHUNK // MESSAGE):
        compute(part * MESSAGE, MESSAGE)
        raw(part, middle).start()
    await_load(1)
    table.wait()
    moves = [differs(tile_row, 1) + 2 * differs(tile_row, 2) for tile_row in range(tile_rows)]
    flips = [differs(tile_row, 0) for tile_row in range(tile_rows)]

    compute(CHUNK, CHUNK)
    send_chunk(1)

    lane = lax.broadcasted_iota(jnp.int32, (LANES, LANES), 1)

    @pl.loop(0, rows // LANES)
    def _(block):
        where = pl.ds(pl.multiple_of(PAD + block * LANES, PAD), LANES)
        result = jnp.zeros((LANES, LANES), jnp.float32)
        for side, low in enumerate((0, cols - LANES)):
            cut = pl.ds(low, LANES)
            openness = mask[where, cut].astype(jnp.float32) * fric[where, cut]
            wet = jnp.where(openness > 0.0, 1.0, 0.0)
            planes = [state[plane, where, cut] * wet for plane in range(3)] + [openness]
            for number, values in enumerate(planes):
                source = (LANES - 4) * side
                target = 16 * side + 4 * number
                moved = pltpu.roll(values, (target - source) % LANES, 1)
                result = jnp.where(lane >= target, moved, result)
        turned = result.T[0:32]
        there = pl.ds(pl.multiple_of(block * LANES, LANES), LANES)
        packed[:, there] = turned
        for number in range(4):
            outer[2 * number : 2 * number + 2, there] = turned[4 * number : 4 * number + 2]
            outer[8 + 2 * number : 10 + 2 * number, there] = turned[18 + 4 * number : 20 + 4 * number]

    @pl.when(lead_left == 1)
    def _():
        halo_to_left.start()

    @pl.when(lead_right == 1)
    def _():
        halo_to_right.start()

    @pl.loop(2, chunks)
    def _(j):
        compute(pl.multiple_of(j * CHUNK, CHUNK), CHUNK)

        @pl.when((chip != 2) | (j < split * MESSAGE // CHUNK))
        def _():
            send_chunk(j)

    @pl.when(follow_right == 1)
    def _():
        halo_to_left.wait_recv()
        halo_to_right.start()

    @pl.when(follow_left == 1)
    def _():
        halo_to_right.wait_recv()
        halo_to_left.start()

    def pass_on(m):
        raw(m, 0).wait_recv()
        relay(m).start()

    @pl.when(is_third)
    def _():
        @pl.loop(0, split)
        def _(m):
            pass_on(m)

        @pl.loop(split, messages)
        def _(m):
            raw(m, 0).wait_recv()
            where = span(m)
            by = of_row(moves, m, (MESSAGE, cols))
            near_out[where, :] = jnp.where(by == 3, first[where, :], inbox[0, where, :])
            near_direct(m).start()

    @pl.when(chip == 1)
    def _():
        pl.semaphore_wait(hello, 1)

        @pl.loop(split, messages)
        def _(m):
            give(m, first, plane_slot).start()

    @pl.when(lead_right == 1)
    def _():
        halo_to_left.wait_recv()

    @pl.when(lead_left == 1)
    def _():
        halo_to_right.wait_recv()

    for number in range(4):
        base = 4 * number
        pair = pl.ds(2 * number, 2)
        edge[number, 0:2, :] = jnp.where(me > 0, halo_left[pair, :], 0.0)
        edge[number, 2:6, :] = packed[base : base + 4, :]
        edge[number, 8:12, :] = packed[16 + base : 20 + base, :]
        edge[number, 12:14, :] = jnp.where(me < count - 1, halo_right[pair, :], 0.0)

    place = lax.broadcasted_iota(jnp.int32, (16, rows), 1)
    wet, damping = masks(edge[3])
    values = tuple(edge[plane] for plane in range(3))
    for _ in range(STEPS):
        values = advance(
            values,
            wet,
            damping,
            shift(0, -1, 16),
            shift(0, 1, 16),
            lambda a: jnp.where(place == rows - 1, 0.0, pltpu.roll(a, rows - 1, 1)),
            lambda a: jnp.where(place == 0, 0.0, pltpu.roll(a, 1, 1)),
        )
    for plane in range(3):
        edge_turn[16 * plane : 16 * plane + 16, :] = values[plane]
    for tile_row in range(tile_rows):
        cut = pl.ds(tile_row * tile, tile)
        edge_first[4 * tile_row : 4 * tile_row + 2, :] = edge_turn[2:4, cut]
        edge_first[4 * tile_row + 2 : 4 * tile_row + 4, :] = edge_turn[10:12, cut]

    @pl.when(chip != 2)
    def _():
        edge_raw(middle).start()

    @pl.when(chip == 1)
    def _():
        edge_return(plane_slot, edge_first).start()

    line = lax.broadcasted_iota(jnp.int32, (8, cols), 0)

    def by_line(pair):
        value = jnp.full((8, cols), pair[-1], jnp.int32)
        for tile_row in reversed(range(tile_rows - 1)):
            value = jnp.where(line < 4 * (tile_row + 1), pair[tile_row], value)
        return value

    edge_by = by_line(moves)

    def return_second(m):
        where = span(m)
        by = of_row(moves, m, (MESSAGE, cols))
        raw(m, 1).wait_recv()
        relay(m).wait_recv()
        turn[where, :] = for_end(by, first[where, :], inbox[1, where, :], inbox[2, where, :])
        give(m, turn, plane_slot).start()

    def settle_second(m, late):
        where = span(m)
        by = of_row(moves, m, (MESSAGE, cols))
        if late:
            raw(m, 1).wait_recv()
        own = first[where, :]
        end = inbox[0, where, :]
        near = inbox[1, where, :]
        if late:
            mine[where, :] = jnp.where(by >= 2, near, jnp.where(by == 1, end, own))
        else:
            mine[where, :] = for_middle(by, own, end, near, inbox[2, where, :])
        swap(m, 2 if late else 0).start()

    @pl.when(is_third)
    def _():
        edge_raw(0).wait_recv()
        edge_near[...] = jnp.where(edge_by == 3, edge_first[...], edge_in[0])
        edge_near_direct.start()
        pl.semaphore_wait(hello, 1)
        edge_far[...] = jnp.where(edge_by == 2, edge_first[...], edge_in[0])
        edge_far_direct(odd).start()

        @pl.loop(split, messages)
        def _(m):
            where = span(m)
            by = of_row(moves, m, (MESSAGE, cols))
            far_out[where, :] = jnp.where(by == 2, first[where, :], inbox[0, where, :])
            far_direct(m, odd).start()

    def edge_relays():
        edge_raw(0).wait_recv()
        edge_relay.start()

    @pl.when((chip == 1) & (odd == 0))
    def _():
        @pl.loop(0, AHEAD)
        def _(m):
            return_second(m)

        @pl.loop(0, split - AHEAD)
        def _(m):
            pass_on(m)
            return_second(m + AHEAD)

        @pl.loop(split - AHEAD, messages - 2)
        def _(m):
            pass_on(m)

        edge_relays()
        for m in range(messages - 2, messages):
            pass_on(m)

    @pl.when((chip == 1) & (odd == 1))
    def _():
        @pl.loop(0, LAG)
        def _(m):
            pass_on(m)

        @pl.loop(0, messages - LAG)
        def _(m):
            return_second(m)
            pass_on(m + LAG)

        @pl.loop(messages - LAG, split)
        def _(m):
            return_second(m)

        edge_relays()

    @pl.when(chip == 1)
    def _():
        @pl.loop(0, split)
        def _(m):
            settle_second(m, False)

    def patch_fields():
        @pl.loop(0, rows // LANES)
        def _(block):
            where = pl.ds(pl.multiple_of(block * LANES, LANES), LANES)
            turned = edge_turn[:, where].T
            for plane in range(3):
                on_left = pltpu.roll(turned, (-16 * plane - 2) % LANES, 1)
                cut = pl.ds(0, LANES)
                out_fields[plane, where, cut] = jnp.where(
                    lane < 2, on_left, out_fields[plane, where, cut]
                )
                on_right = pltpu.roll(turned, (LANES - 2 - 16 * plane - 10) % LANES, 1)
                cut = pl.ds(cols - LANES, LANES)
                out_fields[plane, where, cut] = jnp.where(
                    lane >= LANES - 2, on_right, out_fields[plane, where, cut]
                )

    @pl.when(is_end)
    def _():
        patch_fields()

    def settle(m, late):
        where = span(m)
        by = of_row(moves, m, (MESSAGE, cols))
        slot = 2 if late else 0

        @pl.when(is_third)
        def _():
            raw(m, 1).wait_recv()
            relay(m).wait_recv()
            own = first[where, :]
            near = inbox[1, where, :]
            far = inbox[2, where, :]
            turn[where, :] = for_end(by, own, near, far)
            give(m, turn, 0).start()
            mine[where, :] = for_middle(by, own, inbox[0, where, :], near, far)
            swap(m, slot).start()

        @pl.when(is_leaf)
        def _():
            mine[where, :] = first[where, :]
            swap(m, slot).start()

        @pl.when(is_keeper)
        def _():
            flipped = of_row(flips, m, (MESSAGE, cols)) == 1
            parts = []
            for core in range(2):
                give(m, turn, core).wait_recv()
                part = back[core, where, :]
                if late:
                    far_direct(m, core).wait_recv()
                    part = jnp.where(by >= 2, inbox[1 + core, where, :], part)
                parts.append(part)
            settled = jnp.where(by == 0, first[where, :], parts[1])
            near_out[where, :] = jnp.where(flipped, settled, parts[0])
            pass_back(m, slot).start()
            mine[where, :] = jnp.where(flipped, parts[0], settled)

        @pl.when(chip == 3)
        def _():
            give(m, turn, 0).wait_recv()
            mine[where, :] = jnp.where(by == 0, first[where, :], back[0, where, :])
            swap(m, slot).start()

    @pl.when(chip != 1)
    def _():
        @pl.loop(0, split)
        def _(m):
            settle(m, False)

    def settle_edges():
        @pl.when(is_third)
        def _():
            edge_raw(1).wait_recv()
            edge_relay.wait_recv()
            own = edge_first[...]
            near = edge_in[1]
            far = edge_in[2]
            edge_give[...] = for_end(edge_by, own, near, far)
            edge_return(0, edge_give).start()
            edge_mine[...] = for_middle(edge_by, own, edge_in[0], near, far)
            edge_swap.start()

        @pl.when(chip == 1)
        def _():
            edge_raw(1).wait_recv()
            end_or_own = jnp.where(edge_by == 1, edge_in[0], edge_first[...])
            edge_mine[...] = jnp.where(edge_by >= 2, edge_in[1], end_or_own)
            edge_swap.start()

        @pl.when(is_leaf)
        def _():
            edge_mine[...] = edge_first[...]
            edge_swap.start()

        @pl.when(is_keeper)
        def _():
            parts = []
            for core in range(2):
                edge_return(core, edge_give).wait_recv()
                edge_far_direct(core).wait_recv()
                parts.append(jnp.where(edge_by >= 2, edge_in[1 + core], edge_back[core]))
            flipped = by_line(flips) == 1
            settled = jnp.where(edge_by == 0, edge_first[...], parts[1])
            edge_near[...] = jnp.where(flipped, settled, parts[0])
            edge_pass.start()
            edge_mine[...] = jnp.where(flipped, parts[0], settled)

        @pl.when(chip == 3)
        def _():
            edge_return(0, edge_give).wait_recv()
            edge_mine[...] = jnp.where(edge_by == 0, edge_first[...], edge_back[0])
            edge_swap.start()

    choices = []
    for tile_row in range(tile_rows):
        still = jnp.where(moves[tile_row] == 0, 1, 0)
        flipped = flips[tile_row]
        choice = jnp.where(is_keeper, flipped * still, flipped)
        choices.append(jnp.where(is_leaf, 1 - (1 - flipped) * still, choice))

    def deliver(m, size=MESSAGE):
        where = pl.ds(pl.multiple_of(m * MESSAGE, MESSAGE), size)
        column = lax.broadcasted_iota(jnp.int32, (size, cols), 1)
        inside = (column >= 2) & (column < cols - 2)
        taken = of_row(choices, m, (size, cols)) == 1
        value = jnp.where(taken, other[where, :], mine[where, :])
        out_depth[where, :] = jnp.where(inside, value, edge_wide[where, :])

    def deliver_early():
        edge_swap.wait_recv()
        edge_final[0:8, :] = jnp.where(by_line(choices) == 1, edge_other[...], edge_mine[...])
        for tile_row in range(tile_rows):
            for block in range(tile // LANES):
                turned = edge_final[:, block * LANES : (block + 1) * LANES].T
                where = pl.ds(tile_row * tile + block * LANES, LANES)
                edge_wide[where, 0:LANES] = pltpu.roll(turned, (-4 * tile_row) % LANES, 1)
                edge_wide[where, cols - LANES : cols] = pltpu.roll(
                    turned, (LANES - 2 - 4 * tile_row - 2) % LANES, 1
                )
        early_rows = pl.ds(0, split * MESSAGE)
        remote(
            mine.at[early_rows, :], other.at[early_rows, :], swap_send.at[0], swap_recv.at[0], sibling
        ).wait_recv()

        @pl.loop(0, split)
        def _(m):
            deliver(m)

    @pl.when(chip == 0)
    def _():
        settle_edges()
        deliver_early()

        @pl.loop(split, messages)
        def _(m):
            settle(m, True)

    @pl.when(chip == 1)
    def _():
        settle_edges()

        @pl.loop(split, messages)
        def _(m):
            settle_second(m, True)

        patch_fields()
        deliver_early()

    @pl.when(is_third)
    def _():
        @pl.loop(split, messages - 2)
        def _(m):
            settle(m, True)

        settle_edges()
        for m in range(messages - 2, messages):
            settle(m, True)
        patch_fields()
        deliver_early()

    @pl.when(chip == 3)
    def _():
        @pl.loop(split, messages - 2)
        def _(m):
            settle(m, True)

        settle_edges()
        for m in range(messages - 2, messages):
            settle(m, True)
        deliver_early()

    start = split * MESSAGE
    late_rows = pl.ds(start, rows - start)
    remote(
        mine.at[late_rows, :], other.at[late_rows, :], swap_send.at[0], swap_recv.at[2], sibling
    ).wait_recv()
    deliver(split, rows - start)

    @pl.when((lead_left == 1) | (follow_left == 1))
    def _():
        halo_to_left.wait_send()

    @pl.when((lead_right == 1) | (follow_right == 1))
    def _():
        halo_to_right.wait_send()

    edge_raw(middle).wait_send()
    edge_swap.wait_send()

    remote(first, inbox.at[0], raw_send.at[0], in_recv.at[0, 0], toward).wait_send()
    remote(mine, other, swap_send.at[0], swap_recv.at[0], sibling).wait_send()

    @pl.when(is_middle)
    def _():
        edge_relay.wait_send()
        edge_return(plane_slot, edge_give).wait_send()
        remote(inbox.at[0], inbox.at[2], relay_send.at[0], in_recv.at[2, 0], toward).wait_send()
        remote(turn, back.at[0], back_send.at[0], in_recv.at[0, 0], outward).wait_send()


def flush(fields_ref, depth_ref, out_fields, out_depth, sem):
    copies = [
        pltpu.make_async_copy(depth_ref, out_depth, sem.at[0]),
        pltpu.make_async_copy(fields_ref, out_fields, sem.at[1]),
    ]
    for copy in copies:
        copy.start()
    for copy in copies:
        copy.wait()


def solution(mesh):
    axis = "gx"
    count = mesh.shape[axis]

    def body(fields, friction, wet_mask, owner_table):
        rows, cols = friction.shape
        padded = rows + 2 * PAD
        slots = rows // MESSAGE + 1
        f32 = jnp.float32
        whole = pltpu.VMEM((rows, cols), f32)
        small = pltpu.VMEM((8, cols), f32)
        scratch = [
            pltpu.VMEM((3, padded, cols), f32),
            pltpu.VMEM((padded, cols), f32),
            pltpu.VMEM((padded, cols), jnp.int32),
            pltpu.SMEM(owner_table.shape, jnp.int32),
            whole,
            pltpu.VMEM((3, rows, cols), f32),
            pltpu.VMEM((2, rows, cols), f32),
            whole,
            whole,
            whole,
            whole,
            whole,
            pltpu.VMEM((32, rows), f32),
            pltpu.VMEM((16, rows), f32),
            pltpu.VMEM((8, rows), f32),
            pltpu.VMEM((8, rows), f32),
            pltpu.VMEM((4, 16, rows), f32),
            pltpu.VMEM((LANES, rows), f32),
            small,
            pltpu.VMEM((3, 8, cols), f32),
            pltpu.VMEM((2, 8, cols), f32),
            small,
            small,
            small,
            small,
            small,
            pltpu.VMEM((LANES, cols), f32),
            whole,
            pltpu.SemaphoreType.DMA((2, 3)),
            pltpu.SemaphoreType.DMA,
            pltpu.SemaphoreType.DMA((2,)),
            pltpu.SemaphoreType.DMA((2,)),
            pltpu.SemaphoreType.DMA((3, slots)),
            pltpu.SemaphoreType.DMA((2,)),
            pltpu.SemaphoreType.DMA((2,)),
            pltpu.SemaphoreType.DMA((3,)),
            pltpu.SemaphoreType.DMA((2,)),
            pltpu.SemaphoreType.DMA((2,)),
            pltpu.SemaphoreType.REGULAR,
        ]
        arrays = [
            pltpu.with_memory_space_constraint(array, pltpu.HBM)
            for array in (fields, friction, wet_mask, owner_table)
        ]
        results = pl.pallas_call(
            functools.partial(kernel, axis, count),
            out_shape=(
                jax.ShapeDtypeStruct(fields.shape, f32),
                jax.ShapeDtypeStruct(friction.shape, f32),
            ),
            in_specs=[pl.BlockSpec(memory_space=pltpu.HBM)] * 4,
            out_specs=(
                pl.BlockSpec(memory_space=pltpu.VMEM),
                pl.BlockSpec(memory_space=pltpu.VMEM),
            ),
            scratch_shapes=scratch,
            compiler_params=pltpu.CompilerParams(
                collective_id=0, has_side_effects=True, vmem_limit_bytes=32 * 2**20
            ),
            name="shallow_water",
        )(*arrays)
        return pl.pallas_call(
            flush,
            out_shape=(
                jax.ShapeDtypeStruct(fields.shape, f32),
                jax.ShapeDtypeStruct(friction.shape, f32),
            ),
            in_specs=[pl.BlockSpec(memory_space=pltpu.VMEM)] * 2,
            out_specs=(
                pl.BlockSpec(memory_space=pltpu.HBM),
                pl.BlockSpec(memory_space=pltpu.HBM),
            ),
            scratch_shapes=[pltpu.SemaphoreType.DMA((2,))],
            compiler_params=pltpu.CompilerParams(vmem_limit_bytes=32 * 2**20),
            name="flush",
        )(*results)

    in_specs = (P(None, "groups", axis), P("groups", axis), P("groups", axis), P("groups", None))
    out_specs = (P(None, "groups", axis), P("groups", axis))
    return jax.shard_map(body, mesh=mesh, in_specs=in_specs, out_specs=out_specs, check_vma=False)
```
